256 devices in a mesh: wide: 128 (over y_lo, z, x, core), narrow: 2 (over y_hi).
Axes of the slice: x: 4, y: 4 (y_hi: 2, y_lo: 2; y = y_hi * 2 + y_lo), z: 8, core: 2. Of those that a mesh axis runs over, the one named last changes fastest.
Arguments:
- points: bfloat16 [4096, 3, 512], P('wide'), may hold values from -6 to 6
- vectors: bfloat16 [4096, 16, 512], P('wide', None, 'narrow'), may hold values from -6 to 6
- counts: int32 [128], P('wide'), may hold values from 8 to 32, as said below
- src_basis: bfloat16 [4096, 64, 512], P('wide', None, 'narrow'), may hold values from -0.25 to 0.25
- tgt_basis: bfloat16 [4096, 64, 512], P('wide'), may hold values from -0.75 to 0.75
- adm_src: int32 [4096, 8], P('wide'), may hold values from 0 to 4095, as said below
- couplings: bfloat16 [4096, 64, 512], P('wide'), may hold values from -0.25 to 0.25
Outputs:
- field: bfloat16 [4096, 16, 512], P('wide', None, 'narrow')
The draws below stay inside these ranges and needn't reach their ends.
Inputs may be any that keep to these rules, and one draw needn't show every extreme that they name: `counts`: some index of wide holds exactly 32 live slots. `adm_src`: every entry is a live slot: d * 32 + s with s < counts[d].
All inputs are finite; a program needn't handle non-finite values.
Results may differ from the reference program's by a relative error of at most 0.005.
Values may be sent and summed in bfloat16 or wider, within the bound.
No kernel may reach another device: no remote copies, remote signals or barrier semaphores. Data moves between devices by JAX's collectives and lax.ppermute only.
A program may use at most 64 MiB of HBM per device.

```python
import math
import jax
import jax.numpy as jnp
from jax import lax

LEAF = 512
RANK = 64
RHS = 16
ADM = 8
LEAF_DEV = 32
LEAVES = 4096
N_WIDE = 128


def shared_counts(key):
    inner = jax.random.fold_in(key, 7)
    first_key, second_key = jax.random.split(inner)
    base = jax.random.randint(first_key, (N_WIDE,), LEAF_DEV // 4, LEAF_DEV + 1)
    fullest = jax.random.randint(second_key, (), 0, N_WIDE)
    return base.at[fullest].set(LEAF_DEV).astype(jnp.int32)


def draw_counts(key, part):
    return shared_counts(key)


def draw_adm_src(key, part):
    live_counts = shared_counts(key)
    inner = jax.random.fold_in(key, 19)
    first_key, second_key = jax.random.split(inner)
    source_dev = jax.random.randint(first_key, (LEAF_DEV * N_WIDE, ADM), 0, N_WIDE)
    raw_slot = jax.random.randint(second_key, (LEAF_DEV * N_WIDE, ADM), 0, 1048576)
    slot_pick = raw_slot % live_counts[source_dev]
    return (source_dev * LEAF_DEV + slot_pick).astype(jnp.int32)


def block_scale(own_key, dims, cuts, low, high):
    gain, own = 1.0, jax.random.fold_in(own_key, 6)
    for dim, blocks in cuts:
        heights = jnp.exp(jax.random.uniform(jax.random.fold_in(own, dim), (blocks,), jnp.float32, low / len(cuts), high / len(cuts)))
        gain = gain * jnp.repeat(heights, dims[dim] // blocks).reshape([-1 if axis == dim else 1 for axis in range(len(dims))])
    return gain


def normal_values(key, shape, scale, reach, cuts=(), held_as=jnp.bfloat16):
    array = scale * jax.random.normal(key, shape, jnp.float32)
    if cuts:
        array = array * block_scale(key, shape, cuts, -0.22, 0.18)
    return jnp.clip(array, -reach, reach).astype(held_as)


def setup_inputs(seed: int = 0) -> dict:
    key_list = jax.random.split(jax.random.key(seed), 8)
    return {
        "points": normal_values(key_list[0], (LEAVES, 3, LEAF), 1.0, 6.0, ((0, 128),)),
        "vectors": normal_values(key_list[1], (LEAVES, RHS, LEAF), 1.0, 6.0, ((0, 128), (2, 2))),
        "counts": draw_counts(jax.random.fold_in(key_list[7], 71), 0),
        "src_basis": normal_values(key_list[3], (LEAVES, RANK, LEAF), LEAF ** -0.5, 0.25, ((0, 128), (2, 2))),
        "tgt_basis": normal_values(key_list[4], (LEAVES, RANK, LEAF), RANK ** -0.5, 0.75, ((0, 128),)),
        "adm_src": draw_adm_src(jax.random.fold_in(key_list[7], 71), 0),
        "couplings": normal_values(key_list[6], (LEAVES, RANK, ADM * RANK), (ADM * RANK) ** -0.5, 0.25, ((0, 128),)),
    }


inverse_four_pi = 1.0 / (4.0 * math.pi)
soften_sq = 0.0025

def kernel_block(targets, sources):
    target_f = targets.astype(jnp.float32)
    source_f = sources.astype(jnp.float32)
    squared = jnp.zeros((targets.shape[1], sources.shape[1]), jnp.float32)
    for axis_index in range(3):
        differ = target_f[axis_index][:, None] - source_f[axis_index][None, :]
        squared = squared + differ * differ
    return (inverse_four_pi / jnp.sqrt(squared + soften_sq)).astype(jnp.bfloat16)

def near_leaf(targets, sources, source_vals):
    kernel = kernel_block(targets, sources)
    return jnp.einsum('pq,rq->rp', kernel.astype(jnp.float32), source_vals.astype(jnp.float32))

def near_block_sum(points, source_points, source_vals, group_size):
    leaves = points.shape[0]
    shaped = (points.reshape((leaves // group_size, group_size) + points.shape[1:]), source_points.reshape((leaves // group_size, group_size) + source_points.shape[1:]), source_vals.reshape((leaves // group_size, group_size) + source_vals.shape[1:]))

    def run_group(blocks):
        return jax.vmap(near_leaf)(blocks[0], blocks[1], blocks[2])
    result = lax.map(run_group, shaped)
    return result.reshape((leaves,) + result.shape[2:])

def reference(points, vectors, counts, src_basis, tgt_basis, adm_src, couplings):
    leaf_ids = jnp.arange(LEAF_DEV * N_WIDE, dtype=jnp.int32)
    device_ids = leaf_ids // LEAF_DEV
    slot_ids = leaf_ids % LEAF_DEV
    own_count = counts[device_ids]
    is_live = slot_ids < own_count
    values = jnp.where(is_live[:, None, None], vectors, jnp.zeros_like(vectors))
    before_dev = (device_ids + N_WIDE - 1) % N_WIDE
    after_dev = (device_ids + 1) % N_WIDE
    previous = jnp.where(slot_ids > 0, leaf_ids - 1, before_dev * LEAF_DEV + counts[before_dev] - 1).astype(jnp.int32)
    following = jnp.where(slot_ids < own_count - 1, leaf_ids + 1, after_dev * LEAF_DEV).astype(jnp.int32)
    source_points = jnp.concatenate([points[previous], points, points[following]], 2)
    source_vals = jnp.concatenate([values[previous], values, values[following]], 2)
    near_part = near_block_sum(points, source_points, source_vals, 8)
    partial_value = jnp.einsum('lrp,lap->lra', values.astype(jnp.float32), src_basis.astype(jnp.float32))
    coeffs = partial_value.astype(jnp.bfloat16)
    selected = coeffs[adm_src]
    selected = selected.transpose(0, 2, 1, 3).reshape(LEAF_DEV * N_WIDE, RHS, ADM * RANK)
    target_coeffs = jnp.einsum('lrk,lak->lra', selected.astype(jnp.float32), couplings.astype(jnp.float32)).astype(jnp.bfloat16)
    far_field = jnp.einsum('lra,lap->lrp', target_coeffs.astype(jnp.float32), tgt_basis.astype(jnp.float32))
    summed = near_part + far_field
    return jnp.where(is_live[:, None, None], summed, jnp.zeros_like(summed)).astype(jnp.bfloat16)
```

```python
import math

import jax
import jax.numpy as jnp
from jax import lax
from jax.experimental import pallas as pl
from jax.experimental.pallas import tpu as pltpu
from jax.sharding import Mesh
from jax.sharding import PartitionSpec as P

WIDE = ("y", "z", "x", "c")
PEERS = ("y", "x", "c")

inverse_four_pi = 1.0 / (4.0 * math.pi)
soften_sq = 0.0025

T, R, A, J, HALF, LEAF = 32, 16, 64, 8, 256, 512
RH = R // 2
N_Z, N_PEER = 8, 16
CAP = 48
ENTRIES = T * J
COLUMN = N_Z * T
bf16, f32, i32 = jnp.bfloat16, jnp.float32, jnp.int32

VMEM = pl.BlockSpec(memory_space=pltpu.VMEM)
SMEM = pl.BlockSpec(memory_space=pltpu.SMEM)


def nt(a, b):
    return lax.dot_general(a, b, (((1,), (1,)), ((), ())), preferred_element_type=f32)


def nn(a, b):
    return lax.dot_general(a, b, (((1,), (0,)), ((), ())), preferred_element_type=f32)


def iota(shape, dim):
    return lax.broadcasted_iota(i32, shape, dim)


def folded(wide):
    two = wide[:, :128] + wide[:, 128:]
    return two[:, :64] + two[:, 64:]


def index_kernel(count_ref, adm_ref, sel_ref, req_ref):
    count = count_ref[0]
    adm = jnp.concatenate([adm_ref[...].astype(f32), jnp.zeros((8, 96), f32)], 1).T
    leaf = jnp.concatenate(
        [jnp.broadcast_to(adm[:T, j : j + 1], (T, 128)) for j in range(J)], 0
    ).astype(i32)
    live = (iota((ENTRIES, 128), 0) & (T - 1)) < count
    column = (leaf >> 11) * 8 + ((leaf >> 5) & 7)
    row = ((leaf >> 8) & 7) * T + (leaf & (T - 1))
    member = jnp.where((column == iota((ENTRIES, 128), 1)) & live, 1.0, 0.0)
    below = jnp.where(iota((ENTRIES, ENTRIES), 0) > iota((ENTRIES, ENTRIES), 1), 1.0, 0.0)
    rank = nn(below.astype(bf16), member.astype(bf16))
    place = jnp.sum(member * rank, axis=1, keepdims=True)
    over = jnp.max(place) > CAP - 0.5
    place = jnp.broadcast_to(place, (ENTRIES, 128))
    fits = live & (place < CAP - 0.5)
    sel = jnp.where(fits, column * CAP + place.astype(i32), -1)
    sel_ref[...] = sel
    sel_row = sel.astype(f32).T[:1]
    slots = N_PEER * CAP
    pick = jnp.where(iota((slots, ENTRIES), 0) == sel_row.astype(i32), 1.0, 0.0).astype(bf16)
    wanted = nn(pick, (row + 1).astype(f32).astype(bf16))
    wanted = jnp.where(over, -1.0, wanted)
    req_ref[...] = wanted.astype(bf16).reshape(N_PEER, CAP, 128)


def index_call(counts, adm):
    return pl.pallas_call(
        index_kernel,
        out_shape=(
            jax.ShapeDtypeStruct((ENTRIES, 128), i32),
            jax.ShapeDtypeStruct((N_PEER, CAP, 128), bf16),
        ),
        in_specs=[SMEM, VMEM],
        out_specs=(VMEM, VMEM),
        name="requests",
    )(counts, adm)


def coeff_kernel(n_ref, vec_ref, basis_ref, keep_ref, send_ref, rows):
    n = n_ref[0]
    same = (iota((64, 256), 0) >> 4) == (iota((64, 256), 1) >> 6)
    for g in range(T // 4):
        lhs = vec_ref[4 * g : 4 * g + 4].reshape(64, HALF)
        rhs = basis_ref[4 * g : 4 * g + 4].reshape(4 * A, HALF)
        rows[64 * g : 64 * g + 64, :64] = folded(jnp.where(same, nt(lhs, rhs), 0.0))
    for out, first in ((send_ref, (1 - n) * RH), (keep_ref, n * RH)):
        for r in range(0, RH, 2):
            pair = [rows[pl.ds(first + r + k, T, stride=R), :][:, :64] for k in range(2)]
            out[:, r * A : (r + 2) * A] = jnp.concatenate(pair, 1)


def coeff_call(n, vectors, basis):
    shape = jax.ShapeDtypeStruct((T, RH * A), f32)
    return pl.pallas_call(
        coeff_kernel,
        out_shape=(shape, shape),
        in_specs=[SMEM, VMEM, VMEM],
        out_specs=(VMEM, VMEM),
        scratch_shapes=[pltpu.VMEM((T * R, 128), f32)],
        name="coeffs",
    )(n, vectors, basis)


def pack_kernel(req_ref, table_ref, out_ref):
    lanes = iota((CAP, 128), 1).astype(f32) + 1.0
    for r in range(0, N_PEER, 4):
        want = [req_ref[r + k].astype(f32) for k in range(4)]
        hot = [
            jnp.concatenate(
                [jnp.where(w == lanes, 1.0, 0.0), jnp.where(w == lanes + 128.0, 1.0, 0.0)], 1
            )
            for w in want
        ]
        picked = nn(jnp.concatenate(hot, 0).astype(bf16), table_ref[...])
        out_ref[r : r + 4] = picked.astype(bf16).reshape(4, CAP, RH * A)


def pack_call(req, table):
    return pl.pallas_call(
        pack_kernel,
        out_shape=jax.ShapeDtypeStruct((N_PEER, CAP, RH * A), bf16),
        in_specs=[VMEM, VMEM],
        out_specs=VMEM,
        name="pack",
    )(req, table)


def couple(picked, couple_ref, out_ref):
    lows = [picked[j * T : (j + 1) * T] for j in range(J)]
    by_rhs = []
    for r in range(RH):
        cols = [low[:, r * A : (r + 1) * A] for low in lows]
        by_rhs.append(jnp.concatenate(cols, 1).astype(bf16))
    row_t = iota((16 * RH, 256), 0) & 15
    col_t = iota((16 * RH, 256), 1) >> 6
    for h in range(2):
        lhs = jnp.concatenate([s[16 * h : 16 * h + 16] for s in by_rhs], 0)
        total = jnp.zeros((16 * RH, A), f32)
        for g in range(4):
            first = 16 * h + 4 * g
            rhs = couple_ref[first : first + 4].reshape(4 * A, J * A)
            total = total + folded(jnp.where(row_t == col_t + 4 * g, nt(lhs, rhs), 0.0))
        total = total.reshape(RH, 16, A)
        for r in range(0, RH, 2):
            pair = jnp.concatenate([total[r], total[r + 1]], 1)
            out_ref[r // 2, 16 * h : 16 * h + 16, :] = pair.astype(bf16)


def select_kernel(sel_ref, got_ref, couple_ref, out_ref):
    slots = N_PEER * CAP
    sel = sel_ref[...]
    lanes = iota((ENTRIES, 128), 1)
    hot = jnp.concatenate(
        [jnp.where(sel == lanes + 128 * k, 1.0, 0.0) for k in range(slots // 128)], 1
    )
    couple(nn(hot.astype(bf16), got_ref[...].reshape(slots, RH * A)), couple_ref, out_ref)


TC_SHAPE = jax.ShapeDtypeStruct((RH // 2, T, 2 * A), bf16)


def select_call(sel, got, couplings):
    return pl.pallas_call(
        select_kernel,
        out_shape=TC_SHAPE,
        in_specs=[VMEM, VMEM, VMEM],
        out_specs=VMEM,
        name="select",
    )(sel, got, couplings)


def couple_kernel(picked_ref, couple_ref, out_ref):
    couple(picked_ref[...], couple_ref, out_ref)


def couple_call(picked, couplings):
    return pl.pallas_call(
        couple_kernel,
        out_shape=TC_SHAPE,
        in_specs=[VMEM, VMEM],
        out_specs=VMEM,
        name="couple",
    )(picked, couplings)


def near_kernel(leaves, scalar_ref, pts_ref, vec_ref, other_ref, left_ref, right_ref, out_ref, *bufs):
    vals, pts, kern0, kern1 = bufs
    count, n = scalar_ref[0], scalar_ref[1]
    own = pl.multiple_of(n * HALF, HALF)
    other = pl.multiple_of((1 - n) * HALF, HALF)
    vals[:T, :, pl.ds(own, HALF)] = vec_ref[...]
    vals[:T, :, pl.ds(other, HALF)] = other_ref[...]
    pts[:T] = pts_ref[...]
    for k, edge in enumerate((left_ref, right_ref)):
        vals[T + k] = edge[:R]
        pts[T + k] = edge[R : R + 3]

    def sources(t):
        return jnp.where(t == 0, T, t - 1), t, jnp.where(t == count - 1, T + 1, jnp.minimum(t + 1, T - 1))

    def fill(t, kern):
        x = pts[t, :, pl.ds(own, HALF)].astype(f32)
        x = jnp.concatenate([x, jnp.zeros((5, HALF), f32)], 0).T.astype(bf16)
        for k, u in enumerate(sources(t)):
            y = pts[u]
            for p in range(0, HALF, 32):
                squared = None
                for i in range(3):
                    differ = x[p : p + 32, i : i + 1] - y[i : i + 1, :]
                    differ = differ * differ
                    squared = differ + bf16(soften_sq) if squared is None else squared + differ
                kern[p : p + 32, k * LEAF : (k + 1) * LEAF] = lax.rsqrt(squared)

    def product(t, kern):
        values = jnp.concatenate([vals[u] for u in sources(t)], 1)
        out_ref[t - leaves[0]] = nt(values, kern[...]) * inverse_four_pi

    first, last = leaves
    fill(first, kern0)

    def body(i, _):
        t = first + 2 * i
        fill(t + 1, kern1)
        product(t, kern0)
        fill(jnp.minimum(t + 2, last - 1), kern0)
        product(t + 1, kern1)
        return 0

    lax.fori_loop(0, (last - first) // 2, body, 0)


def near_call(leaves, scalars, pts, vectors, other, left, right):
    size = leaves[1] - leaves[0]
    return pl.pallas_call(
        lambda *refs: near_kernel(leaves, *refs),
        out_shape=jax.ShapeDtypeStruct((size, R, HALF), f32),
        in_specs=[SMEM] + [VMEM] * 5,
        out_specs=VMEM,
        scratch_shapes=[
            pltpu.VMEM((T + 2, R, LEAF), bf16),
            pltpu.VMEM((T + 2, 3, LEAF), bf16),
            pltpu.VMEM((HALF, 3 * LEAF), bf16),
            pltpu.VMEM((HALF, 3 * LEAF), bf16),
        ],
        cost_estimate=pl.CostEstimate(
            flops=size * 200_000_000, bytes_accessed=2_000_000, transcendentals=0
        ),
        name="near",
    )(scalars, pts, vectors, other, left, right)


def final_kernel(scalar_ref, mine_ref, theirs_ref, tgt_ref, near0_ref, near1_ref, out_ref, rows):
    count, n = scalar_ref[0], scalar_ref[1]
    for ref, first in ((mine_ref, n * RH), (theirs_ref, (1 - n) * RH)):
        for r in range(RH):
            part = ref[r // 2].astype(f32)[:, (r % 2) * A : (r % 2 + 1) * A]
            rows[pl.ds(first + r, T, stride=R), :] = jnp.concatenate([part, part], 1)
    same = (iota((64, 256), 0) >> 4) == (iota((64, 256), 1) >> 6)
    for g in range(T // 4):
        part = rows[64 * g : 64 * g + 64, :]
        lhs = jnp.where(same, jnp.concatenate([part, part], 1), 0.0).astype(bf16)
        far = nn(lhs, tgt_ref[4 * g : 4 * g + 4].reshape(4 * A, HALF)).reshape(4, R, HALF)
        near = near0_ref if g < T // 8 else near1_ref
        first = 4 * g % (T // 2)
        total = far + near[first : first + 4]
        live = (iota((4, R, HALF), 0) + 4 * g) < count
        out_ref[4 * g : 4 * g + 4] = jnp.where(live, total, 0.0).astype(bf16)


def final_call(scalars, mine, theirs, tgt, near0, near1):
    whole = lambda *shape: pl.BlockSpec(shape, lambda i, s: (0,) * len(shape))
    return pl.pallas_call(
        final_kernel,
        out_shape=jax.ShapeDtypeStruct((T, R, HALF), bf16),
        grid_spec=pltpu.PrefetchScalarGridSpec(
            num_scalar_prefetch=1,
            grid=(1,),
            in_specs=[
                whole(RH // 2, T, 2 * A),
                whole(RH // 2, T, 2 * A),
                pl.BlockSpec((T, A, HALF), lambda i, s: (0, 0, s[1])),
                whole(T // 2, R, HALF),
                whole(T // 2, R, HALF),
            ],
            out_specs=whole(T, R, HALF),
            scratch_shapes=[pltpu.VMEM((T * R, 128), f32)],
        ),
        name="final",
    )(scalars, mine, theirs, tgt, near0, near1)


def shifted(array, axis, by):
    devices = lax.axis_size(axis)
    return lax.ppermute(array, axis, [(i, (i + by) % devices) for i in range(devices)])


def to_all(array, axis):
    copies = jnp.broadcast_to(array[None], (lax.axis_size(axis), *array.shape))
    return lax.all_to_all(copies, axis, split_axis=0, concat_axis=0, tiled=True)


def local(points, vectors, counts, src_basis, tgt_basis, adm_src, couplings):
    n = lax.axis_index("n").astype(i32)
    count = counts[0]
    scalars = jnp.stack([count, n])

    keep, send = coeff_call(n[None], vectors, src_basis)
    came = shifted(send, "n", 1)
    other = shifted(vectors, "n", 1)
    sel, req = index_call(counts, adm_src.T)
    asked = lax.all_to_all(req, PEERS, split_axis=0, concat_axis=0, tiled=True)

    coeffs = (keep + came).astype(bf16)
    table = to_all(coeffs, "z").reshape(COLUMN, RH * A)

    def edge(slot):
        halves = [lax.dynamic_index_in_dim(v, slot, 0, keepdims=False) for v in (vectors, other)]
        row = jnp.where(n == 0, jnp.concatenate(halves, 1), jnp.concatenate(halves[::-1], 1))
        pts = lax.dynamic_index_in_dim(points, slot, 0, keepdims=False)
        return jnp.concatenate([row, pts, jnp.zeros((5, LEAF), bf16)], 0)

    left = shifted(edge(count - 1), WIDE, 1)
    right = shifted(edge(0), WIDE, -1)
    near_args = (scalars, points, vectors, other, left, right)
    near0 = near_call((0, T // 2), *near_args)

    def some(table):
        got = lax.all_to_all(pack_call(asked, table), PEERS, split_axis=0, concat_axis=0, tiled=True)
        return select_call(sel, got, couplings), near_call((T // 2, T), *near_args)

    def every(table):
        whole = to_all(table, PEERS).reshape(N_PEER * COLUMN, RH * A)
        leaf = adm_src.T.reshape(ENTRIES)
        place = ((leaf >> 11) * 8 + ((leaf >> 5) & 7)) * COLUMN + ((leaf >> 8) & 7) * T + (leaf & (T - 1))
        hot = (place[:, None] == jnp.arange(N_PEER * COLUMN, dtype=i32)[None, :]).astype(bf16)
        picked = jnp.dot(hot, whole, preferred_element_type=f32)
        return couple_call(picked, couplings), near_call((T // 2, T), *near_args)

    mine, near1 = lax.cond(jnp.min(asked[:, 0, 0]) >= 0, some, every, table)
    theirs = shifted(mine, "n", 1)
    return final_call(scalars, mine, theirs, tgt_basis, near0, near1)


def solution(mesh):
    split = Mesh(
        mesh.devices.reshape(2, 8, 4, 2, mesh.shape["narrow"]), ("y", "z", "x", "c", "n")
    )
    in_specs = (
        P(WIDE, None, None),
        P(WIDE, None, "n"),
        P(WIDE),
        P(WIDE, None, "n"),
        P(WIDE, None, None),
        P(WIDE, None),
        P(WIDE, None, None),
    )
    out_specs = P(WIDE, None, "n")
    return jax.shard_map(local, mesh=split, in_specs=in_specs, out_specs=out_specs, check_vma=False)
```

```python
import math

import jax
import jax.numpy as jnp
from jax import lax
from jax.experimental import pallas as pl
from jax.experimental.pallas import tpu as pltpu
from jax.sharding import Mesh
from jax.sharding import PartitionSpec as P

WIDE = ("y", "z", "x", "c")
CHIPS = ("y", "z", "x")

inverse_four_pi = 1.0 / (4.0 * math.pi)
soften_sq = 0.0025

T, R, A, J, HALF, LEAF = 32, 16, 64, 8, 256, 512
QUARTER = R // 4
N_CHIP = 64
PAIR = 2 * T
CAP = 24
ENTRIES = PAIR * J
SLOTS = N_CHIP * CAP
ROW = QUARTER * A
bf16, f32, i32 = jnp.bfloat16, jnp.float32, jnp.int32

VMEM = pl.BlockSpec(memory_space=pltpu.VMEM)
SMEM = pl.BlockSpec(memory_space=pltpu.SMEM)


def nt(a, b):
    return lax.dot_general(a, b, (((1,), (1,)), ((), ())), preferred_element_type=f32)


def nn(a, b):
    return lax.dot_general(a, b, (((1,), (0,)), ((), ())), preferred_element_type=f32)


def iota(shape, dim):
    return lax.broadcasted_iota(i32, shape, dim)


def folded(wide):
    two = wide[:, :128] + wide[:, 128:]
    return two[:, :64] + two[:, 64:]


def index_kernel(own_ref, next_ref, sel_ref, req_ref):
    adm = jnp.concatenate([own_ref[...], next_ref[...]], 1).astype(f32)
    adm = jnp.concatenate([adm, jnp.zeros((J, 128 - PAIR), f32)], 1).T
    leaf = jnp.concatenate(
        [jnp.broadcast_to(adm[:PAIR, j : j + 1], (PAIR, 128)) for j in range(J)], 0
    ).astype(i32)
    live = leaf >= 0
    chip = leaf >> 6
    row = (leaf & (PAIR - 1)).astype(f32)
    lanes = iota((ENTRIES, 128), 1)
    member = jnp.where((chip == lanes) & live, 1.0, 0.0)
    below = jnp.where(iota((ENTRIES, ENTRIES), 0) > iota((ENTRIES, ENTRIES), 1), 1.0, 0.0)
    rank = nn(below.astype(bf16), member.astype(bf16))
    place = jnp.sum(member * rank, axis=1, keepdims=True)
    over = jnp.max(place) > CAP - 0.5
    place = jnp.broadcast_to(place, (ENTRIES, 128)).astype(i32)
    sel_ref[...] = jnp.where(live & (place < CAP), chip * CAP + place, -1)
    wanted = jnp.where(place == lanes, row + 1.0, 0.0)
    wanted = nn(member.T.astype(bf16), wanted.astype(bf16))[:N_CHIP]
    req_ref[...] = jnp.where(over, -1.0, wanted).reshape(N_CHIP, 1, 128)


def index_call(own, other):
    return pl.pallas_call(
        index_kernel,
        out_shape=(
            jax.ShapeDtypeStruct((ENTRIES, 128), i32),
            jax.ShapeDtypeStruct((N_CHIP, 1, 128), f32),
        ),
        in_specs=[VMEM, VMEM],
        out_specs=(VMEM, VMEM),
        name="requests",
    )(own, other)


def coeff_kernel(place_ref, vec_ref, basis_ref, keep_ref, c_ref, n_ref, nc_ref, rows):
    n, c = place_ref[0], place_ref[1]
    same = (iota((64, 256), 0) >> 4) == (iota((64, 256), 1) >> 6)
    for g in range(T // 4):
        lhs = vec_ref[4 * g : 4 * g + 4].reshape(64, HALF)
        rhs = basis_ref[4 * g : 4 * g + 4].reshape(4 * A, HALF)
        rows[64 * g : 64 * g + 64, :64] = folded(jnp.where(same, nt(lhs, rhs), 0.0))
    for out, to_n, to_c in (
        (c_ref, n, 1 - c),
        (n_ref, 1 - n, c),
        (nc_ref, 1 - n, 1 - c),
        (keep_ref, n, c),
    ):
        first = to_n * (R // 2) + to_c * QUARTER
        for r in range(0, QUARTER, 2):
            pair = [rows[pl.ds(first + r + k, T, stride=R), :][:, :64] for k in range(2)]
            out[:, r * A : (r + 2) * A] = jnp.concatenate(pair, 1)


def coeff_call(place, vectors, basis):
    shape = jax.ShapeDtypeStruct((T, ROW), f32)
    return pl.pallas_call(
        coeff_kernel,
        out_shape=(shape,) * 4,
        in_specs=[SMEM, VMEM, VMEM],
        out_specs=(VMEM,) * 4,
        scratch_shapes=[pltpu.VMEM((T * R, 128), f32)],
        name="coeffs",
    )(place, vectors, basis)


def pack_kernel(place_ref, req_ref, keep_ref, c_ref, n_ref, nc_ref, out_ref, table):
    c = place_ref[1]
    table[pl.ds(pl.multiple_of(c * T, T), T), :] = keep_ref[...] + n_ref[...]
    table[pl.ds(pl.multiple_of((1 - c) * T, T), T), :] = c_ref[...] + nc_ref[...]
    rows = table[...].astype(bf16)
    want = jnp.concatenate([req_ref[...].reshape(N_CHIP, 128), jnp.zeros((64, 128), f32)], 0).T
    lanes = iota((CAP, PAIR), 1).astype(f32) + 1.0
    for p in range(0, N_CHIP, 8):
        hot = [
            jnp.where(jnp.broadcast_to(want[:CAP, p + k : p + k + 1], (CAP, PAIR)) == lanes, 1.0, 0.0)
            for k in range(8)
        ]
        picked = nn(jnp.concatenate(hot, 0).astype(bf16), rows)
        out_ref[p : p + 8] = picked.astype(bf16).reshape(8, CAP, ROW)


def pack_call(place, req, keep, from_c, from_n, from_nc):
    return pl.pallas_call(
        pack_kernel,
        out_shape=jax.ShapeDtypeStruct((N_CHIP, CAP, ROW), bf16),
        in_specs=[SMEM] + [VMEM] * 5,
        out_specs=VMEM,
        scratch_shapes=[pltpu.VMEM((PAIR, ROW), f32)],
        name="pack",
    )(place, req, keep, from_c, from_n, from_nc)


def couple(picked, couple_refs, out_refs):
    lows = [picked[j * PAIR : (j + 1) * PAIR] for j in range(J)]
    by_rhs = []
    for r in range(QUARTER):
        cols = [low[:, r * A : (r + 1) * A] for low in lows]
        by_rhs.append(jnp.concatenate(cols, 1).astype(bf16))
    row_t = iota((16 * QUARTER, 256), 0) & 15
    col_t = iota((16 * QUARTER, 256), 1) >> 6
    for h in range(4):
        ref, out = couple_refs[h // 2], out_refs[h // 2]
        lhs = jnp.concatenate([s[16 * h : 16 * h + 16] for s in by_rhs], 0)
        low = 16 * (h % 2)
        total = jnp.zeros((16 * QUARTER, A), f32)
        for g in range(4):
            rhs = ref[low + 4 * g : low + 4 * g + 4].reshape(4 * A, J * A)
            total = total + folded(jnp.where(row_t == col_t + 4 * g, nt(lhs, rhs), 0.0))
        total = total.reshape(QUARTER, 16, A)
        for r in range(0, QUARTER, 2):
            pair = jnp.concatenate([total[r], total[r + 1]], 1)
            out[r // 2, low : low + 16, :] = pair.astype(bf16)


def select_kernel(sel_ref, got_ref, own_ref, next_ref, own_out, next_out):
    sel = sel_ref[...]
    lanes = iota((ENTRIES, 128), 1)
    hot = jnp.concatenate(
        [jnp.where(sel == lanes + 128 * k, 1.0, 0.0).astype(bf16) for k in range(SLOTS // 128)], 1
    )
    picked = nn(hot, got_ref[...].reshape(SLOTS, ROW))
    couple(picked, (own_ref, next_ref), (own_out, next_out))


def couple_kernel(picked_ref, own_ref, next_ref, own_out, next_out):
    couple(picked_ref[...], (own_ref, next_ref), (own_out, next_out))


TC_SHAPE = jax.ShapeDtypeStruct((QUARTER // 2, T, 2 * A), bf16)


def target_call(kernel, *args):
    return pl.pallas_call(
        kernel,
        out_shape=(TC_SHAPE, TC_SHAPE),
        in_specs=[VMEM] * len(args),
        out_specs=(VMEM, VMEM),
        name="targets",
    )(*args)


def near_kernel(leaves, scalar_ref, pts_ref, vec_ref, other_ref, left_ref, right_ref, out_ref, *bufs):
    vals, pts, *kerns = bufs
    count, n = scalar_ref[0], scalar_ref[1]
    own = pl.multiple_of(n * HALF, HALF)
    other = pl.multiple_of((1 - n) * HALF, HALF)
    vals[:T, :, pl.ds(own, HALF)] = vec_ref[...]
    vals[:T, :, pl.ds(other, HALF)] = other_ref[...]
    pts[:T] = pts_ref[...]
    for k, edge in enumerate((left_ref, right_ref)):
        vals[T + k] = edge[:R]
        pts[T + k] = edge[R : R + 3]

    def sources(t):
        return jnp.where(t == 0, T, t - 1), t, jnp.where(t == count - 1, T + 1, jnp.minimum(t + 1, T - 1))

    def fill(t, kern):
        x = pts[t, :, pl.ds(own, HALF)].astype(f32)
        x = jnp.concatenate([x, jnp.zeros((5, HALF), f32)], 0).T.astype(bf16)
        for k, u in enumerate(sources(t)):
            y = pts[u]
            for p in range(0, HALF, 32):
                squared = None
                for i in range(3):
                    differ = x[p : p + 32, i : i + 1] - y[i : i + 1, :]
                    differ = differ * differ
                    squared = differ + bf16(soften_sq) if squared is None else squared + differ
                kern[p : p + 32, k * LEAF : (k + 1) * LEAF] = lax.rsqrt(squared)

    def product(t, kern):
        values = jnp.concatenate([vals[u] for u in sources(t)], 1)
        out_ref[t - leaves[0]] = nt(values, kern[...]) * inverse_four_pi

    first, last = leaves
    fill(first, kerns[0])

    def body(i, _):
        for s in range(4):
            t = first + 4 * i + s
            fill(jnp.minimum(t + 1, last - 1), kerns[(s + 1) % 4])
            product(t, kerns[s])
        return 0

    lax.fori_loop(0, (last - first) // 4, body, 0)


def near_call(leaves, scalars, pts, vectors, other, left, right):
    size = leaves[1] - leaves[0]
    return pl.pallas_call(
        lambda *refs: near_kernel(leaves, *refs),
        out_shape=jax.ShapeDtypeStruct((size, R, HALF), f32),
        in_specs=[SMEM] + [VMEM] * 5,
        out_specs=VMEM,
        scratch_shapes=[
            pltpu.VMEM((T + 2, R, LEAF), bf16),
            pltpu.VMEM((T + 2, 3, LEAF), bf16),
        ]
        + [pltpu.VMEM((HALF, 3 * LEAF), bf16)] * 4,
        cost_estimate=pl.CostEstimate(
            flops=size * 200_000_000, bytes_accessed=2_000_000, transcendentals=0
        ),
        name="near",
    )(scalars, pts, vectors, other, left, right)


def final_kernel(scalar_ref, own_ref, c_ref, n_ref, nc_ref, tgt_ref, near_ref, out_ref, rows):
    count, n, c = scalar_ref[0], scalar_ref[1], scalar_ref[2]
    for ref, from_n, from_c in (
        (own_ref, n, c),
        (c_ref, n, 1 - c),
        (n_ref, 1 - n, c),
        (nc_ref, 1 - n, 1 - c),
    ):
        first = from_n * (R // 2) + from_c * QUARTER
        for r in range(QUARTER):
            part = ref[r // 2].astype(f32)[:, (r % 2) * A : (r % 2 + 1) * A]
            rows[pl.ds(first + r, T, stride=R), :] = jnp.concatenate([part, part], 1)
    same = (iota((64, 256), 0) >> 4) == (iota((64, 256), 1) >> 6)
    for g in range(T // 4):
        part = rows[64 * g : 64 * g + 64, :]
        lhs = jnp.where(same, jnp.concatenate([part, part], 1), 0.0).astype(bf16)
        far = nn(lhs, tgt_ref[4 * g : 4 * g + 4].reshape(4 * A, HALF)).reshape(4, R, HALF)
        total = far + near_ref[4 * g : 4 * g + 4]
        live = (iota((4, R, HALF), 0) + 4 * g) < count
        out_ref[4 * g : 4 * g + 4] = jnp.where(live, total, 0.0).astype(bf16)


def final_call(scalars, parts, tgt, near):
    whole = lambda *shape: pl.BlockSpec(shape, lambda i, s: (0,) * len(shape))
    return pl.pallas_call(
        final_kernel,
        out_shape=jax.ShapeDtypeStruct((T, R, HALF), bf16),
        grid_spec=pltpu.PrefetchScalarGridSpec(
            num_scalar_prefetch=1,
            grid=(1,),
            in_specs=[whole(QUARTER // 2, T, 2 * A)] * 4
            + [pl.BlockSpec((T, A, HALF), lambda i, s: (0, 0, s[1])), whole(T, R, HALF)],
            out_specs=whole(T, R, HALF),
            scratch_shapes=[pltpu.VMEM((T * R, 128), f32)],
        ),
        name="final",
    )(scalars, *parts, tgt, near)


def shifted(array, axis, by):
    devices = lax.axis_size(axis)
    return lax.ppermute(array, axis, [(i, (i + by) % devices) for i in range(devices)])


def crossed(array):
    return lax.ppermute(array, ("c", "n"), [(i, 3 - i) for i in range(4)])


def after(first, *arrays):
    return lax.optimization_barrier((first, *arrays))[1:]


def local(points, vectors, counts, src_basis, tgt_basis, adm_src, couplings):
    n = lax.axis_index("n").astype(i32)
    c = lax.axis_index("c").astype(i32)
    count = counts[0]
    scalars = jnp.stack([count, n, c])
    place = jnp.stack([n, c])

    live = jnp.arange(T, dtype=i32)[None, :] < count
    own_adm = jnp.where(live, adm_src.T, -1)
    next_adm = shifted(own_adm, "c", 1)

    keep, to_c, to_n, to_nc = coeff_call(place, vectors, src_basis)
    from_n = shifted(to_n, "n", 1)
    from_nc = crossed(to_nc)
    from_c = shifted(to_c, "c", 1)
    (next_adm,) = after(keep, next_adm)
    sel, req = index_call(own_adm, next_adm)
    asked = lax.all_to_all(req, CHIPS, split_axis=0, concat_axis=0, tiled=True)
    next_couplings = shifted(couplings, "c", 1)
    (sent_vectors,) = after(keep, vectors)
    other = shifted(sent_vectors, "n", 1)

    def edge(slot):
        halves = [lax.dynamic_index_in_dim(v, slot, 0, keepdims=False) for v in (vectors, other)]
        row = jnp.where(n == 0, jnp.concatenate(halves, 1), jnp.concatenate(halves[::-1], 1))
        pts = lax.dynamic_index_in_dim(points, slot, 0, keepdims=False)
        return jnp.concatenate([row, pts, jnp.zeros((5, LEAF), bf16)], 0)

    left = shifted(edge(count - 1), WIDE, 1)
    right = shifted(edge(0), WIDE, -1)
    near_args = (scalars, points, vectors, other, left, right)
    coefs = (keep, from_c, from_n, from_nc)

    def some(coefs):
        got = lax.all_to_all(
            pack_call(place, asked, *coefs), CHIPS, split_axis=0, concat_axis=0, tiled=True
        )
        return target_call(select_kernel, sel, got, couplings, next_couplings), near_call((0, T), *near_args)

    def every(coefs):
        own, other_core = coefs[0] + coefs[2], coefs[1] + coefs[3]
        pair = (own, other_core), (other_core, own)
        table = jnp.where(c == 0, jnp.concatenate(pair[0]), jnp.concatenate(pair[1])).astype(bf16)
        copies = jnp.broadcast_to(table[None], (N_CHIP, PAIR, ROW))
        whole = lax.all_to_all(copies, CHIPS, split_axis=0, concat_axis=0, tiled=True)
        leaf = jnp.concatenate([own_adm, next_adm], 1).reshape(ENTRIES)
        hot = (leaf[:, None] == jnp.arange(N_CHIP * PAIR, dtype=i32)[None, :]).astype(bf16)
        picked = jnp.dot(hot, whole.reshape(N_CHIP * PAIR, ROW), preferred_element_type=f32)
        return target_call(couple_kernel, picked, couplings, next_couplings), near_call((0, T), *near_args)

    (mine, nexts), near = lax.cond(jnp.min(asked[:, 0, 0]) >= 0, some, every, coefs)
    parts = mine, shifted(nexts, "c", 1), shifted(mine, "n", 1), crossed(nexts)
    return final_call(scalars, parts, tgt_basis, near)


def solution(mesh):
    split = Mesh(
        mesh.devices.reshape(2, 8, 4, 2, mesh.shape["narrow"]), ("y", "z", "x", "c", "n")
    )
    in_specs = (
        P(WIDE, None, None),
        P(WIDE, None, "n"),
        P(WIDE),
        P(WIDE, None, "n"),
        P(WIDE, None, None),
        P(WIDE, None),
        P(WIDE, None, None),
    )
    out_specs = P(WIDE, None, "n")
    return jax.shard_map(local, mesh=split, in_specs=in_specs, out_specs=out_specs, check_vma=False)
```

```python
import math

import jax
import jax.numpy as jnp
from jax import lax
from jax.experimental import pallas as pl
from jax.experimental.pallas import tpu as pltpu
from jax.sharding import Mesh
from jax.sharding import PartitionSpec as P


WIDE = ("y", "z", "x", "c")
PEERS = ("y", "x", "c")

inverse_four_pi = 1.0 / (4.0 * math.pi)
soften_sq = 0.0025

T, R, A, J, HALF, LEAF = 32, 16, 64, 8, 256, 512
RH = R // 2
N_Z, N_PEER = 8, 16
CAP = 48
CUT = 24
ENTRIES = T * J
COLUMN = N_Z * T
bf16, f32, i32 = jnp.bfloat16, jnp.float32, jnp.int32

VMEM = pl.BlockSpec(memory_space=pltpu.VMEM)
SMEM = pl.BlockSpec(memory_space=pltpu.SMEM)
LIMIT = pltpu.CompilerParams(vmem_limit_bytes=20 * 2**20)


def nt(a, b):
    return lax.dot_general(a, b, (((1,), (1,)), ((), ())), preferred_element_type=f32)


def nn(a, b):
    return lax.dot_general(a, b, (((1,), (0,)), ((), ())), preferred_element_type=f32)


def iota(shape, dim):
    return lax.broadcasted_iota(i32, shape, dim)


def folded(wide):
    two = wide[:, :128] + wide[:, 128:]
    return two[:, :64] + two[:, 64:]


def index_kernel(count_ref, adm_ref, pts_ref, sel_ref, req_ref, rows_ref):
    pts = pts_ref[...].astype(f32)
    blank = jnp.zeros((5, LEAF), f32)
    for t in range(T):
        rows_ref[t] = jnp.concatenate([pts[i, t : t + 1] for i in range(3)] + [blank], 0).astype(bf16)
    count = count_ref[0]
    adm = jnp.concatenate([adm_ref[...].astype(f32), jnp.zeros((8, 96), f32)], 1).T
    leaf = jnp.concatenate(
        [jnp.broadcast_to(adm[:T, j : j + 1], (T, 128)) for j in range(J)], 0
    ).astype(i32)
    live = (iota((ENTRIES, 128), 0) & (T - 1)) < count
    column = (leaf >> 11) * 8 + ((leaf >> 5) & 7)
    row = ((leaf >> 8) & 7) * T + (leaf & (T - 1))
    member = jnp.where((column == iota((ENTRIES, 128), 1)) & live, 1.0, 0.0)
    below = jnp.where(iota((ENTRIES, ENTRIES), 0) > iota((ENTRIES, ENTRIES), 1), 1.0, 0.0)
    rank = nn(below.astype(bf16), member.astype(bf16))
    place = jnp.sum(member * rank, axis=1, keepdims=True)
    over = jnp.max(place) > CAP - 0.5
    place = jnp.broadcast_to(place, (ENTRIES, 128))
    fits = live & (place < CAP - 0.5)
    sel = jnp.where(fits, column * CAP + place.astype(i32), -1)
    sel_ref[...] = sel
    sel_row = sel.astype(f32).T[:1]
    slots = N_PEER * CAP
    pick = jnp.where(iota((slots, ENTRIES), 0) == sel_row.astype(i32), 1.0, 0.0).astype(bf16)
    wanted = nn(pick, (row + 1).astype(f32).astype(bf16))
    wanted = jnp.where(over, -1.0, wanted)
    req_ref[...] = wanted.astype(bf16).reshape(N_PEER, CAP, 128)


def index_call(counts, adm, points):
    return pl.pallas_call(
        index_kernel,
        out_shape=(
            jax.ShapeDtypeStruct((ENTRIES, 128), i32),
            jax.ShapeDtypeStruct((N_PEER, CAP, 128), bf16),
            jax.ShapeDtypeStruct((T, 8, LEAF), bf16),
        ),
        in_specs=[SMEM, VMEM, VMEM],
        out_specs=(VMEM, VMEM, VMEM),
        name="requests",
        compiler_params=LIMIT,
    )(counts, adm, points)


def coeff_kernel(n_ref, vec_ref, basis_ref, keep_ref, send_ref, rows):
    n = n_ref[0]
    same = (iota((64, 256), 0) >> 4) == (iota((64, 256), 1) >> 6)
    for g in range(T // 4):
        lhs = vec_ref[4 * g : 4 * g + 4].reshape(64, HALF)
        rhs = basis_ref[4 * g : 4 * g + 4].reshape(4 * A, HALF)
        rows[64 * g : 64 * g + 64, :64] = folded(jnp.where(same, nt(lhs, rhs), 0.0))
    for out, first in ((send_ref, (1 - n) * RH), (keep_ref, n * RH)):
        for r in range(0, RH, 2):
            pair = [rows[pl.ds(first + r + k, T, stride=R), :][:, :64] for k in range(2)]
            out[:, r * A : (r + 2) * A] = jnp.concatenate(pair, 1)


def coeff_call(n, vectors, basis):
    shape = jax.ShapeDtypeStruct((T, RH * A), f32)
    return pl.pallas_call(
        coeff_kernel,
        out_shape=(shape, shape),
        in_specs=[SMEM, VMEM, VMEM],
        out_specs=(VMEM, VMEM),
        scratch_shapes=[pltpu.VMEM((T * R, 128), f32)],
        name="coeffs",
        compiler_params=LIMIT,
    )(n, vectors, basis)


def pack_kernel(req_ref, table_ref, out_ref):
    lanes = iota((CAP, 128), 1).astype(f32) + 1.0
    for r in range(0, N_PEER, 4):
        want = [req_ref[r + k].astype(f32) for k in range(4)]
        hot = [
            jnp.concatenate(
                [jnp.where(w == lanes, 1.0, 0.0), jnp.where(w == lanes + 128.0, 1.0, 0.0)], 1
            )
            for w in want
        ]
        picked = nn(jnp.concatenate(hot, 0).astype(bf16), table_ref[...])
        out_ref[r : r + 4] = picked.astype(bf16).reshape(4, CAP, RH * A)


def pack_call(req, table):
    return pl.pallas_call(
        pack_kernel,
        out_shape=jax.ShapeDtypeStruct((N_PEER, CAP, RH * A), bf16),
        in_specs=[VMEM, VMEM],
        out_specs=VMEM,
        name="pack",
        compiler_params=LIMIT,
    )(req, table)


def couple(picked, couple_ref, out_ref):
    lows = [picked[j * T : (j + 1) * T] for j in range(J)]
    by_rhs = []
    for r in range(RH):
        cols = [low[:, r * A : (r + 1) * A] for low in lows]
        by_rhs.append(jnp.concatenate(cols, 1).astype(bf16))
    row_t = iota((16 * RH, 256), 0) & 15
    col_t = iota((16 * RH, 256), 1) >> 6
    for h in range(2):
        lhs = jnp.concatenate([s[16 * h : 16 * h + 16] for s in by_rhs], 0)
        total = jnp.zeros((16 * RH, A), f32)
        for g in range(4):
            first = 16 * h + 4 * g
            rhs = couple_ref[first : first + 4].reshape(4 * A, J * A)
            total = total + folded(jnp.where(row_t == col_t + 4 * g, nt(lhs, rhs), 0.0))
        total = total.reshape(RH, 16, A)
        for r in range(0, RH, 2):
            pair = jnp.concatenate([total[r], total[r + 1]], 1)
            out_ref[r // 2, 16 * h : 16 * h + 16, :] = pair.astype(bf16)


def select_kernel(sel_ref, got_ref, couple_ref, out_ref):
    slots = N_PEER * CAP
    sel = sel_ref[...]
    lanes = iota((ENTRIES, 128), 1)
    hot = jnp.concatenate(
        [jnp.where(sel == lanes + 128 * k, 1.0, 0.0) for k in range(slots // 128)], 1
    )
    couple(nn(hot.astype(bf16), got_ref[...].reshape(slots, RH * A)), couple_ref, out_ref)


TC_SHAPE = jax.ShapeDtypeStruct((RH // 2, T, 2 * A), bf16)


def select_call(sel, got, couplings):
    return pl.pallas_call(
        select_kernel,
        out_shape=TC_SHAPE,
        in_specs=[VMEM, VMEM, VMEM],
        out_specs=VMEM,
        name="select",
        compiler_params=LIMIT,
    )(sel, got, couplings)


def couple_kernel(picked_ref, couple_ref, out_ref):
    couple(picked_ref[...], couple_ref, out_ref)


def couple_call(picked, couplings):
    return pl.pallas_call(
        couple_kernel,
        out_shape=TC_SHAPE,
        in_specs=[VMEM, VMEM],
        out_specs=VMEM,
        name="couple",
        compiler_params=LIMIT,
    )(picked, couplings)


def near_kernel(leaves, scalar_ref, pts_ref, vec_ref, other_ref, left_ref, right_ref, out_ref, *bufs):
    vals, pts, *kerns = bufs
    count, n = scalar_ref[0], scalar_ref[1]
    own = pl.multiple_of(n * HALF, HALF)
    other = pl.multiple_of((1 - n) * HALF, HALF)
    vals[:T, :, pl.ds(own, HALF)] = vec_ref[...]
    vals[:T, :, pl.ds(other, HALF)] = other_ref[...]
    pts[:T] = pts_ref[...]
    for k, edge in enumerate((left_ref, right_ref)):
        vals[T + k] = edge[:R]
        pts[T + k] = edge[R : R + 8]

    def sources(t):
        return jnp.where(t == 0, T, t - 1), t, jnp.where(t == count - 1, T + 1, jnp.minimum(t + 1, T - 1))

    def fill(t, kern):
        x = pts[t, :, pl.ds(own, HALF)].astype(f32)
        x = x.T.astype(bf16)
        for k, u in enumerate(sources(t)):
            y = pts[u]
            for p in range(0, HALF, 32):
                squared = None
                for i in range(3):
                    differ = x[p : p + 32, i : i + 1] - y[i : i + 1, :]
                    differ = differ * differ
                    squared = differ + bf16(soften_sq) if squared is None else squared + differ
                kern[p : p + 32, k * LEAF : (k + 1) * LEAF] = lax.rsqrt(squared)

    def product(t, kern):
        values = jnp.concatenate([vals[u] for u in sources(t)], 1)
        out_ref[t - leaves[0]] = nt(values, kern[...]) * inverse_four_pi

    first, last = leaves
    fill(first, kerns[0])

    def body(i, _):
        for s in range(4):
            t = first + 4 * i + s
            fill(jnp.minimum(t + 1, last - 1), kerns[(s + 1) % 4])
            product(t, kerns[s])
        return 0

    lax.fori_loop(0, (last - first) // 4, body, 0)


def near_call(leaves, scalars, pts, vectors, other, left, right):
    size = leaves[1] - leaves[0]
    return pl.pallas_call(
        lambda *refs: near_kernel(leaves, *refs),
        out_shape=jax.ShapeDtypeStruct((size, R, HALF), f32),
        in_specs=[SMEM] + [VMEM] * 5,
        out_specs=VMEM,
        scratch_shapes=[
            pltpu.VMEM((T + 2, R, LEAF), bf16),
            pltpu.VMEM((T + 2, 8, LEAF), bf16),
        ]
        + [pltpu.VMEM((HALF, 3 * LEAF), bf16)] * 4,
        cost_estimate=pl.CostEstimate(
            flops=size * 200_000_000, bytes_accessed=2_000_000, transcendentals=0
        ),
        name="near",
        compiler_params=LIMIT,
    )(scalars, pts, vectors, other, left, right)


def final_kernel(scalar_ref, mine_ref, theirs_ref, tgt_ref, near0_ref, near1_ref, out_ref, rows):
    count, n = scalar_ref[0], scalar_ref[1]
    for ref, first in ((mine_ref, n * RH), (theirs_ref, (1 - n) * RH)):
        for r in range(RH):
            part = ref[r // 2].astype(f32)[:, (r % 2) * A : (r % 2 + 1) * A]
            rows[pl.ds(first + r, T, stride=R), :] = jnp.concatenate([part, part], 1)
    same = (iota((64, 256), 0) >> 4) == (iota((64, 256), 1) >> 6)
    for g in range(T // 4):
        part = rows[64 * g : 64 * g + 64, :]
        lhs = jnp.where(same, jnp.concatenate([part, part], 1), 0.0).astype(bf16)
        tgt = tgt_ref[4 * g : 4 * g + 4, :, pl.ds(pl.multiple_of(n * HALF, HALF), HALF)]
        far = nn(lhs, tgt.reshape(4 * A, HALF)).reshape(4, R, HALF)
        near, first = (near0_ref, 4 * g) if 4 * g < CUT else (near1_ref, 4 * g - CUT)
        total = far + near[first : first + 4]
        live = (iota((4, R, HALF), 0) + 4 * g) < count
        out_ref[4 * g : 4 * g + 4] = jnp.where(live, total, 0.0).astype(bf16)


def final_call(scalars, mine, theirs, tgt, near0, near1):
    return pl.pallas_call(
        final_kernel,
        out_shape=jax.ShapeDtypeStruct((T, R, HALF), bf16),
        in_specs=[SMEM] + [VMEM] * 5,
        out_specs=VMEM,
        scratch_shapes=[pltpu.VMEM((T * R, 128), f32)],
        name="final",
        compiler_params=LIMIT,
    )(scalars, mine, theirs, tgt, near0, near1)


def shifted(array, axis, by):
    devices = lax.axis_size(axis)
    return lax.ppermute(array, axis, [(i, (i + by) % devices) for i in range(devices)])


def to_all(array, axis):
    copies = jnp.broadcast_to(array[None], (lax.axis_size(axis), *array.shape))
    return lax.all_to_all(copies, axis, split_axis=0, concat_axis=0, tiled=True)


def body(points, vectors, counts, src_basis, tgt_basis, adm_src, couplings):
    n = lax.axis_index("n").astype(i32)
    count = counts[0]
    scalars = jnp.stack([count, n])

    keep, send = coeff_call(n[None], vectors, src_basis)
    came = shifted(send, "n", 1)
    other = shifted(vectors, "n", 1)
    sel, req, rows = index_call(counts, adm_src.T, points.transpose(1, 0, 2))
    asked = lax.all_to_all(req, PEERS, split_axis=0, concat_axis=0, tiled=True)

    coeffs = (keep + came).astype(bf16)
    table = to_all(coeffs, "z").reshape(COLUMN, RH * A)

    def edge(slot):
        halves = [lax.dynamic_index_in_dim(v, slot, 0, keepdims=False) for v in (vectors, other)]
        row = jnp.where(n == 0, jnp.concatenate(halves, 1), jnp.concatenate(halves[::-1], 1))
        return jnp.concatenate([row, lax.dynamic_index_in_dim(rows, slot, 0, keepdims=False)], 0)

    last, first = edge(count - 1), edge(0)
    left = shifted(last, WIDE, 1)
    right = shifted(first, WIDE, -1)
    near_args = (scalars, rows, vectors, other, left, right)
    near1 = near_call((CUT, T), *near_args)

    def some(table):
        got = lax.all_to_all(pack_call(asked, table), PEERS, split_axis=0, concat_axis=0, tiled=True)
        return select_call(sel, got, couplings), near_call((0, CUT), *near_args)

    def every(table):
        whole = to_all(table, PEERS).reshape(N_PEER * COLUMN, RH * A)
        leaf = adm_src.T.reshape(ENTRIES)
        place = ((leaf >> 11) * 8 + ((leaf >> 5) & 7)) * COLUMN + ((leaf >> 8) & 7) * T + (leaf & (T - 1))
        hot = (place[:, None] == jnp.arange(N_PEER * COLUMN, dtype=i32)[None, :]).astype(bf16)
        picked = jnp.dot(hot, whole, preferred_element_type=f32)
        return couple_call(picked, couplings), near_call((0, CUT), *near_args)

    mine, near0 = lax.cond(jnp.min(asked[:, 0, 0]) >= 0, some, every, table)
    theirs = shifted(mine, "n", 1)
    return final_call(scalars, mine, theirs, tgt_basis, near0, near1)


def solution(mesh):
    split = Mesh(
        mesh.devices.reshape(2, 8, 4, 2, mesh.shape["narrow"]), ("y", "z", "x", "c", "n")
    )
    in_specs = (
        P(WIDE, None, None),
        P(WIDE, None, "n"),
        P(WIDE),
        P(WIDE, None, "n"),
        P(WIDE, None, None),
        P(WIDE, None),
        P(WIDE, None, None),
    )
    out_specs = P(WIDE, None, "n")
    return jax.shard_map(body, mesh=split, in_specs=in_specs, out_specs=out_specs, check_vma=False)
```

```python
import math

import jax
import jax.numpy as jnp
from jax import lax
from jax.experimental import pallas as pl
from jax.experimental.pallas import tpu as pltpu
from jax.sharding import Mesh
from jax.sharding import PartitionSpec as P


WIDE = ("y", "z", "x", "c")
PEERS = ("y", "x", "c")

inverse_four_pi = 1.0 / (4.0 * math.pi)
soften_sq = 0.0025

T, R, A, J, HALF, LEAF = 32, 16, 64, 8, 256, 512
RH = R // 2
N_Z, N_PEER = 8, 16
CAP = 48
ENTRIES = T * J
OFFSETS = (0,), (2,), (-2,), (4,), (1, 3), (-1, -3)
COLUMN = N_Z * T
bf16, f32, i32 = jnp.bfloat16, jnp.float32, jnp.int32

VMEM = pl.BlockSpec(memory_space=pltpu.VMEM)
SMEM = pl.BlockSpec(memory_space=pltpu.SMEM)
LIMIT = pltpu.CompilerParams(vmem_limit_bytes=20 * 2**20)


def nt(a, b):
    return lax.dot_general(a, b, (((1,), (1,)), ((), ())), preferred_element_type=f32)


def nn(a, b):
    return lax.dot_general(a, b, (((1,), (0,)), ((), ())), preferred_element_type=f32)


def iota(shape, dim):
    return lax.broadcasted_iota(i32, shape, dim)


def folded(wide):
    two = wide[:, :128] + wide[:, 128:]
    return two[:, :64] + two[:, 64:]


def index_kernel(scalar_ref, adm_ref, pts_ref, vec_ref, sel_ref, req_ref, rows_ref, first_ref, last_ref):
    pts = pts_ref[...].astype(f32)
    blank = jnp.zeros((5, LEAF), f32)
    for t in range(T):
        rows_ref[t] = jnp.concatenate([pts[i, t : t + 1] for i in range(3)] + [blank], 0).astype(bf16)
    count, own = scalar_ref[0], pl.multiple_of(scalar_ref[1] * HALF, HALF)
    for ref, t in ((first_ref, 0), (last_ref, count - 1)):
        ref[:R] = vec_ref[t]
        ref[R:] = rows_ref[t, :, pl.ds(own, HALF)]
    adm = jnp.concatenate([adm_ref[...].astype(f32), jnp.zeros((8, 96), f32)], 1).T
    leaf = jnp.concatenate(
        [jnp.broadcast_to(adm[:T, j : j + 1], (T, 128)) for j in range(J)], 0
    ).astype(i32)
    live = (iota((ENTRIES, 128), 0) & (T - 1)) < count
    column = (leaf >> 11) * 8 + ((leaf >> 5) & 7)
    row = ((leaf >> 8) & 7) * T + (leaf & (T - 1))
    member = jnp.where((column == iota((ENTRIES, 128), 1)) & live, 1.0, 0.0)
    below = jnp.where(iota((ENTRIES, ENTRIES), 0) > iota((ENTRIES, ENTRIES), 1), 1.0, 0.0)
    rank = nn(below.astype(bf16), member.astype(bf16))
    place = jnp.sum(member * rank, axis=1, keepdims=True)
    over = jnp.max(place) > CAP - 0.5
    place = jnp.broadcast_to(place, (ENTRIES, 128))
    fits = live & (place < CAP - 0.5)
    sel = jnp.where(fits, column * CAP + place.astype(i32), -1)
    sel_ref[...] = sel
    sel_row = sel.astype(f32).T[:1]
    slots = N_PEER * CAP
    pick = jnp.where(iota((slots, ENTRIES), 0) == sel_row.astype(i32), 1.0, 0.0).astype(bf16)
    wanted = nn(pick, (row + 1).astype(f32).astype(bf16))
    wanted = jnp.where(over, -1.0, wanted)
    req_ref[...] = wanted.astype(bf16).reshape(N_PEER, CAP, 128)


EDGE_SHAPE = jax.ShapeDtypeStruct((R + 8, HALF), bf16)


def index_call(scalars, adm, points, vectors):
    return pl.pallas_call(
        index_kernel,
        out_shape=(
            jax.ShapeDtypeStruct((ENTRIES, 128), i32),
            jax.ShapeDtypeStruct((N_PEER, CAP, 128), bf16),
            jax.ShapeDtypeStruct((T, 8, LEAF), bf16),
            EDGE_SHAPE,
            EDGE_SHAPE,
        ),
        in_specs=[SMEM, VMEM, VMEM, VMEM],
        out_specs=(VMEM,) * 5,
        name="requests",
        compiler_params=LIMIT,
    )(scalars, adm, points, vectors)


def coeff_kernel(n_ref, vec_ref, basis_ref, keep_ref, send_ref, rows):
    n = n_ref[0]
    same = (iota((64, 256), 0) >> 4) == (iota((64, 256), 1) >> 6)
    for g in range(T // 4):
        lhs = vec_ref[4 * g : 4 * g + 4].reshape(64, HALF)
        rhs = basis_ref[4 * g : 4 * g + 4].reshape(4 * A, HALF)
        rows[64 * g : 64 * g + 64, :64] = folded(jnp.where(same, nt(lhs, rhs), 0.0))
    for out, first in ((send_ref, (1 - n) * RH), (keep_ref, n * RH)):
        for r in range(0, RH, 2):
            pair = [rows[pl.ds(first + r + k, T, stride=R), :][:, :64] for k in range(2)]
            out[:, r * A : (r + 2) * A] = jnp.concatenate(pair, 1)


def coeff_call(n, vectors, basis):
    shape = jax.ShapeDtypeStruct((T, RH * A), f32)
    return pl.pallas_call(
        coeff_kernel,
        out_shape=(shape, shape),
        in_specs=[SMEM, VMEM, VMEM],
        out_specs=(VMEM, VMEM),
        scratch_shapes=[pltpu.VMEM((T * R, 128), f32)],
        name="coeffs",
        compiler_params=LIMIT,
    )(n, vectors, basis)


def pack_kernel(z_ref, req_ref, *refs):
    *pieces, out_ref, table_ref = refs
    for piece, offsets in zip(pieces, OFFSETS):
        for k, offset in enumerate(offsets):
            first = pl.multiple_of(((z_ref[0] + offset) & (N_Z - 1)) * T, T)
            table_ref[pl.ds(first, T), :] = piece[k * T : (k + 1) * T]
    lanes = iota((CAP, 128), 1).astype(f32) + 1.0
    for r in range(0, N_PEER, 4):
        want = [req_ref[r + k].astype(f32) for k in range(4)]
        hot = [
            jnp.concatenate(
                [jnp.where(w == lanes, 1.0, 0.0), jnp.where(w == lanes + 128.0, 1.0, 0.0)], 1
            )
            for w in want
        ]
        picked = nn(jnp.concatenate(hot, 0).astype(bf16), table_ref[...])
        out_ref[r : r + 4] = picked.astype(bf16).reshape(4, CAP, RH * A)


def pack_call(z, req, pieces):
    return pl.pallas_call(
        pack_kernel,
        out_shape=jax.ShapeDtypeStruct((N_PEER, CAP, RH * A), bf16),
        in_specs=[SMEM] + [VMEM] * (1 + len(pieces)),
        out_specs=VMEM,
        scratch_shapes=[pltpu.VMEM((COLUMN, RH * A), bf16)],
        name="pack",
        compiler_params=LIMIT,
    )(z, req, *pieces)


def couple(picked, couple_ref, out_ref):
    lows = [picked[j * T : (j + 1) * T] for j in range(J)]
    by_rhs = []
    for r in range(RH):
        cols = [low[:, r * A : (r + 1) * A] for low in lows]
        by_rhs.append(jnp.concatenate(cols, 1).astype(bf16))
    row_t = iota((16 * RH, 256), 0) & 15
    col_t = iota((16 * RH, 256), 1) >> 6
    for h in range(2):
        lhs = jnp.concatenate([s[16 * h : 16 * h + 16] for s in by_rhs], 0)
        total = jnp.zeros((16 * RH, A), f32)
        for g in range(4):
            first = 16 * h + 4 * g
            rhs = couple_ref[first : first + 4].reshape(4 * A, J * A)
            total = total + folded(jnp.where(row_t == col_t + 4 * g, nt(lhs, rhs), 0.0))
        total = total.reshape(RH, 16, A)
        for r in range(0, RH, 2):
            pair = jnp.concatenate([total[r], total[r + 1]], 1)
            out_ref[r // 2, 16 * h : 16 * h + 16, :] = pair.astype(bf16)


def select_kernel(sel_ref, got_ref, couple_ref, out_ref):
    slots = N_PEER * CAP
    sel = sel_ref[...]
    lanes = iota((ENTRIES, 128), 1)
    hot = jnp.concatenate(
        [jnp.where(sel == lanes + 128 * k, 1.0, 0.0) for k in range(slots // 128)], 1
    )
    couple(nn(hot.astype(bf16), got_ref[...].reshape(slots, RH * A)), couple_ref, out_ref)


TC_SHAPE = jax.ShapeDtypeStruct((RH // 2, T, 2 * A), bf16)


def select_call(sel, got, couplings):
    return pl.pallas_call(
        select_kernel,
        out_shape=TC_SHAPE,
        in_specs=[VMEM, VMEM, VMEM],
        out_specs=VMEM,
        name="select",
        compiler_params=LIMIT,
    )(sel, got, couplings)


def couple_kernel(picked_ref, couple_ref, out_ref):
    couple(picked_ref[...], couple_ref, out_ref)


def couple_call(picked, couplings):
    return pl.pallas_call(
        couple_kernel,
        out_shape=TC_SHAPE,
        in_specs=[VMEM, VMEM],
        out_specs=VMEM,
        name="couple",
        compiler_params=LIMIT,
    )(picked, couplings)


def near_kernel(leaves, edges, scalar_ref, pts_ref, vec_ref, other_ref, *refs):
    edge_refs, out_ref, kerns = refs[: 4 * edges], refs[-5], refs[-4:]
    count, n = scalar_ref[0], scalar_ref[1]
    own = pl.multiple_of(n * HALF, HALF)
    other = pl.multiple_of((1 - n) * HALF, HALF)

    def sources(t):
        return (t + T - 1) & (T - 1), t, (t + 1) & (T - 1)

    def taken(t, rows, values):
        if not edges:
            return values
        for k, (u, at) in enumerate(((0, 0), (2, count - 1))):
            halo = [edge_refs[2 * k + h][rows] for h in range(2)]
            values[u] = [jnp.where(t == at, a, b) for a, b in zip(halo, values[u])]
        return values

    def fill(t, kern):
        x = pts_ref[t, :, pl.ds(own, HALF)].astype(f32).T.astype(bf16)
        points = [[pts_ref[u, :, pl.ds(h, HALF)] for h in (own, other)] for u in sources(t)]
        points = taken(t, slice(R, R + 8), points)
        for k in range(3):
            y = jnp.concatenate(points[k], 1)
            for p in range(0, HALF, 32):
                squared = None
                for i in range(3):
                    differ = x[p : p + 32, i : i + 1] - y[i : i + 1, :]
                    differ = differ * differ
                    squared = differ + bf16(soften_sq) if squared is None else squared + differ
                kern[p : p + 32, k * LEAF : (k + 1) * LEAF] = lax.rsqrt(squared)

    def product(t, kern):
        values = [[vec_ref[u], other_ref[u]] for u in sources(t)]
        values = taken(t, slice(0, R), values)
        values = jnp.concatenate([v for pair in values for v in pair], 1)
        out_ref[t] = nt(values, kern[...]) * inverse_four_pi

    def leaf(i):
        if not edges:
            return leaves[0] + i
        i = jnp.where(i < leaves[0], i, i + leaves[1] - leaves[0])
        return jnp.where(i < T, i, count - 1)

    steps = T - leaves[1] + leaves[0] + 1 if edges else leaves[1] - leaves[0]
    group = 3 if edges else 4
    fill(leaf(0), kerns[0])

    def body(i, _):
        for s in range(group):
            fill(leaf(jnp.minimum(group * i + s + 1, steps - 1)), kerns[(s + 1) % group])
            product(leaf(group * i + s), kerns[s])
        return 0

    lax.fori_loop(0, steps // group, body, 0)


def near_call(leaves, args, halos=(), base=None):
    size = T - leaves[1] + leaves[0] + 1 if halos else leaves[1] - leaves[0]
    bases = () if base is None else (base,)
    count = len(args) + len(halos)
    return pl.pallas_call(
        lambda *refs: near_kernel(leaves, bool(halos), *refs),
        out_shape=jax.ShapeDtypeStruct((T, R, HALF), f32),
        in_specs=[SMEM] + [VMEM] * (count - 1 + len(bases)),
        out_specs=VMEM,
        scratch_shapes=[pltpu.VMEM((HALF, 3 * LEAF), bf16)] * 4,
        input_output_aliases={count: 0} if bases else {},
        cost_estimate=pl.CostEstimate(
            flops=size * 200_000_000, bytes_accessed=2_000_000, transcendentals=0
        ),
        name="near",
        compiler_params=LIMIT,
    )(*args, *halos, *bases)


def final_kernel(scalar_ref, mine_ref, theirs_ref, tgt_ref, near_ref, out_ref, rows):
    count, n = scalar_ref[0], scalar_ref[1]
    for ref, first in ((mine_ref, n * RH), (theirs_ref, (1 - n) * RH)):
        for r in range(RH):
            part = ref[r // 2].astype(f32)[:, (r % 2) * A : (r % 2 + 1) * A]
            rows[pl.ds(first + r, T, stride=R), :] = jnp.concatenate([part, part], 1)
    same = (iota((64, 256), 0) >> 4) == (iota((64, 256), 1) >> 6)
    for g in range(T // 4):
        part = rows[64 * g : 64 * g + 64, :]
        lhs = jnp.where(same, jnp.concatenate([part, part], 1), 0.0).astype(bf16)
        tgt = tgt_ref[4 * g : 4 * g + 4, :, pl.ds(pl.multiple_of(n * HALF, HALF), HALF)]
        far = nn(lhs, tgt.reshape(4 * A, HALF)).reshape(4, R, HALF)
        total = far + near_ref[4 * g : 4 * g + 4]
        live = (iota((4, R, HALF), 0) + 4 * g) < count
        out_ref[4 * g : 4 * g + 4] = jnp.where(live, total, 0.0).astype(bf16)


def final_call(scalars, mine, theirs, tgt, near):
    return pl.pallas_call(
        final_kernel,
        out_shape=jax.ShapeDtypeStruct((T, R, HALF), bf16),
        in_specs=[SMEM] + [VMEM] * 4,
        out_specs=VMEM,
        scratch_shapes=[pltpu.VMEM((T * R, 128), f32)],
        name="final",
        compiler_params=LIMIT,
    )(scalars, mine, theirs, tgt, near)


def shifted(array, axis, by):
    devices = lax.axis_size(axis)
    return lax.ppermute(array, axis, [(i, (i + by) % devices) for i in range(devices)])


def to_all(array, axis):
    copies = jnp.broadcast_to(array[None], (lax.axis_size(axis), *array.shape))
    return lax.all_to_all(copies, axis, split_axis=0, concat_axis=0, tiled=True)


def onward(array, by, flip):
    size = 2 * lax.axis_size(WIDE)
    return lax.ppermute(
        array, (*WIDE, "n"), [(i, ((i // 2 * 2 + 2 * by) % size) + (i % 2 ^ flip)) for i in range(size)]
    )


def body(points, vectors, counts, src_basis, tgt_basis, adm_src, couplings):
    n = lax.axis_index("n").astype(i32)
    z = lax.axis_index("z").astype(i32)
    scalars = jnp.stack([counts[0], n])

    keep, send = coeff_call(n[None], vectors, src_basis)
    came = shifted(send, "n", 1)
    other = shifted(vectors, "n", 1)
    sel, req, rows, first, last = index_call(scalars, adm_src.T, points.transpose(1, 0, 2), vectors)
    asked = lax.all_to_all(req, PEERS, split_axis=0, concat_axis=0, tiled=True)

    coeffs = (keep + came).astype(bf16)
    up = shifted(coeffs, "z", -2)
    down = shifted(coeffs, "z", 2)
    across = shifted(coeffs, "z", 4)
    odd_up = shifted(jnp.concatenate([coeffs, up]), "z", -1)
    odd_down = shifted(jnp.concatenate([coeffs, down]), "z", 1)
    pieces = coeffs, up, down, across, odd_up, odd_down

    halos = tuple(onward(edge, by, flip) for edge, by in ((last, 1), (first, -1)) for flip in range(2))
    near_args = (scalars, rows, vectors, other)
    near = near_call((4, 12), near_args)
    near = near_call((12, 28), near_args, base=near)
    near = near_call((4, 28), near_args, halos, near)

    got = lax.all_to_all(pack_call(z[None], asked, pieces), PEERS, split_axis=0, concat_axis=0, tiled=True)
    mine = select_call(sel, got, couplings)

    def every(mine, pieces, couplings):
        blocks = {o % N_Z: p[k * T : (k + 1) * T] for p, os in zip(pieces, OFFSETS) for k, o in enumerate(os)}
        twice = jnp.concatenate([blocks[o % N_Z] for o in range(2 * N_Z)])
        table = lax.dynamic_slice_in_dim(twice, (N_Z - z) % N_Z * T, COLUMN, 0)
        whole = to_all(table, PEERS).reshape(N_PEER * COLUMN, RH * A)
        leaf = adm_src.T.reshape(ENTRIES)
        place = ((leaf >> 11) * 8 + ((leaf >> 5) & 7)) * COLUMN + ((leaf >> 8) & 7) * T + (leaf & (T - 1))
        hot = (place[:, None] == jnp.arange(N_PEER * COLUMN, dtype=i32)[None, :]).astype(bf16)
        return couple_call(jnp.dot(hot, whole, preferred_element_type=f32), couplings)

    fits = jnp.min(asked[:, 0, 0]) >= 0
    mine = lax.cond(fits, lambda mine, *_: mine, every, mine, pieces, couplings)
    theirs = shifted(mine, "n", 1)
    return final_call(scalars, mine, theirs, tgt_basis, near)


def solution(mesh):
    split = Mesh(
        mesh.devices.reshape(2, 8, 4, 2, mesh.shape["narrow"]), ("y", "z", "x", "c", "n")
    )
    in_specs = (
        P(WIDE, None, None),
        P(WIDE, None, "n"),
        P(WIDE),
        P(WIDE, None, "n"),
        P(WIDE, None, None),
        P(WIDE, None),
        P(WIDE, None, None),
    )
    out_specs = P(WIDE, None, "n")
    return jax.shard_map(body, mesh=split, in_specs=in_specs, out_specs=out_specs, check_vma=False)
```

```python
import math

import jax
import jax.numpy as jnp
from jax import lax
from jax.experimental import pallas as pl
from jax.experimental.pallas import tpu as pltpu
from jax.sharding import Mesh
from jax.sharding import PartitionSpec as P


WIDE = ("y", "z", "x", "c")
PEERS = ("y", "x", "c")

inverse_four_pi = 1.0 / (4.0 * math.pi)
soften_sq = 0.0025

T, R, A, J, HALF, LEAF = 32, 16, 64, 8, 256, 512
RH = R // 2
N_Z, N_PEER = 8, 16
CAP = 48
ENTRIES = T * J
OFFSETS = (0,), (2,), (-2,), (4,), (1, 3), (-1, -3)
COLUMN = N_Z * T
bf16, f32, i32 = jnp.bfloat16, jnp.float32, jnp.int32

VMEM = pl.BlockSpec(memory_space=pltpu.VMEM)
SMEM = pl.BlockSpec(memory_space=pltpu.SMEM)
HBM = pl.BlockSpec(memory_space=pltpu.HBM)
LIMIT = pltpu.CompilerParams(vmem_limit_bytes=20 * 2**20)


def nt(a, b):
    return lax.dot_general(a, b, (((1,), (1,)), ((), ())), preferred_element_type=f32)


def nn(a, b):
    return lax.dot_general(a, b, (((1,), (0,)), ((), ())), preferred_element_type=f32)


def iota(shape, dim):
    return lax.broadcasted_iota(i32, shape, dim)


def folded(wide):
    two = wide[:, :128] + wide[:, 128:]
    return two[:, :64] + two[:, 64:]


def chunks(source, target, sems, size):
    copies = [
        pltpu.make_async_copy(source.at[pl.ds(k, size)], target.at[pl.ds(k, size)], sems.at[k // size])
        for k in range(0, T, size)
    ]
    for copy in copies:
        copy.start()
    return copies


def index_kernel(scalar_ref, adm_ref, pts_ref, sel_ref, req_ref, rows_ref):
    pts = pts_ref[...].astype(f32)
    blank = jnp.zeros((5, LEAF), f32)
    for t in range(T):
        rows_ref[t] = jnp.concatenate([pts[i, t : t + 1] for i in range(3)] + [blank], 0).astype(bf16)
    count = scalar_ref[0]
    adm = jnp.concatenate([adm_ref[...].astype(f32), jnp.zeros((8, 96), f32)], 1).T
    leaf = jnp.concatenate(
        [jnp.broadcast_to(adm[:T, j : j + 1], (T, 128)) for j in range(J)], 0
    ).astype(i32)
    live = (iota((ENTRIES, 128), 0) & (T - 1)) < count
    column = (leaf >> 11) * 8 + ((leaf >> 5) & 7)
    row = ((leaf >> 8) & 7) * T + (leaf & (T - 1))
    member = jnp.where((column == iota((ENTRIES, 128), 1)) & live, 1.0, 0.0)
    below = jnp.where(iota((ENTRIES, ENTRIES), 0) > iota((ENTRIES, ENTRIES), 1), 1.0, 0.0)
    rank = nn(below.astype(bf16), member.astype(bf16))
    place = jnp.sum(member * rank, axis=1, keepdims=True)
    over = jnp.max(place) > CAP - 0.5
    place = jnp.broadcast_to(place, (ENTRIES, 128))
    fits = live & (place < CAP - 0.5)
    sel = jnp.where(fits, column * CAP + place.astype(i32), -1)
    sel_ref[...] = sel
    sel_row = sel.astype(f32).T[:1]
    slots = N_PEER * CAP
    pick = jnp.where(iota((slots, ENTRIES), 0) == sel_row.astype(i32), 1.0, 0.0).astype(bf16)
    wanted = nn(pick, (row + 1).astype(f32).astype(bf16))
    wanted = jnp.where(over, -1.0, wanted)
    req_ref[...] = wanted.astype(bf16).reshape(N_PEER, CAP, 128)


def index_call(scalars, adm, points):
    return pl.pallas_call(
        index_kernel,
        out_shape=(
            jax.ShapeDtypeStruct((ENTRIES, 128), i32),
            jax.ShapeDtypeStruct((N_PEER, CAP, 128), bf16),
            jax.ShapeDtypeStruct((T, 8, LEAF), bf16),
        ),
        in_specs=[SMEM, VMEM, VMEM],
        out_specs=(VMEM,) * 3,
        name="requests",
        compiler_params=LIMIT,
    )(scalars, adm, points)


def coeff_kernel(n_ref, vec_hbm, basis_hbm, keep_ref, send_ref, rows, vec_ref, basis_ref, sems):
    vec_copies = chunks(vec_hbm, vec_ref, sems.at[0], 8)
    basis_copies = chunks(basis_hbm, basis_ref, sems.at[1], 8)
    n = n_ref[0]
    same = (iota((64, 256), 0) >> 4) == (iota((64, 256), 1) >> 6)
    for g in range(T // 4):
        if g % 2 == 0:
            vec_copies[g // 2].wait()
            basis_copies[g // 2].wait()
        lhs = vec_ref[4 * g : 4 * g + 4].reshape(64, HALF)
        rhs = basis_ref[4 * g : 4 * g + 4].reshape(4 * A, HALF)
        rows[64 * g : 64 * g + 64, :64] = folded(jnp.where(same, nt(lhs, rhs), 0.0))
    for out, first in ((send_ref, (1 - n) * RH), (keep_ref, n * RH)):
        for r in range(0, RH, 2):
            pair = [rows[pl.ds(first + r + k, T, stride=R), :][:, :64] for k in range(2)]
            out[:, r * A : (r + 2) * A] = jnp.concatenate(pair, 1)


def coeff_call(n, vectors, basis):
    shape = jax.ShapeDtypeStruct((T, RH * A), f32)
    return pl.pallas_call(
        coeff_kernel,
        out_shape=(shape, shape),
        in_specs=[SMEM, HBM, HBM],
        out_specs=(VMEM, VMEM),
        scratch_shapes=[
            pltpu.VMEM((T * R, 128), f32),
            pltpu.VMEM((T, R, HALF), bf16),
            pltpu.VMEM((T, A, HALF), bf16),
            pltpu.SemaphoreType.DMA((2, 4)),
        ],
        name="coeffs",
        compiler_params=LIMIT,
    )(n, vectors, basis)


def pack_kernel(z_ref, req_ref, *refs):
    *pieces, out_ref, fits_ref, table_ref = refs
    refused = jnp.min(req_ref[:, :8].astype(f32)) < 0.0
    fits_ref[0] = jnp.where(refused, 0, 1)
    for piece, offsets in zip(pieces, OFFSETS):
        for k, offset in enumerate(offsets):
            first = pl.multiple_of(((z_ref[0] + offset) & (N_Z - 1)) * T, T)
            table_ref[pl.ds(first, T), :] = piece[k * T : (k + 1) * T]
    lanes = iota((CAP, 128), 1).astype(f32) + 1.0
    for r in range(0, N_PEER, 4):
        want = [req_ref[r + k].astype(f32) for k in range(4)]
        hot = [
            jnp.concatenate(
                [jnp.where(w == lanes, 1.0, 0.0), jnp.where(w == lanes + 128.0, 1.0, 0.0)], 1
            )
            for w in want
        ]
        picked = nn(jnp.concatenate(hot, 0).astype(bf16), table_ref[...])
        out_ref[r : r + 4] = picked.astype(bf16).reshape(4, CAP, RH * A)


def pack_call(z, req, pieces):
    return pl.pallas_call(
        pack_kernel,
        out_shape=(
            jax.ShapeDtypeStruct((N_PEER, CAP, RH * A), bf16),
            jax.ShapeDtypeStruct((1,), i32),
        ),
        in_specs=[SMEM] + [VMEM] * (1 + len(pieces)),
        out_specs=(VMEM, SMEM),
        scratch_shapes=[pltpu.VMEM((COLUMN, RH * A), bf16)],
        name="pack",
        compiler_params=LIMIT,
    )(z, req, *pieces)


def couple(picked, couple_ref, out_ref, copies=()):
    lows = [picked[j * T : (j + 1) * T] for j in range(J)]
    by_rhs = []
    for r in range(RH):
        cols = [low[:, r * A : (r + 1) * A] for low in lows]
        by_rhs.append(jnp.concatenate(cols, 1).astype(bf16))
    row_t = iota((16 * RH, 256), 0) & 15
    col_t = iota((16 * RH, 256), 1) >> 6
    for h in range(2):
        lhs = jnp.concatenate([s[16 * h : 16 * h + 16] for s in by_rhs], 0)
        total = jnp.zeros((16 * RH, A), f32)
        for g in range(4):
            first = 16 * h + 4 * g
            if copies and first % 8 == 0:
                copies[first // 8].wait()
            rhs = couple_ref[first : first + 4].reshape(4 * A, J * A)
            total = total + folded(jnp.where(row_t == col_t + 4 * g, nt(lhs, rhs), 0.0))
        total = total.reshape(RH, 16, A)
        for r in range(0, RH, 2):
            pair = jnp.concatenate([total[r], total[r + 1]], 1)
            out_ref[r // 2, 16 * h : 16 * h + 16, :] = pair.astype(bf16)


def select_kernel(sel_ref, got_ref, couple_hbm, out_ref, couple_ref, sems):
    copies = chunks(couple_hbm, couple_ref, sems, 8)
    slots = N_PEER * CAP
    sel = sel_ref[...]
    lanes = iota((ENTRIES, 128), 1)
    hot = jnp.concatenate(
        [jnp.where(sel == lanes + 128 * k, 1.0, 0.0) for k in range(slots // 128)], 1
    )
    picked = nn(hot.astype(bf16), got_ref[...].reshape(slots, RH * A))
    couple(picked, couple_ref, out_ref, copies)


TC_SHAPE = jax.ShapeDtypeStruct((RH // 2, T, 2 * A), bf16)


def select_call(sel, got, couplings):
    return pl.pallas_call(
        select_kernel,
        out_shape=TC_SHAPE,
        in_specs=[VMEM, VMEM, HBM],
        out_specs=VMEM,
        scratch_shapes=[pltpu.VMEM((T, A, J * A), bf16), pltpu.SemaphoreType.DMA((4,))],
        name="select",
        compiler_params=LIMIT,
    )(sel, got, couplings)


def couple_kernel(picked_ref, couple_ref, out_ref):
    couple(picked_ref[...], couple_ref, out_ref)


def couple_call(picked, couplings):
    return pl.pallas_call(
        couple_kernel,
        out_shape=TC_SHAPE,
        in_specs=[VMEM, VMEM],
        out_specs=VMEM,
        name="couple",
        compiler_params=LIMIT,
    )(picked, couplings)


def near_kernel(leaves, edges, group, scalar_ref, pts_ref, vec_ref, other_ref, *refs):
    edge_refs, kerns, outs = refs[: 2 * edges], refs[-group:], refs[:-group]
    send_refs = () if edges or len(outs) < 3 else outs[-2:]
    out_ref = outs[-3] if send_refs else outs[-1]
    count, n = scalar_ref[0], scalar_ref[1]
    own = pl.multiple_of(n * HALF, HALF)
    other = pl.multiple_of((1 - n) * HALF, HALF)

    for ref, t in zip(send_refs, (0, count - 1)):
        ref[:R, pl.ds(own, HALF)] = vec_ref[t]
        ref[:R, pl.ds(other, HALF)] = other_ref[t]
        ref[R:] = pts_ref[t]

    def sources(t):
        return (t + T - 1) & (T - 1), t, (t + 1) & (T - 1)

    def taken(t, rows, values):
        if not edges:
            return values
        for k, (u, at) in enumerate(((0, 0), (2, count - 1))):
            halo = [edge_refs[k][rows, pl.ds(h, HALF)] for h in (own, other)]
            values[u] = [jnp.where(t == at, a, b) for a, b in zip(halo, values[u])]
        return values

    def fill(t, kern):
        x = pts_ref[t, :, pl.ds(own, HALF)].astype(f32).T.astype(bf16)
        points = [[pts_ref[u, :, pl.ds(h, HALF)] for h in (own, other)] for u in sources(t)]
        points = taken(t, slice(R, R + 8), points)
        for k in range(3):
            y = jnp.concatenate(points[k], 1)
            for p in range(0, HALF, 32):
                squared = None
                for i in range(3):
                    differ = x[p : p + 32, i : i + 1] - y[i : i + 1, :]
                    differ = differ * differ
                    squared = differ + bf16(soften_sq) if squared is None else squared + differ
                kern[p : p + 32, k * LEAF : (k + 1) * LEAF] = lax.rsqrt(squared)

    def product(t, kern):
        values = [[vec_ref[u], other_ref[u]] for u in sources(t)]
        values = taken(t, slice(0, R), values)
        values = jnp.concatenate([v for pair in values for v in pair], 1)
        out_ref[t] = nt(values, kern[...]) * inverse_four_pi

    def leaf(i):
        if not edges:
            return leaves[0] + i
        i = jnp.where(i < leaves[0], i, i + leaves[1] - leaves[0])
        return jnp.where(i < T, i, count - 1)

    steps = T - leaves[1] + leaves[0] + 1 if edges else leaves[1] - leaves[0]
    fill(leaf(0), kerns[0])

    def body(i, _):
        for s in range(group):
            fill(leaf(jnp.minimum(group * i + s + 1, steps - 1)), kerns[(s + 1) % group])
            product(leaf(group * i + s), kerns[s])
        return 0

    lax.fori_loop(0, steps // group, body, 0)


def near_call(leaves, args, halos=(), base=None):
    size = T - leaves[1] + leaves[0] + 1 if halos else leaves[1] - leaves[0]
    bases = () if base is None else (base,)
    count = len(args) + len(halos)
    group = size if halos else 8
    field = jax.ShapeDtypeStruct((T, R, HALF), f32)
    edge = jax.ShapeDtypeStruct((R + 8, LEAF), bf16)
    return pl.pallas_call(
        lambda *refs: near_kernel(leaves, bool(halos), group, *refs),
        out_shape=field if bases else (field, edge, edge),
        in_specs=[SMEM] + [VMEM] * (count - 1 + len(bases)),
        out_specs=VMEM if bases else (VMEM,) * 3,
        scratch_shapes=[pltpu.VMEM((HALF, 3 * LEAF), bf16)] * group,
        input_output_aliases={count: 0} if bases else {},
        cost_estimate=pl.CostEstimate(
            flops=size * 200_000_000, bytes_accessed=2_000_000, transcendentals=0
        ),
        name="near",
        compiler_params=LIMIT,
    )(*args, *halos, *bases)


def final_kernel(scalar_ref, mine_ref, theirs_ref, tgt_ref, near_ref, out_ref, rows):
    count, n = scalar_ref[0], scalar_ref[1]
    for ref, first in ((mine_ref, n * RH), (theirs_ref, (1 - n) * RH)):
        for r in range(RH):
            part = ref[r // 2].astype(f32)[:, (r % 2) * A : (r % 2 + 1) * A]
            rows[pl.ds(first + r, T, stride=R), :] = jnp.concatenate([part, part], 1)
    same = (iota((64, 256), 0) >> 4) == (iota((64, 256), 1) >> 6)
    for g in range(T // 4):
        part = rows[64 * g : 64 * g + 64, :]
        lhs = jnp.where(same, jnp.concatenate([part, part], 1), 0.0).astype(bf16)
        tgt = tgt_ref[4 * g : 4 * g + 4, :, pl.ds(pl.multiple_of(n * HALF, HALF), HALF)]
        far = nn(lhs, tgt.reshape(4 * A, HALF)).reshape(4, R, HALF)
        total = far + near_ref[4 * g : 4 * g + 4]
        live = (iota((4, R, HALF), 0) + 4 * g) < count
        out_ref[4 * g : 4 * g + 4] = jnp.where(live, total, 0.0).astype(bf16)


def final_call(scalars, mine, theirs, tgt, near):
    return pl.pallas_call(
        final_kernel,
        out_shape=jax.ShapeDtypeStruct((T, R, HALF), bf16),
        in_specs=[SMEM] + [VMEM] * 4,
        out_specs=VMEM,
        scratch_shapes=[pltpu.VMEM((T * R, 128), f32)],
        name="final",
        compiler_params=LIMIT,
    )(scalars, mine, theirs, tgt, near)


def shifted(array, axis, by):
    devices = lax.axis_size(axis)
    return lax.ppermute(array, axis, [(i, (i + by) % devices) for i in range(devices)])


def to_all(array, axis):
    copies = jnp.broadcast_to(array[None], (lax.axis_size(axis), *array.shape))
    return lax.all_to_all(copies, axis, split_axis=0, concat_axis=0, tiled=True)


def body(points, vectors, counts, src_basis, tgt_basis, adm_src, couplings):
    n = lax.axis_index("n").astype(i32)
    z = lax.axis_index("z").astype(i32)
    scalars = jnp.stack([counts[0], n])

    keep, send = coeff_call(n[None], vectors, src_basis)
    came = shifted(send, "n", 1)
    other = shifted(vectors, "n", 1)
    sel, req, rows = index_call(scalars, adm_src.T, points.transpose(1, 0, 2))
    asked = lax.all_to_all(req, PEERS, split_axis=0, concat_axis=0, tiled=True)

    coeffs = (keep + came).astype(bf16)
    up = shifted(coeffs, "z", -2)
    down = shifted(coeffs, "z", 2)
    across = shifted(coeffs, "z", 4)
    odd_up = shifted(jnp.concatenate([coeffs, up]), "z", -1)
    odd_down = shifted(jnp.concatenate([coeffs, down]), "z", 1)
    pieces = coeffs, up, down, across, odd_up, odd_down

    near_args = (scalars, rows, vectors, other)
    near, first, last = near_call((4, 12), near_args)
    halos = shifted(last, WIDE, 1), shifted(first, WIDE, -1)
    near = near_call((12, 28), near_args, base=near)
    near = near_call((4, 28), near_args, halos, near)

    packed, fits = pack_call(z[None], asked, pieces)
    got = lax.all_to_all(packed, PEERS, split_axis=0, concat_axis=0, tiled=True)
    mine = select_call(sel, got, couplings)

    def every(mine, pieces, couplings):
        blocks = {o % N_Z: p[k * T : (k + 1) * T] for p, os in zip(pieces, OFFSETS) for k, o in enumerate(os)}
        twice = jnp.concatenate([blocks[o % N_Z] for o in range(2 * N_Z)])
        table = lax.dynamic_slice_in_dim(twice, (N_Z - z) % N_Z * T, COLUMN, 0)
        whole = to_all(table, PEERS).reshape(N_PEER * COLUMN, RH * A)
        leaf = adm_src.T.reshape(ENTRIES)
        place = ((leaf >> 11) * 8 + ((leaf >> 5) & 7)) * COLUMN + ((leaf >> 8) & 7) * T + (leaf & (T - 1))
        hot = (place[:, None] == jnp.arange(N_PEER * COLUMN, dtype=i32)[None, :]).astype(bf16)
        return couple_call(jnp.dot(hot, whole, preferred_element_type=f32), couplings)

    mine = lax.cond(fits[0] != 0, lambda mine, *_: mine, every, mine, pieces, couplings)
    theirs = shifted(mine, "n", 1)
    return final_call(scalars, mine, theirs, tgt_basis, near)


def solution(mesh):
    split = Mesh(
        mesh.devices.reshape(2, 8, 4, 2, mesh.shape["narrow"]), ("y", "z", "x", "c", "n")
    )
    in_specs = (
        P(WIDE, None, None),
        P(WIDE, None, "n"),
        P(WIDE),
        P(WIDE, None, "n"),
        P(WIDE, None, None),
        P(WIDE, None),
        P(WIDE, None, None),
    )
    out_specs = P(WIDE, None, "n")
    return jax.shard_map(body, mesh=split, in_specs=in_specs, out_specs=out_specs, check_vma=False)
```

```python
import math

import jax
import jax.numpy as jnp
from jax import lax
from jax.experimental import pallas as pl
from jax.experimental.pallas import tpu as pltpu
from jax.sharding import Mesh
from jax.sharding import PartitionSpec as P


WIDE = ("y", "z", "x", "c")
PEERS = ("y", "x", "c")

inverse_four_pi = 1.0 / (4.0 * math.pi)
soften_sq = 0.0025

T, R, A, J, HALF, LEAF = 32, 16, 64, 8, 256, 512
RH = R // 2
N_Z, N_PEER = 8, 16
CAP = 48
ENTRIES = T * J
OFFSETS = (0,), (-1,), (1,), (2, 3, 4), (-2, -3)
SENT = T * R + 4 * T
COLUMN = N_Z * T
bf16, f32, i32 = jnp.bfloat16, jnp.float32, jnp.int32

VMEM = pl.BlockSpec(memory_space=pltpu.VMEM)
SMEM = pl.BlockSpec(memory_space=pltpu.SMEM)
HBM = pl.BlockSpec(memory_space=pltpu.HBM)
LIMIT = pltpu.CompilerParams(vmem_limit_bytes=20 * 2**20)


def nt(a, b):
    return lax.dot_general(a, b, (((1,), (1,)), ((), ())), preferred_element_type=f32)


def nn(a, b):
    return lax.dot_general(a, b, (((1,), (0,)), ((), ())), preferred_element_type=f32)


def iota(shape, dim):
    return lax.broadcasted_iota(i32, shape, dim)


def folded(wide):
    two = wide[:, :128] + wide[:, 128:]
    return two[:, :64] + two[:, 64:]


def chunks(source, target, sems, size):
    copies = [
        pltpu.make_async_copy(source.at[pl.ds(k, size)], target.at[pl.ds(k, size)], sems.at[k // size])
        for k in range(0, T, size)
    ]
    for copy in copies:
        copy.start()
    return copies


def index_kernel(scalar_ref, adm_ref, pts_ref, sel_ref, req_ref, rows_ref):
    pts = pts_ref[...].astype(f32)
    blank = jnp.zeros((5, LEAF), f32)
    for t in range(T):
        rows_ref[t] = jnp.concatenate([pts[i, t : t + 1] for i in range(3)] + [blank], 0).astype(bf16)
    count = scalar_ref[0]
    adm = jnp.concatenate([adm_ref[...].astype(f32), jnp.zeros((8, 96), f32)], 1).T
    leaf = jnp.concatenate(
        [jnp.broadcast_to(adm[:T, j : j + 1], (T, 128)) for j in range(J)], 0
    ).astype(i32)
    live = (iota((ENTRIES, 128), 0) & (T - 1)) < count
    column = (leaf >> 11) * 8 + ((leaf >> 5) & 7)
    row = ((leaf >> 8) & 7) * T + (leaf & (T - 1))
    member = jnp.where((column == iota((ENTRIES, 128), 1)) & live, 1.0, 0.0)
    below = jnp.where(iota((ENTRIES, ENTRIES), 0) > iota((ENTRIES, ENTRIES), 1), 1.0, 0.0)
    rank = nn(below.astype(bf16), member.astype(bf16))
    place = jnp.sum(member * rank, axis=1, keepdims=True)
    over = jnp.max(place) > CAP - 0.5
    place = jnp.broadcast_to(place, (ENTRIES, 128))
    fits = live & (place < CAP - 0.5)
    sel = jnp.where(fits, column * CAP + place.astype(i32), -1)
    sel_ref[...] = sel
    sel_row = sel.astype(f32).T[:1]
    slots = N_PEER * CAP
    pick = jnp.where(iota((slots, ENTRIES), 0) == sel_row.astype(i32), 1.0, 0.0).astype(bf16)
    wanted = nn(pick, (row + 1).astype(f32).astype(bf16))
    wanted = jnp.where(over, -1.0, wanted)
    req_ref[...] = wanted.astype(bf16).reshape(N_PEER, CAP, 128)


def index_call(scalars, adm, points):
    return pl.pallas_call(
        index_kernel,
        out_shape=(
            jax.ShapeDtypeStruct((ENTRIES, 128), i32),
            jax.ShapeDtypeStruct((N_PEER, CAP, 128), bf16),
            jax.ShapeDtypeStruct((T, 8, LEAF), bf16),
        ),
        in_specs=[SMEM, VMEM, VMEM],
        out_specs=(VMEM,) * 3,
        name="requests",
        compiler_params=LIMIT,
    )(scalars, adm, points)


def coeff_kernel(n_ref, vec_ref, basis_ref, keep_ref, send_ref, rows):
    n = n_ref[0]
    same = (iota((64, 256), 0) >> 4) == (iota((64, 256), 1) >> 6)
    for g in range(T // 4):
        lhs = vec_ref[4 * g : 4 * g + 4].reshape(64, HALF)
        send_ref[64 * g : 64 * g + 64] = lhs
        rhs = basis_ref[4 * g : 4 * g + 4].reshape(4 * A, HALF)
        rows[64 * g : 64 * g + 64, :64] = folded(jnp.where(same, nt(lhs, rhs), 0.0))
    for mine, first in ((False, (1 - n) * RH), (True, n * RH)):
        for r in range(0, RH, 2):
            pair = [rows[pl.ds(first + r + k, T, stride=R), :][:, :64] for k in range(2)]
            value = jnp.concatenate(pair, 1)
            row, lane = r * A // HALF * T, r * A % HALF
            if mine:
                keep_ref[row : row + T, lane : lane + 2 * A] = value
            else:
                high = value.astype(bf16)
                row += T * R
                send_ref[row : row + T, lane : lane + 2 * A] = high
                row += 2 * T
                send_ref[row : row + T, lane : lane + 2 * A] = (value - high.astype(f32)).astype(bf16)


def coeff_call(n, vectors, basis):
    return pl.pallas_call(
        coeff_kernel,
        out_shape=(
            jax.ShapeDtypeStruct((2 * T, HALF), f32),
            jax.ShapeDtypeStruct((SENT, HALF), bf16),
        ),
        in_specs=[SMEM, VMEM, VMEM],
        out_specs=(VMEM, VMEM),
        scratch_shapes=[pltpu.VMEM((T * R, 128), f32)],
        name="coeffs",
        compiler_params=LIMIT,
    )(n, vectors, basis)


def pack_kernel(z_ref, req_ref, *refs):
    *pieces, out_ref, fits_ref, table_ref = refs
    refused = jnp.min(req_ref[:, :8].astype(f32)) < 0.0
    fits_ref[0] = jnp.where(refused, 0, 1)
    for piece, offsets in zip(pieces, OFFSETS):
        for k, offset in enumerate(offsets):
            first = pl.multiple_of(((z_ref[0] + offset) & (N_Z - 1)) * T, T)
            for h in range(2):
                row = (2 * k + h) * T
                table_ref[pl.ds(first, T), h * HALF : (h + 1) * HALF] = piece[row : row + T]
    lanes = iota((CAP, 128), 1).astype(f32) + 1.0
    for r in range(0, N_PEER, 4):
        want = [req_ref[r + k].astype(f32) for k in range(4)]
        hot = [
            jnp.concatenate(
                [jnp.where(w == lanes, 1.0, 0.0), jnp.where(w == lanes + 128.0, 1.0, 0.0)], 1
            )
            for w in want
        ]
        picked = nn(jnp.concatenate(hot, 0).astype(bf16), table_ref[...])
        out_ref[r : r + 4] = picked.astype(bf16).reshape(4, CAP, RH * A)


def pack_call(z, req, pieces):
    return pl.pallas_call(
        pack_kernel,
        out_shape=(
            jax.ShapeDtypeStruct((N_PEER, CAP, RH * A), bf16),
            jax.ShapeDtypeStruct((1,), i32),
        ),
        in_specs=[SMEM] + [VMEM] * (1 + len(pieces)),
        out_specs=(VMEM, SMEM),
        scratch_shapes=[pltpu.VMEM((COLUMN, RH * A), bf16)],
        name="pack",
        compiler_params=LIMIT,
    )(z, req, *pieces)


def couple(picked, couple_ref, out_ref, copies=()):
    lows = [picked[j * T : (j + 1) * T] for j in range(J)]
    by_rhs = []
    for r in range(RH):
        cols = [low[:, r * A : (r + 1) * A] for low in lows]
        by_rhs.append(jnp.concatenate(cols, 1).astype(bf16))
    row_t = iota((16 * RH, 256), 0) & 15
    col_t = iota((16 * RH, 256), 1) >> 6
    for h in range(2):
        lhs = jnp.concatenate([s[16 * h : 16 * h + 16] for s in by_rhs], 0)
        total = jnp.zeros((16 * RH, A), f32)
        for g in range(4):
            first = 16 * h + 4 * g
            if copies and first % 8 == 0:
                copies[first // 8].wait()
            rhs = couple_ref[first : first + 4].reshape(4 * A, J * A)
            total = total + folded(jnp.where(row_t == col_t + 4 * g, nt(lhs, rhs), 0.0))
        total = total.reshape(RH, 16, A)
        for r in range(0, RH, 2):
            pair = jnp.concatenate([total[r], total[r + 1]], 1)
            out_ref[r // 2, 16 * h : 16 * h + 16, :] = pair.astype(bf16)


def select_kernel(sel_ref, got_ref, couple_hbm, out_ref, couple_ref, sems):
    copies = chunks(couple_hbm, couple_ref, sems, 8)
    slots = N_PEER * CAP
    sel = sel_ref[...]
    lanes = iota((ENTRIES, 128), 1)
    hot = jnp.concatenate(
        [jnp.where(sel == lanes + 128 * k, 1.0, 0.0) for k in range(slots // 128)], 1
    )
    picked = nn(hot.astype(bf16), got_ref[...].reshape(slots, RH * A))
    couple(picked, couple_ref, out_ref, copies)


TC_SHAPE = jax.ShapeDtypeStruct((RH // 2, T, 2 * A), bf16)


def select_call(sel, got, couplings):
    return pl.pallas_call(
        select_kernel,
        out_shape=TC_SHAPE,
        in_specs=[VMEM, VMEM, HBM],
        out_specs=VMEM,
        scratch_shapes=[pltpu.VMEM((T, A, J * A), bf16), pltpu.SemaphoreType.DMA((4,))],
        name="select",
        compiler_params=LIMIT,
    )(sel, got, couplings)


def couple_kernel(picked_ref, couple_ref, out_ref):
    couple(picked_ref[...], couple_ref, out_ref)


def couple_call(picked, couplings):
    return pl.pallas_call(
        couple_kernel,
        out_shape=TC_SHAPE,
        in_specs=[VMEM, VMEM],
        out_specs=VMEM,
        name="couple",
        compiler_params=LIMIT,
    )(picked, couplings)


def near_kernel(kind, leaves, group, scalar_ref, pts_ref, vec_ref, other_ref, *refs):
    edges, send_refs = (), ()
    refs, kerns = refs[:-group], refs[-group:]
    if kind == "early":
        out_ref, *send_refs = refs
    else:
        *edges, _, out_ref = refs
    count, n = scalar_ref[0], scalar_ref[1]
    own = pl.multiple_of(n * HALF, HALF)
    other = pl.multiple_of((1 - n) * HALF, HALF)

    def other_values(t):
        return other_ref[pl.ds(pl.multiple_of(t * R, R), R)]

    for ref, t in zip(send_refs, (0, count - 1)):
        ref[:R, pl.ds(own, HALF)] = vec_ref[t]
        ref[:R, pl.ds(other, HALF)] = other_values(t)
        ref[R:] = pts_ref[t]

    def sources(t):
        return (t + T - 1) & (T - 1), t, (t + 1) & (T - 1)

    def taken(t, rows, values):
        if not edges:
            return values
        for k, (u, at) in enumerate(((0, 0), (2, count - 1))):
            halo = [edges[k][rows, pl.ds(h, HALF)] for h in (own, other)]
            values[u] = [jnp.where(t == at, a, b) for a, b in zip(halo, values[u])]
        return values

    def fill(t, kern):
        x = pts_ref[t, :, pl.ds(own, HALF)].astype(f32).T.astype(bf16)
        points = [[pts_ref[u, :, pl.ds(h, HALF)] for h in (own, other)] for u in sources(t)]
        points = taken(t, slice(R, R + 8), points)
        for k in range(3):
            y = jnp.concatenate(points[k], 1)
            for p in range(0, HALF, 32):
                squared = None
                for i in range(3):
                    differ = x[p : p + 32, i : i + 1] - y[i : i + 1, :]
                    differ = differ * differ
                    squared = differ + bf16(soften_sq) if squared is None else squared + differ
                kern[p : p + 32, k * LEAF : (k + 1) * LEAF] = lax.rsqrt(squared)

    def product(t, kern):
        values = [[vec_ref[u], other_values(u)] for u in sources(t)]
        values = taken(t, slice(0, R), values)
        values = jnp.concatenate([v for pair in values for v in pair], 1)
        out_ref[t] = nt(values, kern[...]) * inverse_four_pi

    def leaf(i):
        if not edges:
            return leaves[0] + i
        i = jnp.where(i < leaves[0], i, i + leaves[1] - leaves[0])
        return jnp.where(i < T, i, count - 1)

    steps, group = near_steps(kind, leaves), len(kerns)
    fill(leaf(0), kerns[0])

    def body(i, _):
        for s in range(group):
            fill(leaf(jnp.minimum(group * i + s + 1, steps - 1)), kerns[(s + 1) % group])
            product(leaf(group * i + s), kerns[s])
        return 0

    lax.fori_loop(0, steps // group, body, 0)


def near_steps(kind, leaves):
    return T - leaves[1] + leaves[0] + 1 if kind == "rest" else leaves[1] - leaves[0]


def near_call(kind, leaves, group, args, more=()):
    field = jax.ShapeDtypeStruct((T, R, HALF), f32)
    edge = jax.ShapeDtypeStruct((R + 8, LEAF), bf16)
    outs = (field, edge, edge) if kind == "early" else (field,)
    return pl.pallas_call(
        lambda *refs: near_kernel(kind, leaves, group, *refs),
        out_shape=outs,
        in_specs=[SMEM] + [VMEM] * (len(args) - 1 + len(more)),
        out_specs=(VMEM,) * len(outs),
        scratch_shapes=[pltpu.VMEM((HALF, 3 * LEAF), bf16)] * group,
        input_output_aliases={} if kind == "early" else {len(args) + len(more) - 1: 0},
        cost_estimate=pl.CostEstimate(
            flops=near_steps(kind, leaves) * 200_000_000, bytes_accessed=2_000_000, transcendentals=0
        ),
        name="near",
        compiler_params=LIMIT,
    )(*args, *more)


def final_kernel(scalar_ref, mine_ref, theirs_ref, tgt_ref, near_ref, out_ref, rows):
    count, n = scalar_ref[0], scalar_ref[1]
    for ref, first in ((mine_ref, n * RH), (theirs_ref, (1 - n) * RH)):
        for r in range(RH):
            part = ref[r // 2].astype(f32)[:, (r % 2) * A : (r % 2 + 1) * A]
            rows[pl.ds(first + r, T, stride=R), :] = jnp.concatenate([part, part], 1)
    same = (iota((64, 256), 0) >> 4) == (iota((64, 256), 1) >> 6)
    for g in range(T // 4):
        part = rows[64 * g : 64 * g + 64, :]
        lhs = jnp.where(same, jnp.concatenate([part, part], 1), 0.0).astype(bf16)
        tgt = tgt_ref[4 * g : 4 * g + 4, :, pl.ds(pl.multiple_of(n * HALF, HALF), HALF)]
        far = nn(lhs, tgt.reshape(4 * A, HALF)).reshape(4, R, HALF)
        total = far + near_ref[4 * g : 4 * g + 4]
        live = (iota((4, R, HALF), 0) + 4 * g) < count
        out_ref[4 * g : 4 * g + 4] = jnp.where(live, total, 0.0).astype(bf16)


def final_call(scalars, mine, theirs, tgt, near):
    return pl.pallas_call(
        final_kernel,
        out_shape=jax.ShapeDtypeStruct((T, R, HALF), bf16),
        in_specs=[SMEM] + [VMEM] * 4,
        out_specs=VMEM,
        scratch_shapes=[pltpu.VMEM((T * R, 128), f32)],
        name="final",
        compiler_params=LIMIT,
    )(scalars, mine, theirs, tgt, near)


def shifted(array, axis, by):
    devices = lax.axis_size(axis)
    return lax.ppermute(array, axis, [(i, (i + by) % devices) for i in range(devices)])


def to_all(array, axis):
    copies = jnp.broadcast_to(array[None], (lax.axis_size(axis), *array.shape))
    return lax.all_to_all(copies, axis, split_axis=0, concat_axis=0, tiled=True)


def body(points, vectors, counts, src_basis, tgt_basis, adm_src, couplings):
    n = lax.axis_index("n").astype(i32)
    z = lax.axis_index("z").astype(i32)
    scalars = jnp.stack([counts[0], n])

    keep, send = coeff_call(n[None], vectors, src_basis)
    came = shifted(send, "n", 1)
    sel, req, rows = index_call(scalars, adm_src.T, points.transpose(1, 0, 2))
    asked = lax.all_to_all(req, PEERS, split_axis=0, concat_axis=0, tiled=True)

    high, low = came[T * R : T * R + 2 * T], came[T * R + 2 * T :]
    coeffs = (keep + high.astype(f32) + low.astype(f32)).astype(bf16)
    below = shifted(coeffs, "z", 1)
    above = shifted(coeffs, "z", -1)
    up = shifted(jnp.concatenate([below, coeffs, above]), "z", -3)
    down = shifted(jnp.concatenate([above, coeffs]), "z", 3)
    pieces = coeffs, below, above, up, down

    near_args = (scalars, rows, vectors, came)
    near, first, last = near_call("early", (2, 10), 8, near_args)
    halos = shifted(last, WIDE, 1), shifted(first, WIDE, -1)
    (near,) = near_call("inner", (10, 30), 10, near_args, (near,))
    (near,) = near_call("rest", (2, 30), 5, near_args, (*halos, near))

    packed, fits = pack_call(z[None], asked, pieces)
    got = lax.all_to_all(packed, PEERS, split_axis=0, concat_axis=0, tiled=True)
    mine = select_call(sel, got, couplings)

    def every(mine, pieces, couplings):
        blocks = {
            o % N_Z: jnp.concatenate([p[2 * k * T :][:T], p[(2 * k + 1) * T :][:T]], 1)
            for p, os in zip(pieces, OFFSETS)
            for k, o in enumerate(os)
        }
        twice = jnp.concatenate([blocks[o % N_Z] for o in range(2 * N_Z)])
        table = lax.dynamic_slice_in_dim(twice, (N_Z - z) % N_Z * T, COLUMN, 0)
        whole = to_all(table, PEERS).reshape(N_PEER * COLUMN, RH * A)
        leaf = adm_src.T.reshape(ENTRIES)
        place = ((leaf >> 11) * 8 + ((leaf >> 5) & 7)) * COLUMN + ((leaf >> 8) & 7) * T + (leaf & (T - 1))
        hot = (place[:, None] == jnp.arange(N_PEER * COLUMN, dtype=i32)[None, :]).astype(bf16)
        return couple_call(jnp.dot(hot, whole, preferred_element_type=f32), couplings)

    mine = lax.cond(fits[0] != 0, lambda mine, *_: mine, every, mine, pieces, couplings)
    theirs = shifted(mine, "n", 1)
    return final_call(scalars, mine, theirs, tgt_basis, near)


def solution(mesh):
    split = Mesh(
        mesh.devices.reshape(2, 8, 4, 2, mesh.shape["narrow"]), ("y", "z", "x", "c", "n")
    )
    in_specs = (
        P(WIDE, None, None),
        P(WIDE, None, "n"),
        P(WIDE),
        P(WIDE, None, "n"),
        P(WIDE, None, None),
        P(WIDE, None),
        P(WIDE, None, None),
    )
    out_specs = P(WIDE, None, "n")
    return jax.shard_map(body, mesh=split, in_specs=in_specs, out_specs=out_specs, check_vma=False)
```

```python
import math

import jax
import jax.numpy as jnp
from jax import lax
from jax.experimental import pallas as pl
from jax.experimental.pallas import tpu as pltpu
from jax.sharding import Mesh
from jax.sharding import PartitionSpec as P


WIDE = ("y", "z", "x", "c")
PEERS = ("y", "x", "c")

inverse_four_pi = 1.0 / (4.0 * math.pi)
soften_sq = 0.0025

T, R, A, J, HALF, LEAF = 32, 16, 64, 8, 256, 512
RH = R // 2
N_Z, N_PEER = 8, 16
CAP = 40
ENTRIES = T * J
OFFSETS = (0,), (-1,), (1,), (2, 3, 4), (-2, -3)
SENT = T * R + 4 * T
COLUMN = N_Z * T
bf16, f32, i32 = jnp.bfloat16, jnp.float32, jnp.int32

VMEM = pl.BlockSpec(memory_space=pltpu.VMEM)
SMEM = pl.BlockSpec(memory_space=pltpu.SMEM)
LIMIT = pltpu.CompilerParams(vmem_limit_bytes=20 * 2**20)


def nt(a, b):
    return lax.dot_general(a, b, (((1,), (1,)), ((), ())), preferred_element_type=f32)


def nn(a, b):
    return lax.dot_general(a, b, (((1,), (0,)), ((), ())), preferred_element_type=f32)


def iota(shape, dim):
    return lax.broadcasted_iota(i32, shape, dim)


def folded(wide):
    two = wide[:, :128] + wide[:, 128:]
    return two[:, :64] + two[:, 64:]


def index_kernel(scalar_ref, adm_ref, pts_ref, sel_ref, req_ref, rows_ref):
    pts = pts_ref[...].astype(f32)
    blank = jnp.zeros((5, LEAF), f32)
    for t in range(T):
        rows_ref[t] = jnp.concatenate([pts[i, t : t + 1] for i in range(3)] + [blank], 0).astype(bf16)
    count = scalar_ref[0]
    adm = jnp.concatenate([adm_ref[...].astype(f32), jnp.zeros((8, 96), f32)], 1).T
    leaf = jnp.concatenate(
        [jnp.broadcast_to(adm[:T, j : j + 1], (T, 128)) for j in range(J)], 0
    ).astype(i32)
    live = (iota((ENTRIES, 128), 0) & (T - 1)) < count
    column = (leaf >> 11) * 8 + ((leaf >> 5) & 7)
    row = ((leaf >> 8) & 7) * T + (leaf & (T - 1))
    member = jnp.where((column == iota((ENTRIES, 128), 1)) & live, 1.0, 0.0)
    below = jnp.where(iota((ENTRIES, ENTRIES), 0) > iota((ENTRIES, ENTRIES), 1), 1.0, 0.0)
    rank = nn(below.astype(bf16), member.astype(bf16))
    place = jnp.sum(member * rank, axis=1, keepdims=True)
    over = jnp.max(place) > CAP - 0.5
    place = jnp.broadcast_to(place, (ENTRIES, 128))
    fits = live & (place < CAP - 0.5)
    sel = jnp.where(fits, column * CAP + place.astype(i32), -1)
    sel_ref[...] = sel
    sel_row = sel.astype(f32).T[:1]
    slots = N_PEER * CAP
    pick = jnp.where(iota((slots, ENTRIES), 0) == sel_row.astype(i32), 1.0, 0.0).astype(bf16)
    wanted = nn(pick, (row + 1).astype(f32).astype(bf16))
    wanted = jnp.where(over, -1.0, wanted)
    req_ref[...] = wanted.astype(bf16).reshape(N_PEER, CAP, 128)


def index_call(scalars, adm, points):
    return pl.pallas_call(
        index_kernel,
        out_shape=(
            jax.ShapeDtypeStruct((ENTRIES, 128), i32),
            jax.ShapeDtypeStruct((N_PEER, CAP, 128), bf16),
            jax.ShapeDtypeStruct((T, 8, LEAF), bf16),
        ),
        in_specs=[SMEM, VMEM, VMEM],
        out_specs=(VMEM,) * 3,
        name="requests",
        compiler_params=LIMIT,
    )(scalars, adm, points)


def coeff_kernel(n_ref, vec_ref, basis_ref, keep_ref, send_ref, rows):
    n = n_ref[0]
    same = (iota((64, 256), 0) >> 4) == (iota((64, 256), 1) >> 6)
    for g in range(T // 4):
        lhs = vec_ref[4 * g : 4 * g + 4].reshape(64, HALF)
        send_ref[64 * g : 64 * g + 64] = lhs
        rhs = basis_ref[4 * g : 4 * g + 4].reshape(4 * A, HALF)
        rows[64 * g : 64 * g + 64, :64] = folded(jnp.where(same, nt(lhs, rhs), 0.0))
    for mine, first in ((False, (1 - n) * RH), (True, n * RH)):
        for r in range(0, RH, 2):
            pair = [rows[pl.ds(first + r + k, T, stride=R), :][:, :64] for k in range(2)]
            value = jnp.concatenate(pair, 1)
            row, lane = r * A // HALF * T, r * A % HALF
            if mine:
                keep_ref[row : row + T, lane : lane + 2 * A] = value
            else:
                high = value.astype(bf16)
                row += T * R
                send_ref[row : row + T, lane : lane + 2 * A] = high
                row += 2 * T
                send_ref[row : row + T, lane : lane + 2 * A] = (value - high.astype(f32)).astype(bf16)


def coeff_call(n, vectors, basis):
    return pl.pallas_call(
        coeff_kernel,
        out_shape=(
            jax.ShapeDtypeStruct((2 * T, HALF), f32),
            jax.ShapeDtypeStruct((SENT, HALF), bf16),
        ),
        in_specs=[SMEM, VMEM, VMEM],
        out_specs=(VMEM, VMEM),
        scratch_shapes=[pltpu.VMEM((T * R, 128), f32)],
        name="coeffs",
        compiler_params=LIMIT,
    )(n, vectors, basis)


def pack_kernel(z_ref, req_ref, *refs):
    *pieces, out_ref, fits_ref, table_ref = refs
    refused = jnp.min(req_ref[:, :8].astype(f32)) < 0.0
    fits_ref[0] = jnp.where(refused, 0, 1)
    for piece, offsets in zip(pieces, OFFSETS):
        for k, offset in enumerate(offsets):
            first = pl.multiple_of(((z_ref[0] + offset) & (N_Z - 1)) * T, T)
            for h in range(2):
                row = (2 * k + h) * T
                table_ref[pl.ds(first, T), h * HALF : (h + 1) * HALF] = piece[row : row + T]
    lanes = iota((CAP, 128), 1).astype(f32) + 1.0
    for r in range(0, N_PEER, 4):
        want = [req_ref[r + k].astype(f32) for k in range(4)]
        hot = [
            jnp.concatenate(
                [jnp.where(w == lanes, 1.0, 0.0), jnp.where(w == lanes + 128.0, 1.0, 0.0)], 1
            )
            for w in want
        ]
        picked = nn(jnp.concatenate(hot, 0).astype(bf16), table_ref[...])
        out_ref[r : r + 4] = picked.astype(bf16).reshape(4, CAP, RH * A)


def pack_call(z, req, pieces):
    return pl.pallas_call(
        pack_kernel,
        out_shape=(
            jax.ShapeDtypeStruct((N_PEER, CAP, RH * A), bf16),
            jax.ShapeDtypeStruct((1,), i32),
        ),
        in_specs=[SMEM] + [VMEM] * (1 + len(pieces)),
        out_specs=(VMEM, SMEM),
        scratch_shapes=[pltpu.VMEM((COLUMN, RH * A), bf16)],
        name="pack",
        compiler_params=LIMIT,
    )(z, req, *pieces)


def couple(picked, couple_ref, out_ref):
    lows = [picked[j * T : (j + 1) * T] for j in range(J)]
    by_rhs = []
    for r in range(RH):
        cols = [low[:, r * A : (r + 1) * A] for low in lows]
        by_rhs.append(jnp.concatenate(cols, 1).astype(bf16))
    row_t = iota((16 * RH, 256), 0) & 15
    col_t = iota((16 * RH, 256), 1) >> 6
    for h in range(2):
        lhs = jnp.concatenate([s[16 * h : 16 * h + 16] for s in by_rhs], 0)
        total = jnp.zeros((16 * RH, A), f32)
        for g in range(4):
            first = 16 * h + 4 * g
            rhs = couple_ref[first : first + 4].reshape(4 * A, J * A)
            total = total + folded(jnp.where(row_t == col_t + 4 * g, nt(lhs, rhs), 0.0))
        total = total.reshape(RH, 16, A)
        for r in range(0, RH, 2):
            pair = jnp.concatenate([total[r], total[r + 1]], 1)
            out_ref[r // 2, 16 * h : 16 * h + 16, :] = pair.astype(bf16)


def select_kernel(sel_ref, got_ref, couple_ref, out_ref):
    slots = N_PEER * CAP
    sel = sel_ref[...]
    lanes = iota((ENTRIES, 128), 1)
    hot = jnp.concatenate(
        [jnp.where(sel == lanes + 128 * k, 1.0, 0.0) for k in range(slots // 128)], 1
    )
    picked = nn(hot.astype(bf16), got_ref[...].reshape(slots, RH * A))
    couple(picked, couple_ref, out_ref)


TC_SHAPE = jax.ShapeDtypeStruct((RH // 2, T, 2 * A), bf16)


def select_call(sel, got, couplings):
    return pl.pallas_call(
        select_kernel,
        out_shape=TC_SHAPE,
        in_specs=[VMEM, VMEM, VMEM],
        out_specs=VMEM,
        name="select",
        compiler_params=LIMIT,
    )(sel, got, couplings)


def couple_kernel(picked_ref, couple_ref, out_ref):
    couple(picked_ref[...], couple_ref, out_ref)


def couple_call(picked, couplings):
    return pl.pallas_call(
        couple_kernel,
        out_shape=TC_SHAPE,
        in_specs=[VMEM, VMEM],
        out_specs=VMEM,
        name="couple",
        compiler_params=LIMIT,
    )(picked, couplings)


def near_kernel(kind, leaves, group, scalar_ref, pts_ref, vec_ref, other_ref, *refs):
    edges, send_refs = (), ()
    refs, kerns = refs[:-group], refs[-group:]
    if kind == "early":
        out_ref, *send_refs = refs
    else:
        *edges, _, out_ref = refs
    count, n = scalar_ref[0], scalar_ref[1]
    own = pl.multiple_of(n * HALF, HALF)
    other = pl.multiple_of((1 - n) * HALF, HALF)

    def values_of(ref, t):
        return ref[pl.ds(pl.multiple_of(t * R, R), R)]

    for ref, t in zip(send_refs, (0, count - 1)):
        ref[:R, pl.ds(own, HALF)] = values_of(vec_ref, t)
        ref[:R, pl.ds(other, HALF)] = values_of(other_ref, t)
        ref[R:] = pts_ref[t]

    def sources(t):
        return (t + T - 1) & (T - 1), t, (t + 1) & (T - 1)

    def taken(t, rows, values):
        if not edges:
            return values
        for k, (u, at) in enumerate(((0, 0), (2, count - 1))):
            halo = [edges[k][rows, pl.ds(h, HALF)] for h in (own, other)]
            values[u] = [jnp.where(t == at, a, b) for a, b in zip(halo, values[u])]
        return values

    def fill(t, kern):
        x = pts_ref[t, :, pl.ds(own, HALF)].astype(f32).T.astype(bf16)
        points = [[pts_ref[u, :, pl.ds(h, HALF)] for h in (own, other)] for u in sources(t)]
        points = taken(t, slice(R, R + 8), points)
        for k in range(3):
            y = jnp.concatenate(points[k], 1)
            for p in range(0, HALF, 32):
                squared = None
                for i in range(3):
                    differ = x[p : p + 32, i : i + 1] - y[i : i + 1, :]
                    differ = differ * differ
                    squared = differ + bf16(soften_sq) if squared is None else squared + differ
                kern[p : p + 32, k * LEAF : (k + 1) * LEAF] = lax.rsqrt(squared)

    def product(t, kern):
        values = [[values_of(vec_ref, u), values_of(other_ref, u)] for u in sources(t)]
        values = taken(t, slice(0, R), values)
        values = jnp.concatenate([v for pair in values for v in pair], 1)
        out_ref[t] = nt(values, kern[...]) * inverse_four_pi

    def leaf(i):
        if not edges:
            return leaves[0] + i
        i = jnp.where(i < leaves[0], i, i + leaves[1] - leaves[0])
        return jnp.where(i < T, i, count - 1)

    steps, group = near_steps(kind, leaves), len(kerns)
    fill(leaf(0), kerns[0])

    def body(i, _):
        for s in range(group):
            fill(leaf(jnp.minimum(group * i + s + 1, steps - 1)), kerns[(s + 1) % group])
            product(leaf(group * i + s), kerns[s])
        return 0

    lax.fori_loop(0, steps // group, body, 0)


def near_steps(kind, leaves):
    return T - leaves[1] + leaves[0] + 1 if kind == "rest" else leaves[1] - leaves[0]


def near_call(kind, leaves, group, args, more=()):
    field = jax.ShapeDtypeStruct((T, R, HALF), f32)
    edge = jax.ShapeDtypeStruct((R + 8, LEAF), bf16)
    outs = (field, edge, edge) if kind == "early" else (field,)
    return pl.pallas_call(
        lambda *refs: near_kernel(kind, leaves, group, *refs),
        out_shape=outs,
        in_specs=[SMEM] + [VMEM] * (len(args) - 1 + len(more)),
        out_specs=(VMEM,) * len(outs),
        scratch_shapes=[pltpu.VMEM((HALF, 3 * LEAF), bf16)] * group,
        input_output_aliases={} if kind == "early" else {len(args) + len(more) - 1: 0},
        cost_estimate=pl.CostEstimate(
            flops=near_steps(kind, leaves) * 200_000_000, bytes_accessed=2_000_000, transcendentals=0
        ),
        name="near",
        compiler_params=LIMIT,
    )(*args, *more)


def final_kernel(scalar_ref, mine_ref, theirs_ref, tgt_ref, near_ref, out_ref, rows):
    count, n = scalar_ref[0], scalar_ref[1]
    for ref, first in ((mine_ref, n * RH), (theirs_ref, (1 - n) * RH)):
        for r in range(RH):
            part = ref[r // 2].astype(f32)[:, (r % 2) * A : (r % 2 + 1) * A]
            rows[pl.ds(first + r, T, stride=R), :] = jnp.concatenate([part, part], 1)
    same = (iota((64, 256), 0) >> 4) == (iota((64, 256), 1) >> 6)
    for g in range(T // 4):
        part = rows[64 * g : 64 * g + 64, :]
        lhs = jnp.where(same, jnp.concatenate([part, part], 1), 0.0).astype(bf16)
        tgt = tgt_ref[4 * g : 4 * g + 4, :, pl.ds(pl.multiple_of(n * HALF, HALF), HALF)]
        far = nn(lhs, tgt.reshape(4 * A, HALF)).reshape(4, R, HALF)
        total = far + near_ref[4 * g : 4 * g + 4]
        live = (iota((4, R, HALF), 0) + 4 * g) < count
        out_ref[4 * g : 4 * g + 4] = jnp.where(live, total, 0.0).astype(bf16)


def final_call(scalars, mine, theirs, tgt, near):
    return pl.pallas_call(
        final_kernel,
        out_shape=jax.ShapeDtypeStruct((T, R, HALF), bf16),
        in_specs=[SMEM] + [VMEM] * 4,
        out_specs=VMEM,
        scratch_shapes=[pltpu.VMEM((T * R, 128), f32)],
        name="final",
        compiler_params=LIMIT,
    )(scalars, mine, theirs, tgt, near)


def shifted(array, axis, by):
    devices = lax.axis_size(axis)
    return lax.ppermute(array, axis, [(i, (i + by) % devices) for i in range(devices)])


def to_all(array, axis):
    copies = jnp.broadcast_to(array[None], (lax.axis_size(axis), *array.shape))
    return lax.all_to_all(copies, axis, split_axis=0, concat_axis=0, tiled=True)


def body(points, vectors, counts, src_basis, tgt_basis, adm_src, couplings):
    n = lax.axis_index("n").astype(i32)
    z = lax.axis_index("z").astype(i32)
    scalars = jnp.stack([counts[0], n])

    keep, send = coeff_call(n[None], vectors, src_basis)
    came = shifted(send, "n", 1)
    sel, req, rows = index_call(scalars, adm_src.T, points.transpose(1, 0, 2))
    asked = lax.all_to_all(req, PEERS, split_axis=0, concat_axis=0, tiled=True)

    high, low = came[T * R : T * R + 2 * T], came[T * R + 2 * T :]
    coeffs = (keep + high.astype(f32) + low.astype(f32)).astype(bf16)
    below = shifted(coeffs, "z", 1)
    above = shifted(coeffs, "z", -1)
    up = shifted(jnp.concatenate([below, coeffs, above]), "z", -3)
    down = shifted(jnp.concatenate([above, coeffs]), "z", 3)
    pieces = coeffs, below, above, up, down

    near_args = (scalars, rows, send, came)
    near, first, last = near_call("early", (2, 10), 8, near_args)
    halos = shifted(last, WIDE, 1), shifted(first, WIDE, -1)
    (near,) = near_call("inner", (10, 30), 10, near_args, (near,))
    (near,) = near_call("rest", (2, 30), 5, near_args, (*halos, near))

    packed, fits = pack_call(z[None], asked, pieces)
    got = lax.all_to_all(packed, PEERS, split_axis=0, concat_axis=0, tiled=True)

    def every(sel, got, pieces, couplings):
        blocks = {
            o % N_Z: jnp.concatenate([p[2 * k * T :][:T], p[(2 * k + 1) * T :][:T]], 1)
            for p, os in zip(pieces, OFFSETS)
            for k, o in enumerate(os)
        }
        twice = jnp.concatenate([blocks[o % N_Z] for o in range(2 * N_Z)])
        table = lax.dynamic_slice_in_dim(twice, (N_Z - z) % N_Z * T, COLUMN, 0)
        whole = to_all(table, PEERS).reshape(N_PEER * COLUMN, RH * A)
        leaf = adm_src.T.reshape(ENTRIES)
        place = ((leaf >> 11) * 8 + ((leaf >> 5) & 7)) * COLUMN + ((leaf >> 8) & 7) * T + (leaf & (T - 1))
        hot = (place[:, None] == jnp.arange(N_PEER * COLUMN, dtype=i32)[None, :]).astype(bf16)
        return couple_call(jnp.dot(hot, whole, preferred_element_type=f32), couplings)

    def some(sel, got, pieces, couplings):
        return select_call(sel, got, couplings)

    mine = lax.cond(fits[0] != 0, some, every, sel, got, pieces, couplings)
    theirs = shifted(mine, "n", 1)
    return final_call(scalars, mine, theirs, tgt_basis, near)


def solution(mesh):
    split = Mesh(
        mesh.devices.reshape(2, 8, 4, 2, mesh.shape["narrow"]), ("y", "z", "x", "c", "n")
    )
    in_specs = (
        P(WIDE, None, None),
        P(WIDE, None, "n"),
        P(WIDE),
        P(WIDE, None, "n"),
        P(WIDE, None, None),
        P(WIDE, None),
        P(WIDE, None, None),
    )
    out_specs = P(WIDE, None, "n")
    return jax.shard_map(body, mesh=split, in_specs=in_specs, out_specs=out_specs, check_vma=False)
```

```python
import math

import jax
import jax.numpy as jnp
from jax import lax
from jax.experimental import pallas as pl
from jax.experimental.pallas import tpu as pltpu
from jax.sharding import Mesh
from jax.sharding import PartitionSpec as P


WIDE = ("y", "z", "x", "c")
PEERS = ("y", "x", "c")

inverse_four_pi = 1.0 / (4.0 * math.pi)
soften_sq = 0.0025

T, R, A, J, HALF, LEAF = 32, 16, 64, 8, 256, 512
RH = R // 2
N_Z, N_PEER = 8, 16
CAP = 40
ENTRIES = T * J
OFFSETS = (0,), (-1,), (1,), (2, 3, 4), (-2, -3)
COLUMN = N_Z * T
bf16, f32, i32 = jnp.bfloat16, jnp.float32, jnp.int32

VMEM = pl.BlockSpec(memory_space=pltpu.VMEM)
SMEM = pl.BlockSpec(memory_space=pltpu.SMEM)
LIMIT = pltpu.CompilerParams(vmem_limit_bytes=20 * 2**20)


def nt(a, b):
    return lax.dot_general(a, b, (((1,), (1,)), ((), ())), preferred_element_type=f32)


def nn(a, b):
    return lax.dot_general(a, b, (((1,), (0,)), ((), ())), preferred_element_type=f32)


def iota(shape, dim):
    return lax.broadcasted_iota(i32, shape, dim)


def folded(wide):
    two = wide[:, :128] + wide[:, 128:]
    return two[:, :64] + two[:, 64:]


def index_kernel(scalar_ref, adm_ref, pts_ref, sel_ref, req_ref, rows_ref):
    pts = pts_ref[...].astype(f32)
    blank = jnp.zeros((5, LEAF), f32)
    for t in range(T):
        rows_ref[t] = jnp.concatenate([pts[i, t : t + 1] for i in range(3)] + [blank], 0).astype(bf16)
    count = scalar_ref[0]
    adm = jnp.concatenate([adm_ref[...].astype(f32), jnp.zeros((8, 96), f32)], 1).T
    leaf = jnp.concatenate(
        [jnp.broadcast_to(adm[:T, j : j + 1], (T, 128)) for j in range(J)], 0
    ).astype(i32)
    live = (iota((ENTRIES, 128), 0) & (T - 1)) < count
    column = (leaf >> 11) * 8 + ((leaf >> 5) & 7)
    row = ((leaf >> 8) & 7) * T + (leaf & (T - 1))
    member = jnp.where((column == iota((ENTRIES, 128), 1)) & live, 1.0, 0.0)
    below = jnp.where(iota((ENTRIES, ENTRIES), 0) > iota((ENTRIES, ENTRIES), 1), 1.0, 0.0)
    rank = nn(below.astype(bf16), member.astype(bf16))
    place = jnp.sum(member * rank, axis=1, keepdims=True)
    over = jnp.max(place) > CAP - 0.5
    place = jnp.broadcast_to(place, (ENTRIES, 128))
    fits = live & (place < CAP - 0.5)
    sel = jnp.where(fits, column * CAP + place.astype(i32), -1)
    sel_ref[...] = sel
    sel_row = sel.astype(f32).T[:1]
    slots = N_PEER * CAP
    pick = jnp.where(iota((slots, ENTRIES), 0) == sel_row.astype(i32), 1.0, 0.0).astype(bf16)
    wanted = nn(pick, (row + 1).astype(f32).astype(bf16))
    wanted = jnp.where(over, -1.0, wanted)
    req_ref[...] = wanted.astype(bf16).reshape(N_PEER, CAP, 128)


def index_call(scalars, adm, points):
    return pl.pallas_call(
        index_kernel,
        out_shape=(
            jax.ShapeDtypeStruct((ENTRIES, 128), i32),
            jax.ShapeDtypeStruct((N_PEER, CAP, 128), bf16),
            jax.ShapeDtypeStruct((T, 8, LEAF), bf16),
        ),
        in_specs=[SMEM, VMEM, VMEM],
        out_specs=(VMEM,) * 3,
        name="requests",
        compiler_params=LIMIT,
    )(scalars, adm, points)


def coeff_kernel(n_ref, vec_ref, basis_ref, keep_ref, send_ref, held_ref, rows):
    n = n_ref[0]
    same = (iota((64, 256), 0) >> 4) == (iota((64, 256), 1) >> 6)
    for g in range(T // 4):
        lhs = vec_ref[4 * g : 4 * g + 4].reshape(64, HALF)
        held_ref[64 * g : 64 * g + 64] = lhs
        rhs = basis_ref[4 * g : 4 * g + 4].reshape(4 * A, HALF)
        rows[64 * g : 64 * g + 64, :64] = folded(jnp.where(same, nt(lhs, rhs), 0.0))
    for out, first in ((send_ref, (1 - n) * RH), (keep_ref, n * RH)):
        for r in range(0, RH, 2):
            pair = [rows[pl.ds(first + r + k, T, stride=R), :][:, :64] for k in range(2)]
            row, lane = r * A // HALF * T, r * A % HALF
            out[row : row + T, lane : lane + 2 * A] = jnp.concatenate(pair, 1)


def coeff_call(n, vectors, basis):
    return pl.pallas_call(
        coeff_kernel,
        out_shape=(
            jax.ShapeDtypeStruct((2 * T, HALF), f32),
            jax.ShapeDtypeStruct((2 * T, HALF), f32),
            jax.ShapeDtypeStruct((T * R, HALF), bf16),
        ),
        in_specs=[SMEM, VMEM, VMEM],
        out_specs=(VMEM, VMEM, VMEM),
        scratch_shapes=[pltpu.VMEM((T * R, 128), f32)],
        name="coeffs",
        compiler_params=LIMIT,
    )(n, vectors, basis)


def pack_kernel(z_ref, req_ref, *refs):
    *pieces, out_ref, fits_ref, table_ref = refs
    refused = jnp.min(req_ref[:, :8].astype(f32)) < 0.0
    fits_ref[0] = jnp.where(refused, 0, 1)
    for piece, offsets in zip(pieces, OFFSETS):
        for k, offset in enumerate(offsets):
            first = pl.multiple_of(((z_ref[0] + offset) & (N_Z - 1)) * T, T)
            for h in range(2):
                row = (2 * k + h) * T
                table_ref[pl.ds(first, T), h * HALF : (h + 1) * HALF] = piece[row : row + T]
    lanes = iota((CAP, 128), 1).astype(f32) + 1.0
    for r in range(0, N_PEER, 4):
        want = [req_ref[r + k].astype(f32) for k in range(4)]
        hot = [
            jnp.concatenate(
                [jnp.where(w == lanes, 1.0, 0.0), jnp.where(w == lanes + 128.0, 1.0, 0.0)], 1
            )
            for w in want
        ]
        picked = nn(jnp.concatenate(hot, 0).astype(bf16), table_ref[...])
        out_ref[r : r + 4] = picked.astype(bf16).reshape(4, CAP, RH * A)


def pack_call(z, req, pieces):
    return pl.pallas_call(
        pack_kernel,
        out_shape=(
            jax.ShapeDtypeStruct((N_PEER, CAP, RH * A), bf16),
            jax.ShapeDtypeStruct((1,), i32),
        ),
        in_specs=[SMEM] + [VMEM] * (1 + len(pieces)),
        out_specs=(VMEM, SMEM),
        scratch_shapes=[pltpu.VMEM((COLUMN, RH * A), bf16)],
        name="pack",
        compiler_params=LIMIT,
    )(z, req, *pieces)


def couple(picked, couple_ref, out_ref):
    lows = [picked[j * T : (j + 1) * T] for j in range(J)]
    by_rhs = []
    for r in range(RH):
        cols = [low[:, r * A : (r + 1) * A] for low in lows]
        by_rhs.append(jnp.concatenate(cols, 1).astype(bf16))
    row_t = iota((16 * RH, 256), 0) & 15
    col_t = iota((16 * RH, 256), 1) >> 6
    for h in range(2):
        lhs = jnp.concatenate([s[16 * h : 16 * h + 16] for s in by_rhs], 0)
        total = jnp.zeros((16 * RH, A), f32)
        for g in range(4):
            first = 16 * h + 4 * g
            rhs = couple_ref[first : first + 4].reshape(4 * A, J * A)
            total = total + folded(jnp.where(row_t == col_t + 4 * g, nt(lhs, rhs), 0.0))
        total = total.reshape(RH, 16, A)
        for r in range(0, RH, 2):
            pair = jnp.concatenate([total[r], total[r + 1]], 1)
            out_ref[r // 2, 16 * h : 16 * h + 16, :] = pair.astype(bf16)


def select_kernel(sel_ref, got_ref, couple_ref, out_ref):
    slots = N_PEER * CAP
    sel = sel_ref[...]
    lanes = iota((ENTRIES, 128), 1)
    hot = jnp.concatenate(
        [jnp.where(sel == lanes + 128 * k, 1.0, 0.0) for k in range(slots // 128)], 1
    )
    picked = nn(hot.astype(bf16), got_ref[...].reshape(slots, RH * A))
    couple(picked, couple_ref, out_ref)


TC_SHAPE = jax.ShapeDtypeStruct((RH // 2, T, 2 * A), bf16)


def select_call(sel, got, couplings):
    return pl.pallas_call(
        select_kernel,
        out_shape=TC_SHAPE,
        in_specs=[VMEM, VMEM, VMEM],
        out_specs=VMEM,
        name="select",
        compiler_params=LIMIT,
    )(sel, got, couplings)


def couple_kernel(picked_ref, couple_ref, out_ref):
    couple(picked_ref[...], couple_ref, out_ref)


def couple_call(picked, couplings):
    return pl.pallas_call(
        couple_kernel,
        out_shape=TC_SHAPE,
        in_specs=[VMEM, VMEM],
        out_specs=VMEM,
        name="couple",
        compiler_params=LIMIT,
    )(picked, couplings)


def near_kernel(kind, leaves, group, scalar_ref, pts_ref, vec_ref, other_ref, *refs):
    edges, send_refs = (), ()
    refs, kerns = refs[:-group], refs[-group:]
    if kind == "early":
        out_ref, *send_refs = refs
    else:
        *edges, _, out_ref = refs
    count, n = scalar_ref[0], scalar_ref[1]
    own = pl.multiple_of(n * HALF, HALF)
    other = pl.multiple_of((1 - n) * HALF, HALF)

    def values_of(ref, t):
        return ref[pl.ds(pl.multiple_of(t * R, R), R)]

    for ref, t in zip(send_refs, (0, count - 1)):
        ref[:R, pl.ds(own, HALF)] = values_of(vec_ref, t)
        ref[:R, pl.ds(other, HALF)] = values_of(other_ref, t)
        ref[R:] = pts_ref[t]

    def sources(t):
        return (t + T - 1) & (T - 1), t, (t + 1) & (T - 1)

    def taken(t, rows, values):
        if not edges:
            return values
        for k, (u, at) in enumerate(((0, 0), (2, count - 1))):
            halo = [edges[k][rows, pl.ds(h, HALF)] for h in (own, other)]
            values[u] = [jnp.where(t == at, a, b) for a, b in zip(halo, values[u])]
        return values

    def fill(t, kern):
        x = pts_ref[t, :, pl.ds(own, HALF)].astype(f32).T.astype(bf16)
        points = [[pts_ref[u, :, pl.ds(h, HALF)] for h in (own, other)] for u in sources(t)]
        points = taken(t, slice(R, R + 8), points)
        for k in range(3):
            y = jnp.concatenate(points[k], 1)
            for p in range(0, HALF, 32):
                squared = None
                for i in range(3):
                    differ = x[p : p + 32, i : i + 1] - y[i : i + 1, :]
                    differ = differ * differ
                    squared = differ + bf16(soften_sq) if squared is None else squared + differ
                kern[p : p + 32, k * LEAF : (k + 1) * LEAF] = lax.rsqrt(squared)

    def product(t, kern):
        values = [[values_of(vec_ref, u), values_of(other_ref, u)] for u in sources(t)]
        values = taken(t, slice(0, R), values)
        values = jnp.concatenate([v for pair in values for v in pair], 1)
        out_ref[t] = nt(values, kern[...]) * inverse_four_pi

    def leaf(i):
        if not edges:
            return leaves[0] + i
        i = jnp.where(i < leaves[0], i, i + leaves[1] - leaves[0])
        return jnp.where(i < T, i, count - 1)

    steps, group = near_steps(kind, leaves), len(kerns)
    fill(leaf(0), kerns[0])

    def body(i, _):
        for s in range(group):
            fill(leaf(jnp.minimum(group * i + s + 1, steps - 1)), kerns[(s + 1) % group])
            product(leaf(group * i + s), kerns[s])
        return 0

    lax.fori_loop(0, steps // group, body, 0)


def near_steps(kind, leaves):
    return T - leaves[1] + leaves[0] + 1 if kind == "rest" else leaves[1] - leaves[0]


def near_call(kind, leaves, group, args, more=()):
    field = jax.ShapeDtypeStruct((T, R, HALF), f32)
    edge = jax.ShapeDtypeStruct((R + 8, LEAF), bf16)
    outs = (field, edge, edge) if kind == "early" else (field,)
    return pl.pallas_call(
        lambda *refs: near_kernel(kind, leaves, group, *refs),
        out_shape=outs,
        in_specs=[SMEM] + [VMEM] * (len(args) - 1 + len(more)),
        out_specs=(VMEM,) * len(outs),
        scratch_shapes=[pltpu.VMEM((HALF, 3 * LEAF), bf16)] * group,
        input_output_aliases={} if kind == "early" else {len(args) + len(more) - 1: 0},
        cost_estimate=pl.CostEstimate(
            flops=near_steps(kind, leaves) * 200_000_000, bytes_accessed=2_000_000, transcendentals=0
        ),
        name="near",
        compiler_params=LIMIT,
    )(*args, *more)


def final_kernel(scalar_ref, mine_ref, theirs_ref, tgt_ref, near_ref, out_ref, rows):
    count, n = scalar_ref[0], scalar_ref[1]
    for ref, first in ((mine_ref, n * RH), (theirs_ref, (1 - n) * RH)):
        for r in range(RH):
            part = ref[r // 2].astype(f32)[:, (r % 2) * A : (r % 2 + 1) * A]
            rows[pl.ds(first + r, T, stride=R), :] = jnp.concatenate([part, part], 1)
    same = (iota((64, 256), 0) >> 4) == (iota((64, 256), 1) >> 6)
    for g in range(T // 4):
        part = rows[64 * g : 64 * g + 64, :]
        lhs = jnp.where(same, jnp.concatenate([part, part], 1), 0.0).astype(bf16)
        tgt = tgt_ref[4 * g : 4 * g + 4, :, pl.ds(pl.multiple_of(n * HALF, HALF), HALF)]
        far = nn(lhs, tgt.reshape(4 * A, HALF)).reshape(4, R, HALF)
        total = far + near_ref[4 * g : 4 * g + 4]
        live = (iota((4, R, HALF), 0) + 4 * g) < count
        out_ref[4 * g : 4 * g + 4] = jnp.where(live, total, 0.0).astype(bf16)


def final_call(scalars, mine, theirs, tgt, near):
    return pl.pallas_call(
        final_kernel,
        out_shape=jax.ShapeDtypeStruct((T, R, HALF), bf16),
        in_specs=[SMEM] + [VMEM] * 4,
        out_specs=VMEM,
        scratch_shapes=[pltpu.VMEM((T * R, 128), f32)],
        name="final",
        compiler_params=LIMIT,
    )(scalars, mine, theirs, tgt, near)


def shifted(array, axis, by):
    devices = lax.axis_size(axis)
    return lax.ppermute(array, axis, [(i, (i + by) % devices) for i in range(devices)])


def to_all(array, axis):
    copies = jnp.broadcast_to(array[None], (lax.axis_size(axis), *array.shape))
    return lax.all_to_all(copies, axis, split_axis=0, concat_axis=0, tiled=True)


def body(points, vectors, counts, src_basis, tgt_basis, adm_src, couplings):
    n = lax.axis_index("n").astype(i32)
    z = lax.axis_index("z").astype(i32)
    scalars = jnp.stack([counts[0], n])

    keep, send, held = coeff_call(n[None], vectors, src_basis)
    came = shifted(send, "n", 1)
    other = shifted(held, "n", 1)
    sel, req, rows = index_call(scalars, adm_src.T, points.transpose(1, 0, 2))
    asked = lax.all_to_all(req, PEERS, split_axis=0, concat_axis=0, tiled=True)

    coeffs = (keep + came).astype(bf16)
    below = shifted(coeffs, "z", 1)
    above = shifted(coeffs, "z", -1)
    up = shifted(jnp.concatenate([below, coeffs, above]), "z", -3)
    down = shifted(jnp.concatenate([above, coeffs]), "z", 3)
    pieces = coeffs, below, above, up, down

    near_args = (scalars, rows, held, other)
    near, first, last = near_call("early", (2, 10), 8, near_args)
    halos = shifted(last, WIDE, 1), shifted(first, WIDE, -1)
    (near,) = near_call("inner", (10, 30), 10, near_args, (near,))
    (near,) = near_call("rest", (2, 30), 5, near_args, (*halos, near))

    packed, fits = pack_call(z[None], asked, pieces)
    got = lax.all_to_all(packed, PEERS, split_axis=0, concat_axis=0, tiled=True)

    def every(sel, got, pieces, couplings):
        blocks = {
            o % N_Z: jnp.concatenate([p[2 * k * T :][:T], p[(2 * k + 1) * T :][:T]], 1)
            for p, os in zip(pieces, OFFSETS)
            for k, o in enumerate(os)
        }
        twice = jnp.concatenate([blocks[o % N_Z] for o in range(2 * N_Z)])
        table = lax.dynamic_slice_in_dim(twice, (N_Z - z) % N_Z * T, COLUMN, 0)
        whole = to_all(table, PEERS).reshape(N_PEER * COLUMN, RH * A)
        leaf = adm_src.T.reshape(ENTRIES)
        place = ((leaf >> 11) * 8 + ((leaf >> 5) & 7)) * COLUMN + ((leaf >> 8) & 7) * T + (leaf & (T - 1))
        hot = (place[:, None] == jnp.arange(N_PEER * COLUMN, dtype=i32)[None, :]).astype(bf16)
        return couple_call(jnp.dot(hot, whole, preferred_element_type=f32), couplings)

    def some(sel, got, pieces, couplings):
        return select_call(sel, got, couplings)

    mine = lax.cond(fits[0] != 0, some, every, sel, got, pieces, couplings)
    theirs = shifted(mine, "n", 1)
    return final_call(scalars, mine, theirs, tgt_basis, near)


def solution(mesh):
    split = Mesh(
        mesh.devices.reshape(2, 8, 4, 2, mesh.shape["narrow"]), ("y", "z", "x", "c", "n")
    )
    in_specs = (
        P(WIDE, None, None),
        P(WIDE, None, "n"),
        P(WIDE),
        P(WIDE, None, "n"),
        P(WIDE, None, None),
        P(WIDE, None),
        P(WIDE, None, None),
    )
    out_specs = P(WIDE, None, "n")
    return jax.shard_map(body, mesh=split, in_specs=in_specs, out_specs=out_specs, check_vma=False)
```

```python
import math

import jax
import jax.numpy as jnp
from jax import lax
from jax.experimental import pallas as pl
from jax.experimental.pallas import tpu as pltpu
from jax.sharding import Mesh
from jax.sharding import PartitionSpec as P


WIDE = ("y", "z", "x", "c")
PEERS = ("y", "x", "c")

inverse_four_pi = 1.0 / (4.0 * math.pi)
soften_sq = 0.0025

T, R, A, J, HALF, LEAF = 32, 16, 64, 8, 256, 512
RH = R // 2
N_Z, N_PEER = 8, 16
CAP = 40
ENTRIES = T * J
OFFSETS = (0,), (2,), (-2,), (4,), (1, 3), (-1, -3)
COLUMN = N_Z * T
bf16, f32, i32 = jnp.bfloat16, jnp.float32, jnp.int32

VMEM = pl.BlockSpec(memory_space=pltpu.VMEM)
SMEM = pl.BlockSpec(memory_space=pltpu.SMEM)
LIMIT = pltpu.CompilerParams(vmem_limit_bytes=20 * 2**20)


def nt(a, b):
    return lax.dot_general(a, b, (((1,), (1,)), ((), ())), preferred_element_type=f32)


def nn(a, b):
    return lax.dot_general(a, b, (((1,), (0,)), ((), ())), preferred_element_type=f32)


def iota(shape, dim):
    return lax.broadcasted_iota(i32, shape, dim)


def folded(wide):
    two = wide[:, :128] + wide[:, 128:]
    return two[:, :64] + two[:, 64:]


def index_kernel(scalar_ref, adm_ref, pts_ref, sel_ref, req_ref, rows_ref):
    pts = pts_ref[...].astype(f32)
    blank = jnp.zeros((5, LEAF), f32)
    for t in range(T):
        rows_ref[t] = jnp.concatenate([pts[i, t : t + 1] for i in range(3)] + [blank], 0).astype(bf16)
    count = scalar_ref[0]
    adm = jnp.concatenate([adm_ref[...].astype(f32), jnp.zeros((8, 96), f32)], 1).T
    leaf = jnp.concatenate(
        [jnp.broadcast_to(adm[:T, j : j + 1], (T, 128)) for j in range(J)], 0
    ).astype(i32)
    live = (iota((ENTRIES, 128), 0) & (T - 1)) < count
    column = (leaf >> 11) * 8 + ((leaf >> 5) & 7)
    row = ((leaf >> 8) & 7) * T + (leaf & (T - 1))
    member = jnp.where((column == iota((ENTRIES, 128), 1)) & live, 1.0, 0.0)
    below = jnp.where(iota((ENTRIES, ENTRIES), 0) > iota((ENTRIES, ENTRIES), 1), 1.0, 0.0)
    rank = nn(below.astype(bf16), member.astype(bf16))
    place = jnp.sum(member * rank, axis=1, keepdims=True)
    over = jnp.max(place) > CAP - 0.5
    place = jnp.broadcast_to(place, (ENTRIES, 128))
    fits = live & (place < CAP - 0.5)
    sel = jnp.where(fits, column * CAP + place.astype(i32), -1)
    sel_ref[...] = sel
    sel_row = sel.astype(f32).T[:1]
    slots = N_PEER * CAP
    pick = jnp.where(iota((slots, ENTRIES), 0) == sel_row.astype(i32), 1.0, 0.0).astype(bf16)
    wanted = nn(pick, (row + 1).astype(f32).astype(bf16))
    wanted = jnp.where(over, -1.0, wanted)
    req_ref[...] = wanted.astype(bf16).reshape(N_PEER, CAP, 128)


def index_call(scalars, adm, points):
    return pl.pallas_call(
        index_kernel,
        out_shape=(
            jax.ShapeDtypeStruct((ENTRIES, 128), i32),
            jax.ShapeDtypeStruct((N_PEER, CAP, 128), bf16),
            jax.ShapeDtypeStruct((T, 8, LEAF), bf16),
        ),
        in_specs=[SMEM, VMEM, VMEM],
        out_specs=(VMEM,) * 3,
        name="requests",
        compiler_params=LIMIT,
    )(scalars, adm, points)


def coeff_kernel(n_ref, vec_ref, basis_ref, keep_ref, send_ref, held_ref, rows):
    n = n_ref[0]
    same = (iota((64, 256), 0) >> 4) == (iota((64, 256), 1) >> 6)
    for g in range(T // 4):
        lhs = vec_ref[4 * g : 4 * g + 4].reshape(64, HALF)
        held_ref[64 * g : 64 * g + 64] = lhs
        rhs = basis_ref[4 * g : 4 * g + 4].reshape(4 * A, HALF)
        rows[64 * g : 64 * g + 64, :64] = folded(jnp.where(same, nt(lhs, rhs), 0.0))
    for out, first in ((send_ref, (1 - n) * RH), (keep_ref, n * RH)):
        for r in range(0, RH, 2):
            pair = [rows[pl.ds(first + r + k, T, stride=R), :][:, :64] for k in range(2)]
            row, lane = r * A // HALF * T, r * A % HALF
            out[row : row + T, lane : lane + 2 * A] = jnp.concatenate(pair, 1)


def coeff_call(n, vectors, basis):
    return pl.pallas_call(
        coeff_kernel,
        out_shape=(
            jax.ShapeDtypeStruct((2 * T, HALF), f32),
            jax.ShapeDtypeStruct((2 * T, HALF), f32),
            jax.ShapeDtypeStruct((T * R, HALF), bf16),
        ),
        in_specs=[SMEM, VMEM, VMEM],
        out_specs=(VMEM, VMEM, VMEM),
        scratch_shapes=[pltpu.VMEM((T * R, 128), f32)],
        name="coeffs",
        compiler_params=LIMIT,
    )(n, vectors, basis)


def pack_kernel(z_ref, req_ref, *refs):
    *pieces, out_ref, fits_ref, table_ref = refs
    refused = jnp.min(req_ref[:, :8].astype(f32)) < 0.0
    fits_ref[0] = jnp.where(refused, 0, 1)
    for piece, offsets in zip(pieces, OFFSETS):
        for k, offset in enumerate(offsets):
            first = pl.multiple_of(((z_ref[0] + offset) & (N_Z - 1)) * T, T)
            for h in range(2):
                row = (2 * k + h) * T
                table_ref[pl.ds(first, T), h * HALF : (h + 1) * HALF] = piece[row : row + T]
    lanes = iota((CAP, 128), 1).astype(f32) + 1.0
    for r in range(0, N_PEER, 4):
        want = [req_ref[r + k].astype(f32) for k in range(4)]
        hot = [
            jnp.concatenate(
                [jnp.where(w == lanes, 1.0, 0.0), jnp.where(w == lanes + 128.0, 1.0, 0.0)], 1
            )
            for w in want
        ]
        picked = nn(jnp.concatenate(hot, 0).astype(bf16), table_ref[...])
        out_ref[r : r + 4] = picked.astype(bf16).reshape(4, CAP, RH * A)


def pack_call(z, req, pieces):
    return pl.pallas_call(
        pack_kernel,
        out_shape=(
            jax.ShapeDtypeStruct((N_PEER, CAP, RH * A), bf16),
            jax.ShapeDtypeStruct((1,), i32),
        ),
        in_specs=[SMEM] + [VMEM] * (1 + len(pieces)),
        out_specs=(VMEM, SMEM),
        scratch_shapes=[pltpu.VMEM((COLUMN, RH * A), bf16)],
        name="pack",
        compiler_params=LIMIT,
    )(z, req, *pieces)


def couple(picked, couple_ref, out_ref):
    lows = [picked[j * T : (j + 1) * T] for j in range(J)]
    by_rhs = []
    for r in range(RH):
        cols = [low[:, r * A : (r + 1) * A] for low in lows]
        by_rhs.append(jnp.concatenate(cols, 1).astype(bf16))
    row_t = iota((16 * RH, 256), 0) & 15
    col_t = iota((16 * RH, 256), 1) >> 6
    for h in range(2):
        lhs = jnp.concatenate([s[16 * h : 16 * h + 16] for s in by_rhs], 0)
        total = jnp.zeros((16 * RH, A), f32)
        for g in range(4):
            first = 16 * h + 4 * g
            rhs = couple_ref[first : first + 4].reshape(4 * A, J * A)
            total = total + folded(jnp.where(row_t == col_t + 4 * g, nt(lhs, rhs), 0.0))
        total = total.reshape(RH, 16, A)
        for r in range(0, RH, 2):
            pair = jnp.concatenate([total[r], total[r + 1]], 1)
            out_ref[r // 2, 16 * h : 16 * h + 16, :] = pair.astype(bf16)


def select_kernel(sel_ref, got_ref, couple_ref, out_ref):
    slots = N_PEER * CAP
    sel = sel_ref[...]
    lanes = iota((ENTRIES, 128), 1)
    hot = jnp.concatenate(
        [jnp.where(sel == lanes + 128 * k, 1.0, 0.0) for k in range(slots // 128)], 1
    )
    picked = nn(hot.astype(bf16), got_ref[...].reshape(slots, RH * A))
    couple(picked, couple_ref, out_ref)


TC_SHAPE = jax.ShapeDtypeStruct((RH // 2, T, 2 * A), bf16)


def select_call(sel, got, couplings):
    return pl.pallas_call(
        select_kernel,
        out_shape=TC_SHAPE,
        in_specs=[VMEM, VMEM, VMEM],
        out_specs=VMEM,
        name="select",
        compiler_params=LIMIT,
    )(sel, got, couplings)


def couple_kernel(picked_ref, couple_ref, out_ref):
    couple(picked_ref[...], couple_ref, out_ref)


def couple_call(picked, couplings):
    return pl.pallas_call(
        couple_kernel,
        out_shape=TC_SHAPE,
        in_specs=[VMEM, VMEM],
        out_specs=VMEM,
        name="couple",
        compiler_params=LIMIT,
    )(picked, couplings)


def near_kernel(kind, leaves, group, scalar_ref, pts_ref, vec_ref, other_ref, *refs):
    edges, send_refs = (), ()
    refs, kerns = refs[:-group], refs[-group:]
    if kind == "early":
        out_ref, *send_refs = refs
    else:
        *edges, _, out_ref = refs
    count, n = scalar_ref[0], scalar_ref[1]
    own = pl.multiple_of(n * HALF, HALF)
    other = pl.multiple_of((1 - n) * HALF, HALF)

    def values_of(ref, t):
        return ref[pl.ds(pl.multiple_of(t * R, R), R)]

    for ref, t in zip(send_refs, (0, count - 1)):
        ref[:R, pl.ds(own, HALF)] = values_of(vec_ref, t)
        ref[:R, pl.ds(other, HALF)] = values_of(other_ref, t)
        ref[R:] = pts_ref[t]

    def sources(t):
        return (t + T - 1) & (T - 1), t, (t + 1) & (T - 1)

    def taken(t, rows, values):
        if not edges:
            return values
        for k, (u, at) in enumerate(((0, 0), (2, count - 1))):
            halo = [edges[k][rows, pl.ds(h, HALF)] for h in (own, other)]
            values[u] = [jnp.where(t == at, a, b) for a, b in zip(halo, values[u])]
        return values

    def fill(t, kern):
        x = pts_ref[t, :, pl.ds(own, HALF)].astype(f32).T.astype(bf16)
        points = [[pts_ref[u, :, pl.ds(h, HALF)] for h in (own, other)] for u in sources(t)]
        points = taken(t, slice(R, R + 8), points)
        for k in range(3):
            y = jnp.concatenate(points[k], 1)
            for p in range(0, HALF, 32):
                squared = None
                for i in range(3):
                    differ = x[p : p + 32, i : i + 1] - y[i : i + 1, :]
                    differ = differ * differ
                    squared = differ + bf16(soften_sq) if squared is None else squared + differ
                kern[p : p + 32, k * LEAF : (k + 1) * LEAF] = lax.rsqrt(squared)

    def product(t, kern):
        values = [[values_of(vec_ref, u), values_of(other_ref, u)] for u in sources(t)]
        values = taken(t, slice(0, R), values)
        values = jnp.concatenate([v for pair in values for v in pair], 1)
        out_ref[t] = nt(values, kern[...]) * inverse_four_pi

    def leaf(i):
        if not edges:
            return leaves[0] + i
        i = jnp.where(i < leaves[0], i, i + leaves[1] - leaves[0])
        return jnp.where(i < T, i, count - 1)

    steps, group = near_steps(kind, leaves), len(kerns)
    fill(leaf(0), kerns[0])

    def body(i, _):
        for s in range(group):
            fill(leaf(jnp.minimum(group * i + s + 1, steps - 1)), kerns[(s + 1) % group])
            product(leaf(group * i + s), kerns[s])
        return 0

    lax.fori_loop(0, steps // group, body, 0)


def near_steps(kind, leaves):
    return T - leaves[1] + leaves[0] + 1 if kind == "rest" else leaves[1] - leaves[0]


def near_call(kind, leaves, group, args, more=()):
    field = jax.ShapeDtypeStruct((T, R, HALF), f32)
    edge = jax.ShapeDtypeStruct((R + 8, LEAF), bf16)
    outs = (field, edge, edge) if kind == "early" else (field,)
    return pl.pallas_call(
        lambda *refs: near_kernel(kind, leaves, group, *refs),
        out_shape=outs,
        in_specs=[SMEM] + [VMEM] * (len(args) - 1 + len(more)),
        out_specs=(VMEM,) * len(outs),
        scratch_shapes=[pltpu.VMEM((HALF, 3 * LEAF), bf16)] * group,
        input_output_aliases={} if kind == "early" else {len(args) + len(more) - 1: 0},
        cost_estimate=pl.CostEstimate(
            flops=near_steps(kind, leaves) * 200_000_000, bytes_accessed=2_000_000, transcendentals=0
        ),
        name="near",
        compiler_params=LIMIT,
    )(*args, *more)


def final_kernel(scalar_ref, mine_ref, theirs_ref, tgt_ref, near_ref, out_ref, rows):
    count, n = scalar_ref[0], scalar_ref[1]
    for ref, first in ((mine_ref, n * RH), (theirs_ref, (1 - n) * RH)):
        for r in range(RH):
            part = ref[r // 2].astype(f32)[:, (r % 2) * A : (r % 2 + 1) * A]
            rows[pl.ds(first + r, T, stride=R), :] = jnp.concatenate([part, part], 1)
    same = (iota((64, 256), 0) >> 4) == (iota((64, 256), 1) >> 6)
    for g in range(T // 4):
        part = rows[64 * g : 64 * g + 64, :]
        lhs = jnp.where(same, jnp.concatenate([part, part], 1), 0.0).astype(bf16)
        tgt = tgt_ref[4 * g : 4 * g + 4, :, pl.ds(pl.multiple_of(n * HALF, HALF), HALF)]
        far = nn(lhs, tgt.reshape(4 * A, HALF)).reshape(4, R, HALF)
        total = far + near_ref[4 * g : 4 * g + 4]
        live = (iota((4, R, HALF), 0) + 4 * g) < count
        out_ref[4 * g : 4 * g + 4] = jnp.where(live, total, 0.0).astype(bf16)


def final_call(scalars, mine, theirs, tgt, near):
    return pl.pallas_call(
        final_kernel,
        out_shape=jax.ShapeDtypeStruct((T, R, HALF), bf16),
        in_specs=[SMEM] + [VMEM] * 4,
        out_specs=VMEM,
        scratch_shapes=[pltpu.VMEM((T * R, 128), f32)],
        name="final",
        compiler_params=LIMIT,
    )(scalars, mine, theirs, tgt, near)


def shifted(array, axis, by):
    devices = lax.axis_size(axis)
    return lax.ppermute(array, axis, [(i, (i + by) % devices) for i in range(devices)])


def to_all(array, axis):
    copies = jnp.broadcast_to(array[None], (lax.axis_size(axis), *array.shape))
    return lax.all_to_all(copies, axis, split_axis=0, concat_axis=0, tiled=True)


def body(points, vectors, counts, src_basis, tgt_basis, adm_src, couplings):
    n = lax.axis_index("n").astype(i32)
    z = lax.axis_index("z").astype(i32)
    scalars = jnp.stack([counts[0], n])

    keep, send, held = coeff_call(n[None], vectors, src_basis)
    came = shifted(send, "n", 1)
    other = shifted(held, "n", 1)
    sel, req, rows = index_call(scalars, adm_src.T, points.transpose(1, 0, 2))
    asked = lax.all_to_all(req, PEERS, split_axis=0, concat_axis=0, tiled=True)

    coeffs = (keep + came).astype(bf16)
    up = shifted(coeffs, "z", -2)
    down = shifted(coeffs, "z", 2)
    across = shifted(coeffs, "z", 4)
    odd_up = shifted(jnp.concatenate([coeffs, up]), "z", -1)
    odd_down = shifted(jnp.concatenate([coeffs, down]), "z", 1)
    pieces = coeffs, up, down, across, odd_up, odd_down

    near_args = (scalars, rows, held, other)
    near, first, last = near_call("early", (2, 10), 8, near_args)
    halos = shifted(last, WIDE, 1), shifted(first, WIDE, -1)
    (near,) = near_call("inner", (10, 30), 10, near_args, (near,))
    (near,) = near_call("rest", (2, 30), 5, near_args, (*halos, near))

    packed, fits = pack_call(z[None], asked, pieces)
    got = lax.all_to_all(packed, PEERS, split_axis=0, concat_axis=0, tiled=True)

    def every(sel, got, pieces, couplings):
        blocks = {
            o % N_Z: jnp.concatenate([p[2 * k * T :][:T], p[(2 * k + 1) * T :][:T]], 1)
            for p, os in zip(pieces, OFFSETS)
            for k, o in enumerate(os)
        }
        twice = jnp.concatenate([blocks[o % N_Z] for o in range(2 * N_Z)])
        table = lax.dynamic_slice_in_dim(twice, (N_Z - z) % N_Z * T, COLUMN, 0)
        whole = to_all(table, PEERS).reshape(N_PEER * COLUMN, RH * A)
        leaf = adm_src.T.reshape(ENTRIES)
        place = ((leaf >> 11) * 8 + ((leaf >> 5) & 7)) * COLUMN + ((leaf >> 8) & 7) * T + (leaf & (T - 1))
        hot = (place[:, None] == jnp.arange(N_PEER * COLUMN, dtype=i32)[None, :]).astype(bf16)
        return couple_call(jnp.dot(hot, whole, preferred_element_type=f32), couplings)

    def some(sel, got, pieces, couplings):
        return select_call(sel, got, couplings)

    mine = lax.cond(fits[0] != 0, some, every, sel, got, pieces, couplings)
    theirs = shifted(mine, "n", 1)
    return final_call(scalars, mine, theirs, tgt_basis, near)


def solution(mesh):
    split = Mesh(
        mesh.devices.reshape(2, 8, 4, 2, mesh.shape["narrow"]), ("y", "z", "x", "c", "n")
    )
    in_specs = (
        P(WIDE, None, None),
        P(WIDE, None, "n"),
        P(WIDE),
        P(WIDE, None, "n"),
        P(WIDE, None, None),
        P(WIDE, None),
        P(WIDE, None, None),
    )
    out_specs = P(WIDE, None, "n")
    return jax.shard_map(body, mesh=split, in_specs=in_specs, out_specs=out_specs, check_vma=False)
```

```python
import math

import jax
import jax.numpy as jnp
from jax import lax
from jax.experimental import pallas as pl
from jax.experimental.pallas import tpu as pltpu
from jax.sharding import Mesh
from jax.sharding import PartitionSpec as P


WIDE = ("y", "z", "x", "c")
PEERS = ("y", "x", "c")

inverse_four_pi = 1.0 / (4.0 * math.pi)
soften_sq = 0.0025

T, R, A, J, HALF, LEAF = 32, 16, 64, 8, 256, 512
RH = R // 2
N_Z, N_PEER = 8, 16
CAP = 40
ENTRIES = T * J
OFFSETS = (0,), (2,), (-2,), (4,), (1, 3), (-1, -3)
COLUMN = N_Z * T
bf16, f32, i32 = jnp.bfloat16, jnp.float32, jnp.int32

VMEM = pl.BlockSpec(memory_space=pltpu.VMEM)
SMEM = pl.BlockSpec(memory_space=pltpu.SMEM)
LIMIT = pltpu.CompilerParams(vmem_limit_bytes=20 * 2**20)


def nt(a, b):
    return lax.dot_general(a, b, (((1,), (1,)), ((), ())), preferred_element_type=f32)


def nn(a, b):
    return lax.dot_general(a, b, (((1,), (0,)), ((), ())), preferred_element_type=f32)


def iota(shape, dim):
    return lax.broadcasted_iota(i32, shape, dim)


def folded(wide):
    two = wide[:, :128] + wide[:, 128:]
    return two[:, :64] + two[:, 64:]


def index_kernel(scalar_ref, adm_ref, pts_ref, sel_ref, req_ref, rows_ref):
    pts = pts_ref[...].astype(f32)
    blank = jnp.zeros((5, LEAF), f32)
    for t in range(T):
        rows_ref[t] = jnp.concatenate([pts[i, t : t + 1] for i in range(3)] + [blank], 0).astype(bf16)
    count = scalar_ref[0]
    adm = jnp.concatenate([adm_ref[...].astype(f32), jnp.zeros((8, 96), f32)], 1).T
    leaf = jnp.concatenate(
        [jnp.broadcast_to(adm[:T, j : j + 1], (T, 128)) for j in range(J)], 0
    ).astype(i32)
    live = (iota((ENTRIES, 128), 0) & (T - 1)) < count
    column = (leaf >> 11) * 8 + ((leaf >> 5) & 7)
    row = ((leaf >> 8) & 7) * T + (leaf & (T - 1))
    member = jnp.where((column == iota((ENTRIES, 128), 1)) & live, 1.0, 0.0)
    below = jnp.where(iota((ENTRIES, ENTRIES), 0) > iota((ENTRIES, ENTRIES), 1), 1.0, 0.0)
    rank = nn(below.astype(bf16), member.astype(bf16))
    place = jnp.sum(member * rank, axis=1, keepdims=True)
    over = jnp.max(place) > CAP - 0.5
    place = jnp.broadcast_to(place, (ENTRIES, 128))
    fits = live & (place < CAP - 0.5)
    sel = jnp.where(fits, column * CAP + place.astype(i32), -1)
    sel_ref[...] = sel
    sel_row = sel.astype(f32).T[:1]
    slots = N_PEER * CAP
    pick = jnp.where(iota((slots, ENTRIES), 0) == sel_row.astype(i32), 1.0, 0.0).astype(bf16)
    wanted = nn(pick, (row + 1).astype(f32).astype(bf16))
    wanted = jnp.where(over, -1.0, wanted)
    req_ref[...] = wanted.astype(bf16).reshape(N_PEER, CAP, 128)


def index_call(scalars, adm, points):
    return pl.pallas_call(
        index_kernel,
        out_shape=(
            jax.ShapeDtypeStruct((ENTRIES, 128), i32),
            jax.ShapeDtypeStruct((N_PEER, CAP, 128), bf16),
            jax.ShapeDtypeStruct((T, 8, LEAF), bf16),
        ),
        in_specs=[SMEM, VMEM, VMEM],
        out_specs=(VMEM,) * 3,
        name="requests",
        compiler_params=LIMIT,
    )(scalars, adm, points)


def coeff_kernel(n_ref, vec_ref, basis_ref, keep_ref, send_ref, held_ref, rows):
    n = n_ref[0]
    same = (iota((64, 256), 0) >> 4) == (iota((64, 256), 1) >> 6)
    for g in range(T // 4):
        lhs = vec_ref[4 * g : 4 * g + 4].reshape(64, HALF)
        held_ref[64 * g : 64 * g + 64] = lhs
        rhs = basis_ref[4 * g : 4 * g + 4].reshape(4 * A, HALF)
        rows[64 * g : 64 * g + 64, :64] = folded(jnp.where(same, nt(lhs, rhs), 0.0))
    for out, first in ((send_ref, (1 - n) * RH), (keep_ref, n * RH)):
        for r in range(0, RH, 2):
            pair = [rows[pl.ds(first + r + k, T, stride=R), :][:, :64] for k in range(2)]
            row, lane = r * A // HALF * T, r * A % HALF
            out[row : row + T, lane : lane + 2 * A] = jnp.concatenate(pair, 1)


def coeff_call(n, vectors, basis):
    return pl.pallas_call(
        coeff_kernel,
        out_shape=(
            jax.ShapeDtypeStruct((2 * T, HALF), f32),
            jax.ShapeDtypeStruct((2 * T, HALF), f32),
            jax.ShapeDtypeStruct((T * R, HALF), bf16),
        ),
        in_specs=[SMEM, VMEM, VMEM],
        out_specs=(VMEM, VMEM, VMEM),
        scratch_shapes=[pltpu.VMEM((T * R, 128), f32)],
        name="coeffs",
        compiler_params=LIMIT,
    )(n, vectors, basis)


def pack_kernel(z_ref, req_ref, *refs):
    *pieces, out_ref, fits_ref, table_ref = refs
    refused = jnp.min(req_ref[:, :8].astype(f32)) < 0.0
    fits_ref[0] = jnp.where(refused, 0, 1)
    for piece, offsets in zip(pieces, OFFSETS):
        for k, offset in enumerate(offsets):
            first = pl.multiple_of(((z_ref[0] + offset) & (N_Z - 1)) * T, T)
            for h in range(2):
                row = (2 * k + h) * T
                table_ref[pl.ds(first, T), h * HALF : (h + 1) * HALF] = piece[row : row + T]
    lanes = iota((CAP, 128), 1).astype(f32) + 1.0
    for r in range(0, N_PEER, 4):
        want = [req_ref[r + k].astype(f32) for k in range(4)]
        hot = [
            jnp.concatenate(
                [jnp.where(w == lanes, 1.0, 0.0), jnp.where(w == lanes + 128.0, 1.0, 0.0)], 1
            )
            for w in want
        ]
        picked = nn(jnp.concatenate(hot, 0).astype(bf16), table_ref[...])
        out_ref[r : r + 4] = picked.astype(bf16).reshape(4, CAP, RH * A)


def pack_call(z, req, pieces):
    return pl.pallas_call(
        pack_kernel,
        out_shape=(
            jax.ShapeDtypeStruct((N_PEER, CAP, RH * A), bf16),
            jax.ShapeDtypeStruct((1,), i32),
        ),
        in_specs=[SMEM] + [VMEM] * (1 + len(pieces)),
        out_specs=(VMEM, SMEM),
        scratch_shapes=[pltpu.VMEM((COLUMN, RH * A), bf16)],
        name="pack",
        compiler_params=LIMIT,
    )(z, req, *pieces)


def couple(picked, couple_ref, out_ref):
    lows = [picked[j * T : (j + 1) * T] for j in range(J)]
    by_rhs = []
    for r in range(RH):
        cols = [low[:, r * A : (r + 1) * A] for low in lows]
        by_rhs.append(jnp.concatenate(cols, 1).astype(bf16))
    row_t = iota((16 * RH, 256), 0) & 15
    col_t = iota((16 * RH, 256), 1) >> 6
    for h in range(2):
        lhs = jnp.concatenate([s[16 * h : 16 * h + 16] for s in by_rhs], 0)
        total = jnp.zeros((16 * RH, A), f32)
        for g in range(4):
            first = 16 * h + 4 * g
            rhs = couple_ref[first : first + 4].reshape(4 * A, J * A)
            total = total + folded(jnp.where(row_t == col_t + 4 * g, nt(lhs, rhs), 0.0))
        total = total.reshape(RH, 16, A)
        for r in range(0, RH, 2):
            pair = jnp.concatenate([total[r], total[r + 1]], 1)
            out_ref[r // 2, 16 * h : 16 * h + 16, :] = pair.astype(bf16)


def select_kernel(sel_ref, got_ref, couple_ref, out_ref):
    slots = N_PEER * CAP
    sel = sel_ref[...]
    lanes = iota((ENTRIES, 128), 1)
    hot = jnp.concatenate(
        [jnp.where(sel == lanes + 128 * k, 1.0, 0.0) for k in range(slots // 128)], 1
    )
    picked = nn(hot.astype(bf16), got_ref[...].reshape(slots, RH * A))
    couple(picked, couple_ref, out_ref)


TC_SHAPE = jax.ShapeDtypeStruct((RH // 2, T, 2 * A), bf16)


def select_call(sel, got, couplings):
    return pl.pallas_call(
        select_kernel,
        out_shape=TC_SHAPE,
        in_specs=[VMEM, VMEM, VMEM],
        out_specs=VMEM,
        name="select",
        compiler_params=LIMIT,
    )(sel, got, couplings)


def couple_kernel(picked_ref, couple_ref, out_ref):
    couple(picked_ref[...], couple_ref, out_ref)


def couple_call(picked, couplings):
    return pl.pallas_call(
        couple_kernel,
        out_shape=TC_SHAPE,
        in_specs=[VMEM, VMEM],
        out_specs=VMEM,
        name="couple",
        compiler_params=LIMIT,
    )(picked, couplings)


def near_kernel(kind, leaves, group, scalar_ref, pts_ref, vec_ref, other_ref, *refs):
    edges, send_refs = (), ()
    refs, kerns = refs[:-group], refs[-group:]
    if kind == "early":
        out_ref, *send_refs = refs
    else:
        *edges, _, out_ref = refs
    count, n = scalar_ref[0], scalar_ref[1]
    own = pl.multiple_of(n * HALF, HALF)
    other = pl.multiple_of((1 - n) * HALF, HALF)

    def values_of(ref, t):
        return ref[pl.ds(pl.multiple_of(t * R, R), R)]

    for ref, t in zip(send_refs, (0, count - 1)):
        ref[:R, pl.ds(own, HALF)] = values_of(vec_ref, t)
        ref[:R, pl.ds(other, HALF)] = values_of(other_ref, t)
        ref[R:] = pts_ref[t]

    def sources(t):
        return (t + T - 1) & (T - 1), t, (t + 1) & (T - 1)

    def taken(t, rows, values):
        if not edges:
            return values
        for k, (u, at) in enumerate(((0, 0), (2, count - 1))):
            halo = [edges[k][rows, pl.ds(h, HALF)] for h in (own, other)]
            values[u] = [jnp.where(t == at, a, b) for a, b in zip(halo, values[u])]
        return values

    def fill(t, kern):
        x = pts_ref[t, :, pl.ds(own, HALF)].astype(f32).T.astype(bf16)
        points = [[pts_ref[u, :, pl.ds(h, HALF)] for h in (own, other)] for u in sources(t)]
        points = taken(t, slice(R, R + 8), points)
        for k in range(3):
            y = jnp.concatenate(points[k], 1)
            for p in range(0, HALF, 32):
                squared = None
                for i in range(3):
                    differ = x[p : p + 32, i : i + 1] - y[i : i + 1, :]
                    differ = differ * differ
                    squared = differ + bf16(soften_sq) if squared is None else squared + differ
                kern[p : p + 32, k * LEAF : (k + 1) * LEAF] = lax.rsqrt(squared)

    def product(t, kern):
        values = [[values_of(vec_ref, u), values_of(other_ref, u)] for u in sources(t)]
        values = taken(t, slice(0, R), values)
        values = jnp.concatenate([v for pair in values for v in pair], 1)
        out_ref[t] = nt(values, kern[...]) * inverse_four_pi

    def leaf(i):
        if not edges:
            return leaves[0] + i
        i = jnp.where(i < leaves[0], i, i + leaves[1] - leaves[0])
        return jnp.where(i < T, i, count - 1)

    steps, group = near_steps(kind, leaves), len(kerns)
    fill(leaf(0), kerns[0])

    def body(i, ends):
        for s in range(group):
            if not ends or s < group - 1:
                fill(leaf(group * i + s + 1), kerns[(s + 1) % group])
            product(leaf(group * i + s), kerns[s])
        return 0

    whole = steps // group - 1
    if whole:
        lax.fori_loop(0, whole, lambda i, _: body(i, False), 0)
    lax.fori_loop(whole, whole + 1, lambda i, _: body(i, True), 0)


def near_steps(kind, leaves):
    return T - leaves[1] + leaves[0] + 1 if kind == "rest" else leaves[1] - leaves[0]


def near_call(kind, leaves, group, args, more=()):
    field = jax.ShapeDtypeStruct((T, R, HALF), f32)
    edge = jax.ShapeDtypeStruct((R + 8, LEAF), bf16)
    outs = (field, edge, edge) if kind == "early" else (field,)
    return pl.pallas_call(
        lambda *refs: near_kernel(kind, leaves, group, *refs),
        out_shape=outs,
        in_specs=[SMEM] + [VMEM] * (len(args) - 1 + len(more)),
        out_specs=(VMEM,) * len(outs),
        scratch_shapes=[pltpu.VMEM((HALF, 3 * LEAF), bf16)] * group,
        input_output_aliases={} if kind == "early" else {len(args) + len(more) - 1: 0},
        cost_estimate=pl.CostEstimate(
            flops=near_steps(kind, leaves) * 200_000_000, bytes_accessed=2_000_000, transcendentals=0
        ),
        name="near",
        compiler_params=LIMIT,
    )(*args, *more)


def final_kernel(scalar_ref, mine_ref, theirs_ref, tgt_ref, near_ref, out_ref, rows):
    count, n = scalar_ref[0], scalar_ref[1]
    for ref, first in ((mine_ref, n * RH), (theirs_ref, (1 - n) * RH)):
        for r in range(RH):
            part = ref[r // 2].astype(f32)[:, (r % 2) * A : (r % 2 + 1) * A]
            rows[pl.ds(first + r, T, stride=R), :] = jnp.concatenate([part, part], 1)
    same = (iota((64, 256), 0) >> 4) == (iota((64, 256), 1) >> 6)
    for g in range(T // 4):
        part = rows[64 * g : 64 * g + 64, :]
        lhs = jnp.where(same, jnp.concatenate([part, part], 1), 0.0).astype(bf16)
        tgt = tgt_ref[4 * g : 4 * g + 4, :, pl.ds(pl.multiple_of(n * HALF, HALF), HALF)]
        far = nn(lhs, tgt.reshape(4 * A, HALF)).reshape(4, R, HALF)
        total = far + near_ref[4 * g : 4 * g + 4]
        live = (iota((4, R, HALF), 0) + 4 * g) < count
        out_ref[4 * g : 4 * g + 4] = jnp.where(live, total, 0.0).astype(bf16)


def final_call(scalars, mine, theirs, tgt, near):
    return pl.pallas_call(
        final_kernel,
        out_shape=jax.ShapeDtypeStruct((T, R, HALF), bf16),
        in_specs=[SMEM] + [VMEM] * 4,
        out_specs=VMEM,
        scratch_shapes=[pltpu.VMEM((T * R, 128), f32)],
        name="final",
        compiler_params=LIMIT,
    )(scalars, mine, theirs, tgt, near)


def shifted(array, axis, by):
    devices = lax.axis_size(axis)
    return lax.ppermute(array, axis, [(i, (i + by) % devices) for i in range(devices)])


def to_all(array, axis):
    copies = jnp.broadcast_to(array[None], (lax.axis_size(axis), *array.shape))
    return lax.all_to_all(copies, axis, split_axis=0, concat_axis=0, tiled=True)


def body(points, vectors, counts, src_basis, tgt_basis, adm_src, couplings):
    n = lax.axis_index("n").astype(i32)
    z = lax.axis_index("z").astype(i32)
    scalars = jnp.stack([counts[0], n])

    keep, send, held = coeff_call(n[None], vectors, src_basis)
    came = shifted(send, "n", 1)
    other = shifted(held, "n", 1)
    sel, req, rows = index_call(scalars, adm_src.T, points.transpose(1, 0, 2))
    asked = lax.all_to_all(req, PEERS, split_axis=0, concat_axis=0, tiled=True)

    coeffs = (keep + came).astype(bf16)
    up = shifted(coeffs, "z", -2)
    down = shifted(coeffs, "z", 2)
    across = shifted(coeffs, "z", 4)
    odd_up = shifted(jnp.concatenate([coeffs, up]), "z", -1)
    odd_down = shifted(jnp.concatenate([coeffs, down]), "z", 1)
    pieces = coeffs, up, down, across, odd_up, odd_down

    near_args = (scalars, rows, held, other)
    near, first, last = near_call("early", (3, 11), 8, near_args)
    halos = shifted(last, WIDE, 1), shifted(first, WIDE, -1)
    (near,) = near_call("inner", (11, 29), 9, near_args, (near,))
    (near,) = near_call("rest", (3, 29), 7, near_args, (*halos, near))

    packed, fits = pack_call(z[None], asked, pieces)
    got = lax.all_to_all(packed, PEERS, split_axis=0, concat_axis=0, tiled=True)

    def every(sel, got, pieces, couplings):
        blocks = {
            o % N_Z: jnp.concatenate([p[2 * k * T :][:T], p[(2 * k + 1) * T :][:T]], 1)
            for p, os in zip(pieces, OFFSETS)
            for k, o in enumerate(os)
        }
        twice = jnp.concatenate([blocks[o % N_Z] for o in range(2 * N_Z)])
        table = lax.dynamic_slice_in_dim(twice, (N_Z - z) % N_Z * T, COLUMN, 0)
        whole = to_all(table, PEERS).reshape(N_PEER * COLUMN, RH * A)
        leaf = adm_src.T.reshape(ENTRIES)
        place = ((leaf >> 11) * 8 + ((leaf >> 5) & 7)) * COLUMN + ((leaf >> 8) & 7) * T + (leaf & (T - 1))
        hot = (place[:, None] == jnp.arange(N_PEER * COLUMN, dtype=i32)[None, :]).astype(bf16)
        return couple_call(jnp.dot(hot, whole, preferred_element_type=f32), couplings)

    def some(sel, got, pieces, couplings):
        return select_call(sel, got, couplings)

    mine = lax.cond(fits[0] != 0, some, every, sel, got, pieces, couplings)
    theirs = shifted(mine, "n", 1)
    return final_call(scalars, mine, theirs, tgt_basis, near)


def solution(mesh):
    split = Mesh(
        mesh.devices.reshape(2, 8, 4, 2, mesh.shape["narrow"]), ("y", "z", "x", "c", "n")
    )
    in_specs = (
        P(WIDE, None, None),
        P(WIDE, None, "n"),
        P(WIDE),
        P(WIDE, None, "n"),
        P(WIDE, None, None),
        P(WIDE, None),
        P(WIDE, None, None),
    )
    out_specs = P(WIDE, None, "n")
    return jax.shard_map(body, mesh=split, in_specs=in_specs, out_specs=out_specs, check_vma=False)
```

```python
import math

import jax
import jax.numpy as jnp
from jax import lax
from jax.experimental import pallas as pl
from jax.experimental.pallas import tpu as pltpu
from jax.sharding import Mesh
from jax.sharding import PartitionSpec as P


WIDE = ("y", "z", "x", "c")
PEERS = ("y", "x", "c")

inverse_four_pi = 1.0 / (4.0 * math.pi)
soften_sq = 0.0025

T, R, A, J, HALF, LEAF = 32, 16, 64, 8, 256, 512
RH = R // 2
N_Z, N_PEER = 8, 16
CAP = 40
ENTRIES = T * J
OFFSETS = (0,), (2,), (-2,), (4,), (1, 3), (-1, -3)
COLUMN = N_Z * T
bf16, f32, i32 = jnp.bfloat16, jnp.float32, jnp.int32

VMEM = pl.BlockSpec(memory_space=pltpu.VMEM)
SMEM = pl.BlockSpec(memory_space=pltpu.SMEM)
LIMIT = pltpu.CompilerParams(vmem_limit_bytes=20 * 2**20)


def nt(a, b):
    return lax.dot_general(a, b, (((1,), (1,)), ((), ())), preferred_element_type=f32)


def nn(a, b):
    return lax.dot_general(a, b, (((1,), (0,)), ((), ())), preferred_element_type=f32)


def iota(shape, dim):
    return lax.broadcasted_iota(i32, shape, dim)


def folded(wide):
    two = wide[:, :128] + wide[:, 128:]
    return two[:, :64] + two[:, 64:]


def index_kernel(scalar_ref, adm_ref, pts_ref, sel_ref, req_ref, rows_ref):
    pts = pts_ref[...].astype(f32)
    blank = jnp.zeros((5, LEAF), f32)
    for t in range(T):
        rows_ref[t] = jnp.concatenate([pts[i, t : t + 1] for i in range(3)] + [blank], 0).astype(bf16)
    count = scalar_ref[0]
    adm = jnp.concatenate([adm_ref[...].astype(f32), jnp.zeros((8, 96), f32)], 1).T
    leaf = jnp.concatenate(
        [jnp.broadcast_to(adm[:T, j : j + 1], (T, 128)) for j in range(J)], 0
    ).astype(i32)
    live = (iota((ENTRIES, 128), 0) & (T - 1)) < count
    column = (leaf >> 11) * 8 + ((leaf >> 5) & 7)
    row = ((leaf >> 8) & 7) * T + (leaf & (T - 1))
    member = jnp.where((column == iota((ENTRIES, 128), 1)) & live, 1.0, 0.0)
    below = jnp.where(iota((ENTRIES, ENTRIES), 0) > iota((ENTRIES, ENTRIES), 1), 1.0, 0.0)
    rank = nn(below.astype(bf16), member.astype(bf16))
    place = jnp.sum(member * rank, axis=1, keepdims=True)
    over = jnp.max(place) > CAP - 0.5
    place = jnp.broadcast_to(place, (ENTRIES, 128))
    fits = live & (place < CAP - 0.5)
    sel = jnp.where(fits, column * CAP + place.astype(i32), -1)
    sel_ref[...] = sel
    sel_row = sel.astype(f32).T[:1]
    slots = N_PEER * CAP
    pick = jnp.where(iota((slots, ENTRIES), 0) == sel_row.astype(i32), 1.0, 0.0).astype(bf16)
    wanted = nn(pick, (row + 1).astype(f32).astype(bf16))
    wanted = jnp.where(over, -1.0, wanted)
    req_ref[...] = wanted.astype(bf16).reshape(N_PEER, CAP, 128)


def index_call(scalars, adm, points):
    return pl.pallas_call(
        index_kernel,
        out_shape=(
            jax.ShapeDtypeStruct((ENTRIES, 128), i32),
            jax.ShapeDtypeStruct((N_PEER, CAP, 128), bf16),
            jax.ShapeDtypeStruct((T, 8, LEAF), bf16),
        ),
        in_specs=[SMEM, VMEM, VMEM],
        out_specs=(VMEM,) * 3,
        name="requests",
        compiler_params=LIMIT,
    )(scalars, adm, points)


def coeff_kernel(n_ref, vec_ref, basis_ref, keep_ref, send_ref, held_ref, rows):
    n = n_ref[0]
    same = (iota((64, 256), 0) >> 4) == (iota((64, 256), 1) >> 6)
    for g in range(T // 4):
        lhs = vec_ref[4 * g : 4 * g + 4].reshape(64, HALF)
        held_ref[64 * g : 64 * g + 64] = lhs
        rhs = basis_ref[4 * g : 4 * g + 4].reshape(4 * A, HALF)
        rows[64 * g : 64 * g + 64, :64] = folded(jnp.where(same, nt(lhs, rhs), 0.0))
    for out, first in ((send_ref, (1 - n) * RH), (keep_ref, n * RH)):
        for r in range(0, RH, 2):
            pair = [rows[pl.ds(first + r + k, T, stride=R), :][:, :64] for k in range(2)]
            row, lane = r * A // HALF * T, r * A % HALF
            out[row : row + T, lane : lane + 2 * A] = jnp.concatenate(pair, 1)


def coeff_call(n, vectors, basis):
    return pl.pallas_call(
        coeff_kernel,
        out_shape=(
            jax.ShapeDtypeStruct((2 * T, HALF), f32),
            jax.ShapeDtypeStruct((2 * T, HALF), f32),
            jax.ShapeDtypeStruct((T * R, HALF), bf16),
        ),
        in_specs=[SMEM, VMEM, VMEM],
        out_specs=(VMEM, VMEM, VMEM),
        scratch_shapes=[pltpu.VMEM((T * R, 128), f32)],
        name="coeffs",
        compiler_params=LIMIT,
    )(n, vectors, basis)


def pack_kernel(z_ref, req_ref, *refs):
    *pieces, out_ref, fits_ref, table_ref = refs
    refused = jnp.min(req_ref[:, :8].astype(f32)) < 0.0
    fits_ref[0] = jnp.where(refused, 0, 1)
    for piece, offsets in zip(pieces, OFFSETS):
        for k, offset in enumerate(offsets):
            first = pl.multiple_of(((z_ref[0] + offset) & (N_Z - 1)) * T, T)
            for h in range(2):
                row = (2 * k + h) * T
                table_ref[pl.ds(first, T), h * HALF : (h + 1) * HALF] = piece[row : row + T]
    lanes = iota((CAP, 128), 1).astype(f32) + 1.0
    for r in range(0, N_PEER, 4):
        want = [req_ref[r + k].astype(f32) for k in range(4)]
        hot = [
            jnp.concatenate(
                [jnp.where(w == lanes, 1.0, 0.0), jnp.where(w == lanes + 128.0, 1.0, 0.0)], 1
            )
            for w in want
        ]
        picked = nn(jnp.concatenate(hot, 0).astype(bf16), table_ref[...])
        out_ref[r : r + 4] = picked.astype(bf16).reshape(4, CAP, RH * A)


def pack_call(z, req, pieces):
    return pl.pallas_call(
        pack_kernel,
        out_shape=(
            jax.ShapeDtypeStruct((N_PEER, CAP, RH * A), bf16),
            jax.ShapeDtypeStruct((1,), i32),
        ),
        in_specs=[SMEM] + [VMEM] * (1 + len(pieces)),
        out_specs=(VMEM, SMEM),
        scratch_shapes=[pltpu.VMEM((COLUMN, RH * A), bf16)],
        name="pack",
        compiler_params=LIMIT,
    )(z, req, *pieces)


def couple(picked, couple_ref, out_ref):
    lows = [picked[j * T : (j + 1) * T] for j in range(J)]
    by_rhs = []
    for r in range(RH):
        cols = [low[:, r * A : (r + 1) * A] for low in lows]
        by_rhs.append(jnp.concatenate(cols, 1).astype(bf16))
    row_t = iota((16 * RH, 256), 0) & 15
    col_t = iota((16 * RH, 256), 1) >> 6
    for h in range(2):
        lhs = jnp.concatenate([s[16 * h : 16 * h + 16] for s in by_rhs], 0)
        total = jnp.zeros((16 * RH, A), f32)
        for g in range(4):
            first = 16 * h + 4 * g
            rhs = couple_ref[first : first + 4].reshape(4 * A, J * A)
            total = total + folded(jnp.where(row_t == col_t + 4 * g, nt(lhs, rhs), 0.0))
        total = total.reshape(RH, 16, A)
        for r in range(0, RH, 2):
            pair = jnp.concatenate([total[r], total[r + 1]], 1)
            out_ref[r // 2, 16 * h : 16 * h + 16, :] = pair.astype(bf16)


def select_kernel(sel_ref, got_ref, couple_ref, out_ref):
    slots = N_PEER * CAP
    sel = sel_ref[...]
    lanes = iota((ENTRIES, 128), 1)
    hot = jnp.concatenate(
        [jnp.where(sel == lanes + 128 * k, 1.0, 0.0) for k in range(slots // 128)], 1
    )
    picked = nn(hot.astype(bf16), got_ref[...].reshape(slots, RH * A))
    couple(picked, couple_ref, out_ref)


TC_SHAPE = jax.ShapeDtypeStruct((RH // 2, T, 2 * A), bf16)


def select_call(sel, got, couplings):
    return pl.pallas_call(
        select_kernel,
        out_shape=TC_SHAPE,
        in_specs=[VMEM, VMEM, VMEM],
        out_specs=VMEM,
        name="select",
        compiler_params=LIMIT,
    )(sel, got, couplings)


def couple_kernel(picked_ref, couple_ref, out_ref):
    couple(picked_ref[...], couple_ref, out_ref)


def couple_call(picked, couplings):
    return pl.pallas_call(
        couple_kernel,
        out_shape=TC_SHAPE,
        in_specs=[VMEM, VMEM],
        out_specs=VMEM,
        name="couple",
        compiler_params=LIMIT,
    )(picked, couplings)


def near_kernel(kind, leaves, group, scalar_ref, pts_ref, vec_ref, other_ref, *refs):
    edges, send_refs = (), ()
    refs, kerns = refs[:-group], refs[-group:]
    if kind == "early":
        out_ref, *send_refs = refs
    else:
        *edges, _, out_ref = refs
    count, n = scalar_ref[0], scalar_ref[1]
    own = pl.multiple_of(n * HALF, HALF)
    other = pl.multiple_of((1 - n) * HALF, HALF)

    def values_of(ref, t):
        return ref[pl.ds(pl.multiple_of(t * R, R), R)]

    for ref, t in zip(send_refs, (0, count - 1)):
        ref[:R, pl.ds(own, HALF)] = values_of(vec_ref, t)
        ref[:R, pl.ds(other, HALF)] = values_of(other_ref, t)
        ref[R:] = pts_ref[t]

    def sources(t):
        return (t + T - 1) & (T - 1), t, (t + 1) & (T - 1)

    def taken(t, rows, values):
        if not edges:
            return values
        for k, (u, at) in enumerate(((0, 0), (2, count - 1))):
            halo = [edges[k][rows, pl.ds(h, HALF)] for h in (own, other)]
            values[u] = [jnp.where(t == at, a, b) for a, b in zip(halo, values[u])]
        return values

    def fill(t, kern):
        x = pts_ref[t, :, pl.ds(own, HALF)].astype(f32).T.astype(bf16)
        points = [[pts_ref[u, :, pl.ds(h, HALF)] for h in (own, other)] for u in sources(t)]
        points = taken(t, slice(R, R + 8), points)
        for k in range(3):
            for p in range(0, HALF, 32):
                for h, y in enumerate(points[k]):
                    squared = None
                    for i in range(3):
                        differ = x[p : p + 32, i : i + 1] - y[i : i + 1, :]
                        differ = differ * differ
                        squared = differ + bf16(soften_sq) if squared is None else squared + differ
                    lane = k * LEAF + h * HALF
                    kern[p : p + 32, lane : lane + HALF] = lax.rsqrt(squared)

    def product(t, kern):
        values = [[values_of(vec_ref, u), values_of(other_ref, u)] for u in sources(t)]
        values = taken(t, slice(0, R), values)
        values = jnp.concatenate([v for pair in values for v in pair], 1)
        out_ref[t] = nt(values, kern[...]) * inverse_four_pi

    def leaf(i):
        if not edges:
            return leaves[0] + i
        i = jnp.where(i < leaves[0], i, i + leaves[1] - leaves[0])
        return jnp.where(i < T, i, count - 1)

    steps, group = near_steps(kind, leaves), len(kerns)
    fill(leaf(0), kerns[0])

    def body(i, ends):
        for s in range(group):
            if not ends or s < group - 1:
                fill(leaf(group * i + s + 1), kerns[(s + 1) % group])
            product(leaf(group * i + s), kerns[s])
        return 0

    whole = steps // group - 1
    if whole:
        lax.fori_loop(0, whole, lambda i, _: body(i, False), 0)
    lax.fori_loop(whole, whole + 1, lambda i, _: body(i, True), 0)


def near_steps(kind, leaves):
    return T - leaves[1] + leaves[0] + 1 if kind == "rest" else leaves[1] - leaves[0]


def near_call(kind, leaves, group, args, more=()):
    field = jax.ShapeDtypeStruct((T, R, HALF), f32)
    edge = jax.ShapeDtypeStruct((R + 8, LEAF), bf16)
    outs = (field, edge, edge) if kind == "early" else (field,)
    return pl.pallas_call(
        lambda *refs: near_kernel(kind, leaves, group, *refs),
        out_shape=outs,
        in_specs=[SMEM] + [VMEM] * (len(args) - 1 + len(more)),
        out_specs=(VMEM,) * len(outs),
        scratch_shapes=[pltpu.VMEM((HALF, 3 * LEAF), bf16)] * group,
        input_output_aliases={} if kind == "early" else {len(args) + len(more) - 1: 0},
        cost_estimate=pl.CostEstimate(
            flops=near_steps(kind, leaves) * 200_000_000, bytes_accessed=2_000_000, transcendentals=0
        ),
        name="near",
        compiler_params=LIMIT,
    )(*args, *more)


def final_kernel(scalar_ref, mine_ref, theirs_ref, tgt_ref, near_ref, out_ref, rows):
    count, n = scalar_ref[0], scalar_ref[1]
    for ref, first in ((mine_ref, n * RH), (theirs_ref, (1 - n) * RH)):
        for r in range(RH):
            part = ref[r // 2].astype(f32)[:, (r % 2) * A : (r % 2 + 1) * A]
            rows[pl.ds(first + r, T, stride=R), :] = jnp.concatenate([part, part], 1)
    same = (iota((64, 256), 0) >> 4) == (iota((64, 256), 1) >> 6)
    for g in range(T // 4):
        part = rows[64 * g : 64 * g + 64, :]
        lhs = jnp.where(same, jnp.concatenate([part, part], 1), 0.0).astype(bf16)
        tgt = tgt_ref[4 * g : 4 * g + 4, :, pl.ds(pl.multiple_of(n * HALF, HALF), HALF)]
        far = nn(lhs, tgt.reshape(4 * A, HALF)).reshape(4, R, HALF)
        total = far + near_ref[4 * g : 4 * g + 4]
        live = (iota((4, R, HALF), 0) + 4 * g) < count
        out_ref[4 * g : 4 * g + 4] = jnp.where(live, total, 0.0).astype(bf16)


def final_call(scalars, mine, theirs, tgt, near):
    return pl.pallas_call(
        final_kernel,
        out_shape=jax.ShapeDtypeStruct((T, R, HALF), bf16),
        in_specs=[SMEM] + [VMEM] * 4,
        out_specs=VMEM,
        scratch_shapes=[pltpu.VMEM((T * R, 128), f32)],
        name="final",
        compiler_params=LIMIT,
    )(scalars, mine, theirs, tgt, near)


def shifted(array, axis, by):
    devices = lax.axis_size(axis)
    return lax.ppermute(array, axis, [(i, (i + by) % devices) for i in range(devices)])


def to_all(array, axis):
    copies = jnp.broadcast_to(array[None], (lax.axis_size(axis), *array.shape))
    return lax.all_to_all(copies, axis, split_axis=0, concat_axis=0, tiled=True)


def body(points, vectors, counts, src_basis, tgt_basis, adm_src, couplings):
    n = lax.axis_index("n").astype(i32)
    z = lax.axis_index("z").astype(i32)
    scalars = jnp.stack([counts[0], n])

    keep, send, held = coeff_call(n[None], vectors, src_basis)
    came = shifted(send, "n", 1)
    other = shifted(held, "n", 1)
    sel, req, rows = index_call(scalars, adm_src.T, points.transpose(1, 0, 2))
    asked = lax.all_to_all(req, PEERS, split_axis=0, concat_axis=0, tiled=True)

    coeffs = (keep + came).astype(bf16)
    up = shifted(coeffs, "z", -2)
    down = shifted(coeffs, "z", 2)
    across = shifted(coeffs, "z", 4)
    odd_up = shifted(jnp.concatenate([coeffs, up]), "z", -1)
    odd_down = shifted(jnp.concatenate([coeffs, down]), "z", 1)
    pieces = coeffs, up, down, across, odd_up, odd_down

    near_args = (scalars, rows, held, other)
    near, first, last = near_call("early", (3, 11), 8, near_args)
    halos = shifted(last, WIDE, 1), shifted(first, WIDE, -1)
    (near,) = near_call("inner", (11, 29), 18, near_args, (near,))
    (near,) = near_call("rest", (3, 29), 7, near_args, (*halos, near))

    packed, fits = pack_call(z[None], asked, pieces)
    got = lax.all_to_all(packed, PEERS, split_axis=0, concat_axis=0, tiled=True)

    def every(sel, got, pieces, couplings):
        blocks = {
            o % N_Z: jnp.concatenate([p[2 * k * T :][:T], p[(2 * k + 1) * T :][:T]], 1)
            for p, os in zip(pieces, OFFSETS)
            for k, o in enumerate(os)
        }
        twice = jnp.concatenate([blocks[o % N_Z] for o in range(2 * N_Z)])
        table = lax.dynamic_slice_in_dim(twice, (N_Z - z) % N_Z * T, COLUMN, 0)
        whole = to_all(table, PEERS).reshape(N_PEER * COLUMN, RH * A)
        leaf = adm_src.T.reshape(ENTRIES)
        place = ((leaf >> 11) * 8 + ((leaf >> 5) & 7)) * COLUMN + ((leaf >> 8) & 7) * T + (leaf & (T - 1))
        hot = (place[:, None] == jnp.arange(N_PEER * COLUMN, dtype=i32)[None, :]).astype(bf16)
        return couple_call(jnp.dot(hot, whole, preferred_element_type=f32), couplings)

    def some(sel, got, pieces, couplings):
        return select_call(sel, got, couplings)

    mine = lax.cond(fits[0] != 0, some, every, sel, got, pieces, couplings)
    theirs = shifted(mine, "n", 1)
    return final_call(scalars, mine, theirs, tgt_basis, near)


def solution(mesh):
    split = Mesh(
        mesh.devices.reshape(2, 8, 4, 2, mesh.shape["narrow"]), ("y", "z", "x", "c", "n")
    )
    in_specs = (
        P(WIDE, None, None),
        P(WIDE, None, "n"),
        P(WIDE),
        P(WIDE, None, "n"),
        P(WIDE, None, None),
        P(WIDE, None),
        P(WIDE, None, None),
    )
    out_specs = P(WIDE, None, "n")
    return jax.shard_map(body, mesh=split, in_specs=in_specs, out_specs=out_specs, check_vma=False)
```
